256 devices in a mesh: groups: 2 (over y), gx: 16 (over z), gy: 4 (over x), gz: 2 (over core).
Axes of the slice: x: 4, y: 2, z: 16, core: 2. Of those that a mesh axis runs over, the one named last changes fastest.
The devices are a block of a 4x16x16 slice.
Arguments:
- charge: float32 [512, 128, 256], P(('groups', 'gx'), 'gy', 'gz'), parts along dimension 0, may hold values from -6 to 6
Outputs:
- potential: float32 [512, 128, 256], P(('groups', 'gx'), 'gy', 'gz'), parts along dimension 0
The draws below stay inside these ranges and needn't reach their ends.
There are 2 independent parts, one for each index of `groups`. The reference program is written for one: setup_inputs(seed, part) draws one part's arguments, and reference() takes and returns one part's arrays. A program takes and returns all parts, laid end to end along the dimension named above; each array names one. Nothing has to cross between parts.
All inputs are finite; a program needn't handle non-finite values.
Results may differ from the reference program's by a relative error of at most 0.0001.
Values sent between devices are 32-bit elements; how exact they have to be, the bound alone decides.
No kernel may reach another device: no remote copies, remote signals or barrier semaphores. Data moves between devices by JAX's collectives and lax.ppermute only.
A program may use at most 128 MiB of HBM per device.

```python
import jax
import jax.numpy as jnp

CYCLES = 2
SWEEPS = 2
SLEV = 4
RLEV = 3
NX = 256
NY = 128
NZ = 256


def block_levels(own_key, extent, pieces, low, top_value):
    level = 1.0
    for dim, parts in pieces:
        heights = jax.random.uniform(jax.random.fold_in(jax.random.fold_in(own_key, 6), dim), (parts,), jnp.float32, low / len(pieces), top_value / len(pieces))
        level = level * jnp.repeat(jnp.exp(heights), extent[dim] // parts).reshape((-1,) + (1,) * (len(extent) - 1 - dim))
    return level


def gaussian(key, shape, scale, most, pieces=(), dtype=jnp.bfloat16):
    drawn = jax.random.normal(key, shape, jnp.float32) * scale
    if len(pieces) > 0:
        drawn = block_levels(key, shape, pieces, -0.22, 0.18) * drawn
    return jnp.clip(drawn, min=-most, max=most).astype(dtype)


def setup_inputs(seed: int = 0, part: int = 0) -> dict:
    streams_of = jax.random.split(jax.random.key(seed), 2)
    part_splits = jax.random.split(jax.random.fold_in(streams_of[1], part), 2)
    return {
        "charge": gaussian(part_splits[0], (NX, NY, NZ), 1.0, 6.0, ((0, 16), (1, 4), (2, 2)), jnp.float32),
    }


OMEGA = 2.0 / 3.0
SCREEN = 0.001


def operate(field, scale):
    beside_all = jnp.roll(field, 1, 0) + jnp.roll(field, -1, 0)
    beside_all = beside_all + jnp.roll(field, 1, 1) + jnp.roll(field, -1, 1)
    beside_all = beside_all + jnp.roll(field, 1, 2) + jnp.roll(field, -1, 2)
    return (6.0 * field - beside_all) * scale + SCREEN * field


def relax(field, source, scale):
    return field + OMEGA * (source - operate(field, scale)) / (6.0 * scale + SCREEN)


def restrict(field):
    size_x, size_y, size_z = field.shape
    blocks = field.reshape(size_x // 2, 2, size_y // 2, 2, size_z // 2, 2)
    return blocks.mean(axis=(1, 3, 5))


def prolong(field):
    return jnp.repeat(jnp.repeat(jnp.repeat(field, 2, 0), 2, 1), 2, 2)


def cycle(level, source, field):
    scale = 0.25 ** level
    for sweep in range(SWEEPS):
        field = relax(field, source, scale)
    if level == SLEV + RLEV - 1:
        return field
    residual = source - operate(field, scale)
    coarse_rhs = restrict(residual)
    correction = cycle(level + 1, coarse_rhs, jnp.zeros(coarse_rhs.shape, jnp.float32))
    field = field + prolong(correction)
    for sweep in range(SWEEPS):
        field = relax(field, source, scale)
    return field


def reference(charge):
    potential = jnp.zeros(charge.shape, jnp.float32)
    for turn in range(CYCLES):
        potential = cycle(0, charge, potential)
    return potential
```

```python
import functools

import jax
import jax.numpy as jnp
from jax import lax
from jax.experimental import pallas as pl
from jax.experimental.pallas import tpu as pltpu
from jax.sharding import PartitionSpec as P

CYCLES = 2
LANES = 128
OMEGA = 2.0 / 3.0
SCREEN = 0.001
F32 = jnp.float32

BX, BY = 16, 32
X0, Y0, XA0, YA0 = 12, 24, 40, 80
X1, Y1, XA1, YA1 = 10, 16, 32, 48
HALO = 10


def coefficients(level):
    a = 0.25**level
    d = 6.0 * a + SCREEN
    k = OMEGA / d
    return a, d, k


def iota(shape, dim):
    return lax.broadcasted_iota(jnp.int32, shape, dim)


def parts(v):
    high = v.astype(jnp.bfloat16)
    rest = v - high.astype(F32)
    middle = rest.astype(jnp.bfloat16)
    return high, middle, (rest - middle.astype(F32)).astype(jnp.bfloat16)


def product(a, b):
    return lax.dot_general(a, b, (((1,), (0,)), ((), ())), preferred_element_type=F32)


def dot(a, b):
    b = b.astype(jnp.bfloat16)
    high, middle, low = (product(p, b) for p in parts(a))
    return high + (middle + low)


def dot_rows(a, b):
    a = a.astype(jnp.bfloat16)
    high, middle, low = (product(a, p) for p in parts(b))
    return high + (middle + low)


def halves_beside(lo, hi):
    lane = iota(lo.shape, 1)
    first, last = lane == 0, lane == LANES - 1
    rl, rh = pltpu.roll(lo, 1, 1), pltpu.roll(hi, 1, 1)
    sl, sh = pltpu.roll(lo, LANES - 1, 1), pltpu.roll(hi, LANES - 1, 1)
    return (
        jnp.where(first, rh, rl) + jnp.where(last, sh, sl),
        jnp.where(first, rl, rh) + jnp.where(last, sl, sh),
    )


def beside_0(refs, i, j, rows):
    centre = [r[i, pl.ds(j, rows), :] for r in refs]
    along_z = halves_beside(*centre)
    out = []
    for r, z in zip(refs, along_z):
        out.append(
            (r[i - 1, pl.ds(j, rows), :] + r[i + 1, pl.ds(j, rows), :])
            + (r[i, pl.ds(j - 1, rows), :] + r[i, pl.ds(j + 1, rows), :])
            + z
        )
    return centre, out


def over_layers(start, count, block, body):
    def step(b, carry):
        for u in range(block):
            body(start + b * block + u)
        return carry

    lax.fori_loop(0, -(-count // block), step, 0)


def sweep_0(dst, src, force, halo, first=False, rows=48, chunk=16, block=4):
    a, d, k = coefficients(0)

    def body(i):
        for j in range(Y0 - 8, Y0 - 8 + rows, chunk) if not first else range(Y0 - 16, Y0 + 48, chunk):
            centre, nb = beside_0(src, i, j, chunk)
            for h in range(len(dst)):
                if first:
                    dst[h][i, pl.ds(j, chunk), :] = k * (2.0 - OMEGA) * centre[h] + k * k * a * nb[h]
                else:
                    f = force[h][i, pl.ds(j, chunk), :]
                    dst[h][i, pl.ds(j, chunk), :] = (1.0 - OMEGA) * centre[h] + k * f + k * a * nb[h]

    over_layers(X0 - halo, BX + 2 * halo, block, body)


def residual_0(dst, src, force, halo, block=4, chunk=16):
    a, d, _ = coefficients(0)

    def body(i):
        for j in range(Y0 - 8, Y0 + 40, chunk):
            centre, nb = beside_0(src, i, j, chunk)
            for h in range(2):
                f = force[h][i, pl.ds(j, chunk), :]
                dst[h][i, pl.ds(j, chunk), :] = f - d * centre[h] + a * nb[h]

    over_layers(X0 - halo, BX + 2 * halo, block, body)


def mean_matrix(coarse, fine_of_out, weight):
    source, out = iota((LANES, LANES), 0), fine_of_out(iota((LANES, LANES), 1))
    return jnp.where((source == out) | (source == out + 1), weight, 0.0).astype(F32)


def pick_matrix(source_of_out):
    return jnp.where(iota((LANES, LANES), 0) == source_of_out(iota((LANES, LANES), 1)), 1.0, 0.0).astype(F32)


def restrict_0(f1, r, halo):
    low = mean_matrix(64, lambda o: jnp.where(o < 64, 2 * o, -2), 0.125)
    high = mean_matrix(64, lambda o: jnp.where(o >= 64, 2 * o - 128, -2), 0.125)
    layers = BX // 2 + 2 * halo

    def step(b, carry):
        sums = []
        for h in range(2):
            rows = []
            for u in range(2):
                i = X0 - 2 * halo + 2 * (2 * b + u)
                rows.append(
                    (r[h][i, pl.ds(Y0 - 8, 24, stride=2), :] + r[h][i, pl.ds(Y0 - 7, 24, stride=2), :])
                    + (r[h][i + 1, pl.ds(Y0 - 8, 24, stride=2), :] + r[h][i + 1, pl.ds(Y0 - 7, 24, stride=2), :])
                )
            sums.append(jnp.concatenate(rows, axis=0))
        out = dot(sums[0], low) + dot(sums[1], high)
        for u in range(2):
            f1[X1 - halo + 2 * b + u, pl.ds(Y1 - 4, 24), :] = out[24 * u : 24 * u + 24]
        return carry

    lax.fori_loop(0, layers // 2, step, 0)


def beside_1(ref, i, j, rows):
    centre = ref[i, pl.ds(j, rows), :]
    nb = (
        (ref[i - 1, pl.ds(j, rows), :] + ref[i + 1, pl.ds(j, rows), :])
        + (ref[i, pl.ds(j - 1, rows), :] + ref[i, pl.ds(j + 1, rows), :])
        + (pltpu.roll(centre, 1, 1) + pltpu.roll(centre, LANES - 1, 1))
    )
    return centre, nb


def sweep_1(dst, src, force, halo, first=False, block=8):
    a, d, k = coefficients(1)

    def body(i):
        centre, nb = beside_1(src, i, Y1 - 8, 32)
        if first:
            new = k * (2.0 - OMEGA) * centre + k * k * a * nb
        else:
            new = (1.0 - OMEGA) * centre + k * force[i, pl.ds(Y1 - 8, 32), :] + k * a * nb
        dst[i, pl.ds(Y1 - 8, 32), :] = new

    over_layers(X1 - halo, BX // 2 + 2 * halo, block, body)


def coarse_source(out, f1, v1, r1, core):
    a, d, _ = coefficients(1)
    sweep_1(v1, f1, None, 1, first=True, block=5)

    def body(i):
        centre, nb = beside_1(v1, i, Y1, 16)
        r1[i, pl.ds(Y1, 16), :] = f1[i, pl.ds(Y1, 16), :] - d * centre + a * nb

    over_layers(X1, BX // 2, 8, body)
    layers = []
    for q in range(4):
        i = X1 + 2 * q
        s = (r1[i, pl.ds(Y1, 8, stride=2), :] + r1[i, pl.ds(Y1 + 1, 8, stride=2), :]) + (
            r1[i + 1, pl.ds(Y1, 8, stride=2), :] + r1[i + 1, pl.ds(Y1 + 1, 8, stride=2), :]
        )
        layers.append(jnp.where(core == 0, s[0:4], s[4:8]))
    low = mean_matrix(64, lambda o: jnp.where(o < 64, 2 * o, -2), 0.125)
    high = mean_matrix(64, lambda o: jnp.where(o >= 64, 2 * o - 128, -2), 0.125)
    packed = dot(jnp.concatenate(layers[0:2], axis=0), low) + dot(jnp.concatenate(layers[2:4], axis=0), high)
    for s in range(out.shape[0]):
        out[s] = packed


def beside_whole(v):
    n = v.shape[0]
    up = jnp.concatenate([v[n - 1 :], v[: n - 1]], axis=0)
    down = jnp.concatenate([v[1:], v[:1]], axis=0)
    y = pltpu.roll(v, 1, 1) + pltpu.roll(v, v.shape[1] - 1, 1)
    return (up + down) + y + (pltpu.roll(v, 1, 2) + pltpu.roll(v, LANES - 1, 2))


def from_zero(level, f):
    a, d, k = coefficients(level)
    return k * (2.0 - OMEGA) * f + k * k * a * beside_whole(f)


def residual_whole(level, f, v):
    a, d, k = coefficients(level)
    return f - d * v + a * beside_whole(v)


def smooth_whole(level, f, v):
    a, d, k = coefficients(level)
    for _ in range(2):
        v = (1.0 - OMEGA) * v + k * f + k * a * beside_whole(v)
    return v


def down_z(level):
    n = 256 >> (level + 1)
    return mean_matrix(n, lambda o: 2 * lax.rem(o, n), 0.125)


def up_z(level):
    n = 256 >> level
    return pick_matrix(lambda o: lax.div(lax.rem(o, n), 2))


def pair_layers(v):
    v = v.reshape(v.shape[0] // 2, 2, *v.shape[1:])
    return v[:, 0] + v[:, 1]


def twice(v):
    return jnp.concatenate([v[:, None], v[:, None]], axis=1).reshape(2 * v.shape[0], *v.shape[1:])


def row_sums(size, y_size):
    out, source = iota((size, size), 0), iota((size, size), 1)
    first = (out // 8) * 8 + 2 * lax.rem(lax.rem(out, 8), y_size)
    return jnp.where((source == first) | (source == first + 1), 1.0, 0.0).astype(F32)


def row_picks(size, y_size):
    out, source = iota((size, size), 0), iota((size, size), 1)
    first = (out // 8) * 8 + lax.div(lax.rem(lax.rem(out, 8), y_size), 2)
    return jnp.where(source == first, 1.0, 0.0).astype(F32)


def solve_3(f3, t3):
    v3 = from_zero(3, f3)
    t3[...] = pair_layers(residual_whole(3, f3, v3))
    s = t3[:, pl.ds(0, 8, stride=2), :] + t3[:, pl.ds(1, 8, stride=2), :]
    f4 = dot(s.reshape(128, LANES), down_z(3)).reshape(16, 8, LANES)
    v4 = from_zero(4, f4)
    s = pair_layers(residual_whole(4, f4, v4)).reshape(64, LANES)
    f5 = dot_rows(row_sums(64, 4), dot(s, down_z(4))).reshape(8, 8, LANES)
    v5 = from_zero(5, f5)
    s = pair_layers(residual_whole(5, f5, v5)).reshape(32, LANES)
    f6 = dot_rows(row_sums(32, 2), dot(s, down_z(5))).reshape(4, 8, LANES)
    v6 = from_zero(6, f6)
    e5 = dot_rows(row_picks(32, 4), dot(v6.reshape(32, LANES), up_z(5))).reshape(4, 8, LANES)
    v5 = smooth_whole(5, f5, v5 + twice(e5))
    e4 = dot_rows(row_picks(64, 8), dot(v5.reshape(64, LANES), up_z(4))).reshape(8, 8, LANES)
    v4 = smooth_whole(4, f4, v4 + twice(e4))
    e3 = dot(v4.reshape(128, LANES), up_z(3)).reshape(16, 8, LANES)
    t3[:, pl.ds(0, 8, stride=2), :] = e3
    t3[:, pl.ds(1, 8, stride=2), :] = e3
    return smooth_whole(3, f3, v3 + twice(t3[...]))


def unpack_2(f2, mine, other, core):
    low = iota((8, LANES), 1) < 64
    top = iota((8, LANES), 0) < 4

    def step(gx, carry):
        for gy in range(4):
            t, p = mine[gx * 4 + gy], other[gx * 4 + gy]
            tr, pr = pltpu.roll(t, 64, 1), pltpu.roll(p, 64, 1)
            for xp in range(2):
                d = jnp.where(low, t, tr) if xp == 0 else jnp.where(low, tr, t)
                e = jnp.where(low, p, pr) if xp == 0 else jnp.where(low, pr, p)
                e = pltpu.roll(e, 32, 1)
                u, w = jnp.where(core == 0, d, e), jnp.where(core == 0, e, d)
                f2[gx * 4 + 2 * xp, pl.ds(gy * 8, 8), :] = jnp.where(top, u, pltpu.roll(w, 4, 0))
                f2[gx * 4 + 2 * xp + 1, pl.ds(gy * 8, 8), :] = jnp.where(top, pltpu.roll(u, 4, 0), w)
        return carry

    lax.fori_loop(0, f2.shape[0] // 4, step, 0)


def beside_2(ref, i):
    n = ref.shape[0]
    centre = ref[i]
    nb = (
        (ref[lax.rem(i + n - 1, n)] + ref[lax.rem(i + 1, n)])
        + (pltpu.roll(centre, 1, 0) + pltpu.roll(centre, 31, 0))
        + (pltpu.roll(centre, 1, 1) + pltpu.roll(centre, LANES - 1, 1))
    )
    return centre, nb


def level_2(near, f2, v2, t2, t3, s3, p2, a2, b2, gx, halo):
    a, d, k = coefficients(2)

    def first(i):
        centre, nb = beside_2(f2, i)
        v2[i] = k * (2.0 - OMEGA) * centre + k * k * a * nb

    over_layers(0, 64, 8, first)

    def step(b, carry):
        for u in range(4):
            q = 4 * b + u
            pair = []
            for i in (2 * q, 2 * q + 1):
                centre, nb = beside_2(v2, i)
                pair.append(f2[i] - d * centre + a * nb)
            t2[q] = pair[0] + pair[1]
        return carry

    lax.fori_loop(0, 8, step, 0)
    s = t2[:, pl.ds(0, 16, stride=2), :] + t2[:, pl.ds(1, 16, stride=2), :]
    f3 = dot(s.reshape(512, LANES), down_z(2)).reshape(32, 16, LANES)
    s3[...] = solve_3(f3, t3)

    count = 4 + 2 * halo + 4
    start = gx * 4 - halo - 2 + 64
    e = jnp.concatenate([s3[lax.rem(lax.div(start, 2) + m, 32)] for m in range(count // 2)], axis=0)
    e = dot(e, up_z(2)).reshape(count // 2, 16, LANES)
    p2[pl.ds(0, count // 2), pl.ds(0, 16, stride=2), :] = e
    p2[pl.ds(0, count // 2), pl.ds(1, 16, stride=2), :] = e
    for m in range(count):
        a2[m] = v2[lax.rem(start + m, 64)] + p2[m // 2]
    for dst, src, low, high in ((b2, a2, 1, count - 1), (near, b2, 2, count - 2)):
        for m in range(low, high):
            centre = src[m]
            nb = (
                (src[m - 1] + src[m + 1])
                + (pltpu.roll(centre, 1, 0) + pltpu.roll(centre, 31, 0))
                + (pltpu.roll(centre, 1, 1) + pltpu.roll(centre, LANES - 1, 1))
            )
            at = m if dst is b2 else m - 2
            dst[at] = (1.0 - OMEGA) * centre + k * f2[lax.rem(start + m, 64)] + k * a * nb


def add_from_2(v1, near, y2, p1, gy, halo):
    layers = 4 + 2 * halo
    for m in range(layers):
        y2[m, pl.ds(0, 32), :] = near[m]
        y2[m, pl.ds(32, 32), :] = near[m]
    start = pl.multiple_of(lax.rem(gy * 8 + 28, 32), 4)
    picked = jnp.concatenate([y2[m, pl.ds(start, 16), :] for m in range(layers)], axis=0)
    e = dot(picked, pick_matrix(lambda o: lax.div(o, 2))).reshape(layers, 16, LANES)
    p1[pl.ds(0, layers), pl.ds(0, 16, stride=2), :] = e
    p1[pl.ds(0, layers), pl.ds(1, 16, stride=2), :] = e
    for m in range(2 * layers):
        i = X1 - 2 * halo + m
        v1[i, pl.ds(Y1 - 8, 32), :] = v1[i, pl.ds(Y1 - 8, 32), :] + p1[m // 2]


def add_from_1(w, v, v1, p0, halo, offset):
    low = pick_matrix(lambda o: lax.div(o, 2))
    high = pick_matrix(lambda o: 64 + lax.div(o, 2))
    x_at, y_at, rows = offset

    def step(b, carry):
        lines = jnp.concatenate([v1[X1 - halo + 2 * b + u, pl.ds(Y1 - 8, 32), :] for u in range(2)], axis=0)
        for h, matrix in enumerate((low, high)):
            e = dot(lines, matrix)
            for u in range(2):
                p0[2 * h + u, pl.ds(0, 32, stride=2), :] = e[32 * u : 32 * u + 32]
                p0[2 * h + u, pl.ds(1, 32, stride=2), :] = e[32 * u : 32 * u + 32]
        for h in range(2):
            for u in range(4):
                x = -2 * halo + 4 * b + u
                skip = y_at - rows[0]
                w[h][X0 + x, pl.ds(Y0 - skip, rows[1]), :] = (
                    v[h][x_at + x, pl.ds(rows[0], rows[1]), :] + p0[2 * h + u // 2, pl.ds(16 - skip, rows[1]), :]
                )
        return carry

    lax.fori_loop(0, (BX // 2 + 2 * halo) // 2, step, 0)


def lay_out_1(dst, f1, x_low, x_high, y_low, y_high, own, width):
    count = f1.shape[0]
    for m in range(count):
        i = X1 - own + m
        dst[i, pl.ds(Y1 - 4, 24), :] = f1[m]
        dst[i, pl.ds(Y1 - own - width, width), :] = y_low[pl.ds(m * width, width), :]
        dst[i, pl.ds(Y1 + 16 + own, width), :] = y_high[pl.ds(m * width, width), :]
    for m in range(width):
        dst[X1 - own - width + m, pl.ds(Y1 - 4, 24), :] = x_low[m]
        dst[X1 + 8 + own + m, pl.ds(Y1 - 4, 24), :] = x_high[m]


def put_out_1(out, up_y, down_y, f1, own, width):
    for m in range(out.shape[0]):
        i = X1 - own + m
        out[m] = f1[i, pl.ds(Y1 - 4, 24), :]
        up_y[pl.ds(m * width, width), :] = f1[i, pl.ds(Y1 + 16 - own - width, width), :]
        down_y[pl.ds(m * width, width), :] = f1[i, pl.ds(Y1 + own, width), :]


def edges_kernel(mine, x_low, x_high, up, down):
    at = 0
    for ref in (x_low, mine, x_high):
        for i in range(ref.shape[0]):
            down[pl.ds(at * HALO, HALO), :] = ref[i, pl.ds(0, HALO), :]
            up[pl.ds(at * HALO, HALO), :] = ref[i, pl.ds(BY - HALO, HALO), :]
            at += 1


def lay_out_0(dst, mine, x_low, x_high, y_low, y_high):
    dst[pl.ds(X0, BX), pl.ds(Y0, BY), :] = mine[...]
    dst[pl.ds(X0 - HALO, HALO), pl.ds(Y0, BY), :] = x_low[...]
    dst[pl.ds(X0 + BX, HALO), pl.ds(Y0, BY), :] = x_high[...]
    for m in range(BX + 2 * HALO):
        dst[X0 - HALO + m, pl.ds(Y0 - HALO, HALO), :] = y_low[pl.ds(m * HALO, HALO), :]
        dst[X0 - HALO + m, pl.ds(Y0 + BY, HALO), :] = y_high[pl.ds(m * HALO, HALO), :]


def first_kernel(where, *refs):
    ins, refs = refs[:10], refs[10:]
    (f_lo, f_hi, v_lo, v_hi, send, f1_out, f1_up, f1_down), (r_lo, r_hi, f1, v1, r1) = refs[:8], refs[8:]
    core = where()[2]
    lay_out_0(f_lo, *ins[0:5])
    lay_out_0(f_hi, *ins[5:10])
    force, v, r = (f_lo, f_hi), (v_lo, v_hi), (r_lo, r_hi)
    sweep_0(v, force, None, 9, first=True)
    residual_0(r, v, force, 8)
    restrict_0(f1, r, 4)
    coarse_source(send, f1, v1, r1, core)
    put_out_1(f1_out, f1_up, f1_down, f1, 4, 4)


def middle_kernel(where, *refs):
    f_lo, f_hi, v_lo, v_hi, f1_in, x_low, x_high, y_low, y_high, mine, other = refs[:11]
    n_lo, n_hi, send, f1_out, f1_up, f1_down = refs[11:17]
    a_lo, a_hi, b_lo, b_hi, f1, v1, r1, p1, y2, p0, f2, v2, t2, t3, s3, p2, a2, b2, near = refs[17:]
    gx, gy, core = where()
    force, v, a0, b0 = (f_lo, f_hi), (v_lo, v_hi), (a_lo, a_hi), (b_lo, b_hi)
    unpack_2(f2, mine, other, core)
    level_2(near, f2, v2, t2, t3, s3, p2, a2, b2, gx, 4)
    lay_out_1(f1, f1_in, x_low, x_high, y_low, y_high, 4, 4)
    sweep_1(v1, f1, None, 7, first=True)
    add_from_2(v1, near, y2, p1, gy, 4)
    sweep_1(r1, v1, f1, 6)
    sweep_1(v1, r1, f1, 5)
    add_from_1(a0, v, v1, p0, 5, (X0, Y0, (Y0 - 16, 64)))
    sweep_0(b0, a0, force, 8)
    sweep_0(a0, b0, force, 7)
    sweep_0(b0, a0, force, 6)
    sweep_0(a0, b0, force, 5)
    residual_0(b0, a0, force, 4)
    restrict_0(f1, b0, 2)
    coarse_source(send, f1, v1, r1, core)
    put_out_1(f1_out, f1_up, f1_down, f1, 2, 2)
    for src, dst in ((a_lo, n_lo), (a_hi, n_hi)):
        dst[...] = src[pl.ds(X0 - 2, 20), pl.ds(Y0 - 8, 48), :]


def last_kernel(where, *refs):
    f_lo, f_hi, n_lo, n_hi, f1_in, x_low, x_high, y_low, y_high, mine, other, out = refs[:12]
    a_lo, a_hi, b_lo, b_hi, f1, v1, r1, p1, y2, p0, f2, v2, t2, t3, s3, p2, a2, b2, near = refs[12:]
    gx, gy, core = where()
    force, v, a0, b0 = (f_lo, f_hi), (n_lo, n_hi), (a_lo, a_hi), (b_lo, b_hi)
    unpack_2(f2, mine, other, core)
    level_2(near, f2, v2, t2, t3, s3, p2, a2, b2, gx, 2)
    lay_out_1(f1, f1_in, x_low, x_high, y_low, y_high, 2, 2)
    sweep_1(v1, f1, None, 3, first=True)
    add_from_2(v1, near, y2, p1, gy, 2)
    sweep_1(r1, v1, f1, 2)
    sweep_1(v1, r1, f1, 1)
    add_from_1(a0, v, v1, p0, 1, (2, 8, (0, 48)))
    sweep_0(b0, a0, force, 1)
    a, d, k = coefficients(0)

    def body(i):
        for j in range(Y0, Y0 + BY, 16):
            centre, nb = beside_0(b0, i, j, 16)
            f = f_lo[i, pl.ds(j, 16), :]
            out[i - X0, pl.ds(j - Y0, 16), :] = (1.0 - OMEGA) * centre[0] + k * f + k * a * nb[0]

    over_layers(X0, BX, 4, body)


def vm(*shape):
    return pltpu.VMEM(shape, F32)


def kept(*shape):
    return jax.ShapeDtypeStruct(shape, F32)


SCRATCH = (
    [vm(XA0, YA0, LANES)] * 4
    + [vm(XA1, YA1, LANES)] * 3
    + [vm(12, 32, LANES), vm(12, 64, LANES), vm(4, 64, LANES)]
    + [vm(64, 32, LANES)] * 2
    + [vm(32, 32, LANES), vm(16, 16, LANES), vm(32, 16, LANES), vm(8, 32, LANES)]
    + [vm(16, 32, LANES)] * 2
    + [vm(12, 32, LANES)]
)


def run(kernel, outs, scratch, flops, *args):
    return pl.pallas_call(
        kernel,
        out_shape=outs,
        scratch_shapes=scratch,
        compiler_params=pltpu.CompilerParams(vmem_limit_bytes=40 * 2**20),
        cost_estimate=pl.CostEstimate(flops=flops, bytes_accessed=2**20, transcendentals=0),
    )(*args)


def where_am_i():
    return lax.axis_index("gx"), lax.axis_index("gy"), lax.axis_index("gz")


def edges(*args):
    return run(edges_kernel, [kept(360, LANES)] * 2, [], 10**6, *args)


def first(where, *args):
    outs = [kept(XA0, YA0, LANES)] * 4 + [kept(64, 8, LANES), kept(16, 24, LANES)] + [kept(64, LANES)] * 2
    scratch = [vm(XA0, YA0, LANES)] * 2 + [vm(XA1, YA1, LANES)] * 3
    return run(functools.partial(first_kernel, where), outs, scratch, 10**7, *args)


def middle(where, *args):
    outs = [kept(20, 48, LANES)] * 2 + [kept(64, 8, LANES), kept(12, 24, LANES)] + [kept(24, LANES)] * 2
    return run(functools.partial(middle_kernel, where), outs, SCRATCH, 4 * 10**7, *args)


def last(where, *args):
    return run(functools.partial(last_kernel, where), kept(BX, BY, LANES), SCRATCH, 2 * 10**7, *args)


def from_(value, axis, step):
    size = lax.axis_size(axis)
    return lax.ppermute(value, axis, [(i, (i + step) % size) for i in range(size)])


def gather(send):
    mine = lax.all_to_all(send, ("gx", "gy"), 0, 0, tiled=True)
    return mine, from_(mine, "gz", 1)


def local(charge):
    x_low = from_(charge[BX - HALO :], "gx", 1)
    x_high = from_(charge[:HALO], "gx", -1)
    up, down = edges(charge, x_low, x_high)
    y_low, y_high = from_(up, "gy", 1), from_(down, "gy", -1)
    ours = (charge, x_low, x_high, y_low, y_high)
    others = [from_(v, "gz", 1) for v in ours]

    f_lo, f_hi, v_lo, v_hi, send, f1, f1_up, f1_down = first(where_am_i, *ours, *others)
    beside = (
        from_(f1[4:8], "gx", 1),
        from_(f1[8:12], "gx", -1),
        from_(f1_up, "gy", 1),
        from_(f1_down, "gy", -1),
    )
    n_lo, n_hi, send, f1, f1_up, f1_down = middle(where_am_i, f_lo, f_hi, v_lo, v_hi, f1, *beside, *gather(send))
    beside = (
        from_(f1[6:8], "gx", 1),
        from_(f1[4:6], "gx", -1),
        from_(f1_up, "gy", 1),
        from_(f1_down, "gy", -1),
    )
    return last(where_am_i, f_lo, f_hi, n_lo, n_hi, f1, *beside, *gather(send))


def solution(mesh):
    return jax.shard_map(
        local,
        mesh=mesh,
        in_specs=(P(("groups", "gx"), "gy", "gz"),),
        out_specs=P(("groups", "gx"), "gy", "gz"),
        check_vma=False,
    )
```

```python
import functools

import jax
import jax.numpy as jnp
from jax import lax
from jax.experimental import pallas as pl
from jax.experimental.pallas import tpu as pltpu
from jax.sharding import PartitionSpec as P

LANES = 128
OMEGA = 2.0 / 3.0
SCREEN = 0.001
F32 = jnp.float32

BX, BY = 16, 32
X0, Y0, XA0, YA0 = 12, 24, 40, 80
X1, Y1, XA1, YA1 = 10, 16, 32, 48
HALO = 10


def coefficients(level):
    a = 0.25**level
    return a, OMEGA / (6.0 * a + SCREEN)


def residual_of(level, f, v, nb):
    a, _ = coefficients(level)
    apart = 6.0 * v - nb
    if level:
        apart = a * apart
    return (f - apart) - SCREEN * v


def relaxed(level, f, v, nb):
    return v + coefficients(level)[1] * residual_of(level, f, v, nb)


def twice_from_zero(level, f, nb):
    a, k = coefficients(level)
    return (2.0 * k - k * k * SCREEN) * f - (k * k * a) * (6.0 * f - nb)


def iota(shape, dim):
    return lax.broadcasted_iota(jnp.int32, shape, dim)


def parts(v):
    high = v.astype(jnp.bfloat16)
    rest = v - high.astype(F32)
    middle = rest.astype(jnp.bfloat16)
    return high, middle, (rest - middle.astype(F32)).astype(jnp.bfloat16)


def product(a, b):
    return lax.dot_general(a, b, (((1,), (0,)), ((), ())), preferred_element_type=F32)


def dot(a, b):
    b = b.astype(jnp.bfloat16)
    high, middle, low = (product(p, b) for p in parts(a))
    return high + (middle + low)


def dot_rows(a, b):
    a = a.astype(jnp.bfloat16)
    high, middle, low = (product(a, p) for p in parts(b))
    return high + (middle + low)


def over_layers(start, count, block, body):
    def step(b, carry):
        for u in range(block):
            body(start + b * block + u)
        return carry

    lax.fori_loop(0, -(-count // block), step, 0)


def beside_0(refs, i, j, rows):
    even, odd = (r[i, pl.ds(j, rows), :] for r in refs)
    along_z = odd + pltpu.roll(odd, 1, 1), even + pltpu.roll(even, LANES - 1, 1)
    out = []
    for r, z in zip(refs, along_z):
        out.append(
            (r[i - 1, pl.ds(j, rows), :] + r[i + 1, pl.ds(j, rows), :])
            + (r[i, pl.ds(j - 1, rows), :] + r[i, pl.ds(j + 1, rows), :])
            + z
        )
    return (even, odd), out


def sweep_0(dst, src, force, halo, block):
    def body(i):
        for j in range(Y0 - 8, Y0 + 40, 16):
            centre, nb = beside_0(src, i, j, 16)
            for h in range(2):
                dst[h][i, pl.ds(j, 16), :] = relaxed(0, force[h][i, pl.ds(j, 16), :], centre[h], nb[h])

    over_layers(X0 - halo, BX + 2 * halo, block, body)


def start_0(dst, force, halo, block):
    def body(i):
        for j in range(Y0 - 16, Y0 + 48, 16):
            centre, nb = beside_0(force, i, j, 16)
            for h in range(2):
                dst[h][i, pl.ds(j, 16), :] = twice_from_zero(0, centre[h], nb[h])

    over_layers(X0 - halo, BX + 2 * halo, block, body)


def restrict_0(f1, t0, v, force, halo):
    def body(q):
        for j in range(Y0 - 8, Y0 + 40, 16):
            total = None
            for i in (X0 - 2 * halo + 2 * q, X0 - 2 * halo + 2 * q + 1):
                centre, nb = beside_0(v, i, j, 16)
                for h in range(2):
                    r = residual_of(0, force[h][i, pl.ds(j, 16), :], centre[h], nb[h])
                    total = r if total is None else total + r
            t0[q, pl.ds(j - Y0 + 8, 16), :] = total

    layers = BX // 2 + 2 * halo
    over_layers(0, layers, 4, body)
    for m in range(layers):
        f1[X1 - halo + m, pl.ds(Y1 - 4, 24), :] = 0.125 * (t0[m, pl.ds(0, 24, stride=2), :] + t0[m, pl.ds(1, 24, stride=2), :])


def mean_matrix(source_of_out):
    source, out = iota((LANES, LANES), 0), source_of_out(iota((LANES, LANES), 1))
    return jnp.where((source == out) | (source == out + 1), 0.125, 0.0).astype(F32)


def pick_matrix(source_of_out):
    return jnp.where(iota((LANES, LANES), 0) == source_of_out(iota((LANES, LANES), 1)), 1.0, 0.0).astype(F32)


def beside_1(ref, i, j, rows):
    centre = ref[i, pl.ds(j, rows), :]
    nb = (
        (ref[i - 1, pl.ds(j, rows), :] + ref[i + 1, pl.ds(j, rows), :])
        + (ref[i, pl.ds(j - 1, rows), :] + ref[i, pl.ds(j + 1, rows), :])
        + (pltpu.roll(centre, 1, 1) + pltpu.roll(centre, LANES - 1, 1))
    )
    return centre, nb


def sweep_1(dst, src, force, halo, block):
    def body(i):
        centre, nb = beside_1(src, i, Y1 - 8, 32)
        dst[i, pl.ds(Y1 - 8, 32), :] = relaxed(1, force[i, pl.ds(Y1 - 8, 32), :], centre, nb)

    over_layers(X1 - halo, BX // 2 + 2 * halo, block, body)


def start_1(dst, force, halo, block):
    def body(i):
        centre, nb = beside_1(force, i, Y1 - 8, 32)
        dst[i, pl.ds(Y1 - 8, 32), :] = twice_from_zero(1, centre, nb)

    over_layers(X1 - halo, BX // 2 + 2 * halo, block, body)


def sizes_2():
    return lax.axis_size("gx") * BX // 4, lax.axis_size("gy") * BY // 4, lax.axis_size("gz") * LANES // 4


def coarse_source(out, f1, v1, r1, core):
    start_1(v1, f1, 1, 10)

    def body(i):
        centre, nb = beside_1(v1, i, Y1, 16)
        r1[i, pl.ds(Y1, 16), :] = residual_of(1, f1[i, pl.ds(Y1, 16), :], centre, nb)

    over_layers(X1, BX // 2, 8, body)
    layers = []
    for q in range(4):
        i = X1 + 2 * q
        s = (r1[i, pl.ds(Y1, 8, stride=2), :] + r1[i, pl.ds(Y1 + 1, 8, stride=2), :]) + (
            r1[i + 1, pl.ds(Y1, 8, stride=2), :] + r1[i + 1, pl.ds(Y1 + 1, 8, stride=2), :]
        )
        layers.append(jnp.where(core == 0, s[0:4], s[4:8]))
    n = sizes_2()[2]
    at = lambda o: 2 * lax.rem(o + n // 2 * core, n)
    low = mean_matrix(lambda o: jnp.where(o < n, at(o), -2))
    high = mean_matrix(lambda o: jnp.where(o >= n, at(o), -2))
    packed = dot(jnp.concatenate(layers[0:2], axis=0), low) + dot(jnp.concatenate(layers[2:4], axis=0), high)
    for s in range(out.shape[0]):
        out[s] = packed


def beside_whole(v):
    n = v.shape[0]
    up = jnp.concatenate([v[n - 1 :], v[: n - 1]], axis=0)
    down = jnp.concatenate([v[1:], v[:1]], axis=0)
    y = pltpu.roll(v, 1, 1) + pltpu.roll(v, v.shape[1] - 1, 1)
    return (up + down) + y + (pltpu.roll(v, 1, 2) + pltpu.roll(v, LANES - 1, 2))


def from_zero(level, f):
    return twice_from_zero(level, f, beside_whole(f))


def residual_whole(level, f, v):
    return residual_of(level, f, v, beside_whole(v))


def smooth_whole(level, f, v):
    for _ in range(2):
        v = relaxed(level, f, v, beside_whole(v))
    return v


def down_z(level):
    n = sizes_2()[2] >> (level - 1)
    return mean_matrix(lambda o: 2 * lax.rem(o, n))


def up_z(level):
    n = sizes_2()[2] >> (level - 2)
    return pick_matrix(lambda o: lax.div(lax.rem(o, n), 2))


def pair_layers(v):
    v = v.reshape(v.shape[0] // 2, 2, *v.shape[1:])
    return v[:, 0] + v[:, 1]


def twice(v):
    return jnp.concatenate([v[:, None], v[:, None]], axis=1).reshape(2 * v.shape[0], *v.shape[1:])


def flat(v):
    return v.reshape(-1, LANES)


def row_sums(size, y_size):
    out, source = iota((size, size), 0), iota((size, size), 1)
    first = (out // 8) * 8 + 2 * lax.rem(lax.rem(out, 8), y_size)
    return jnp.where((source == first) | (source == first + 1), 1.0, 0.0).astype(F32)


def row_picks(size, y_size):
    out, source = iota((size, size), 0), iota((size, size), 1)
    first = (out // 8) * 8 + lax.div(lax.rem(lax.rem(out, 8), y_size), 2)
    return jnp.where(source == first, 1.0, 0.0).astype(F32)


def solve_3(f3, t3):
    x4, y4 = f3.shape[0] // 2, f3.shape[1] // 2
    v3 = from_zero(3, f3)
    t3[...] = pair_layers(residual_whole(3, f3, v3))
    s = t3[:, pl.ds(0, y4, stride=2), :] + t3[:, pl.ds(1, y4, stride=2), :]
    f4 = dot(flat(s), down_z(3)).reshape(x4, y4, LANES)
    v4 = from_zero(4, f4)
    s = flat(pair_layers(residual_whole(4, f4, v4)))
    f5 = dot_rows(row_sums(s.shape[0], y4 // 2), dot(s, down_z(4))).reshape(x4 // 2, 8, LANES)
    v5 = from_zero(5, f5)
    s = flat(pair_layers(residual_whole(5, f5, v5)))
    f6 = dot_rows(row_sums(s.shape[0], y4 // 4), dot(s, down_z(5))).reshape(x4 // 4, 8, LANES)
    v6 = flat(from_zero(6, f6))
    e5 = dot_rows(row_picks(v6.shape[0], y4 // 2), dot(v6, up_z(5))).reshape(x4 // 4, 8, LANES)
    v5 = flat(smooth_whole(5, f5, v5 + twice(e5)))
    e4 = dot_rows(row_picks(v5.shape[0], y4), dot(v5, up_z(4))).reshape(x4 // 2, 8, LANES)
    v4 = smooth_whole(4, f4, v4 + twice(e4))
    e3 = dot(flat(v4), up_z(3)).reshape(x4, y4, LANES)
    t3[:, pl.ds(0, y4, stride=2), :] = e3
    t3[:, pl.ds(1, y4, stride=2), :] = e3
    return smooth_whole(3, f3, v3 + twice(t3[...]))


def unpack_2(f2, mine, other, core):
    low = iota((8, LANES), 1) < 64
    top = iota((8, LANES), 0) < 4
    along_y = lax.axis_size("gy")

    def body(gx):
        for gy in range(along_y):
            t, p = mine[gx * along_y + gy], other[gx * along_y + gy]
            u, w = jnp.where(core == 0, t, p), jnp.where(core == 0, p, t)
            ur, wr = pltpu.roll(u, 64, 1), pltpu.roll(w, 64, 1)
            for xp in range(2):
                d = jnp.where(low, u, ur) if xp == 0 else jnp.where(low, ur, u)
                e = jnp.where(low, w, wr) if xp == 0 else jnp.where(low, wr, w)
                f2[gx * 4 + 2 * xp, pl.ds(gy * 8, 8), :] = jnp.where(top, d, pltpu.roll(e, 4, 0))
                f2[gx * 4 + 2 * xp + 1, pl.ds(gy * 8, 8), :] = jnp.where(top, pltpu.roll(d, 4, 0), e)

    over_layers(0, f2.shape[0] // 4, 4, body)


def beside_2(centre, before, after):
    rows = centre.shape[0]
    return (
        (before + after)
        + (pltpu.roll(centre, 1, 0) + pltpu.roll(centre, rows - 1, 0))
        + (pltpu.roll(centre, 1, 1) + pltpu.roll(centre, LANES - 1, 1))
    )


def level_2(near, f2, v2, t2, t3, s3, p2, a2, b2, gx, halo):
    n, rows = f2.shape[0], f2.shape[1]

    def around(ref, i):
        return ref[i], ref[lax.rem(i + n - 1, n)], ref[lax.rem(i + 1, n)]

    def first(i):
        centre, before, after = around(f2, i)
        v2[i] = twice_from_zero(2, centre, beside_2(centre, before, after))

    over_layers(0, n, 16, first)

    def second(q):
        pair = []
        for i in (2 * q, 2 * q + 1):
            centre, before, after = around(v2, i)
            pair.append(residual_of(2, f2[i], centre, beside_2(centre, before, after)))
        t2[q] = pair[0] + pair[1]

    over_layers(0, n // 2, 8, second)
    s = t2[:, pl.ds(0, rows // 2, stride=2), :] + t2[:, pl.ds(1, rows // 2, stride=2), :]
    f3 = dot(flat(s), down_z(2)).reshape(n // 2, rows // 2, LANES)
    s3[...] = solve_3(f3, t3)

    count = 4 + 2 * halo + 4
    start = gx * 4 - halo - 2 + n
    e = jnp.concatenate([s3[lax.rem(lax.div(start, 2) + m, n // 2)] for m in range(count // 2)], axis=0)
    e = dot(e, up_z(2)).reshape(count // 2, rows // 2, LANES)
    p2[pl.ds(0, count // 2), pl.ds(0, rows // 2, stride=2), :] = e
    p2[pl.ds(0, count // 2), pl.ds(1, rows // 2, stride=2), :] = e
    for m in range(count):
        a2[m] = v2[lax.rem(start + m, n)] + p2[m // 2]
    for m in range(1, count - 1):
        nb = beside_2(a2[m], a2[m - 1], a2[m + 1])
        b2[m] = relaxed(2, f2[lax.rem(start + m, n)], a2[m], nb)
    for m in range(2, count - 2):
        nb = beside_2(b2[m], b2[m - 1], b2[m + 1])
        near[m - 2] = relaxed(2, f2[lax.rem(start + m, n)], b2[m], nb)


def add_from_2(v1, near, y2, p1, gy, core, halo):
    layers = 4 + 2 * halo
    rows, n = sizes_2()[1:]
    for m in range(layers):
        y2[m, pl.ds(0, rows), :] = near[m]
        y2[m, pl.ds(rows, rows), :] = near[m]
    start = pl.multiple_of(lax.rem(gy * 8 + rows - 4, rows), 4)
    picked = jnp.concatenate([y2[m, pl.ds(start, 16), :] for m in range(layers)], axis=0)
    e = dot(picked, pick_matrix(lambda o: lax.rem(lax.div(o, 2) + n // 2 * core, n))).reshape(layers, 16, LANES)
    p1[pl.ds(0, layers), pl.ds(0, 16, stride=2), :] = e
    p1[pl.ds(0, layers), pl.ds(1, 16, stride=2), :] = e
    for m in range(2 * layers):
        i = X1 - 2 * halo + m
        v1[i, pl.ds(Y1 - 8, 32), :] = v1[i, pl.ds(Y1 - 8, 32), :] + p1[m // 2]


def add_from_1(w, v, v1, p0, halo, x_at, y_from, skip, rows):
    for m in range(BX // 2 + 2 * halo):
        e = v1[X1 - halo + m, pl.ds(Y1 - 8, 32), :]
        p0[m, pl.ds(0, 32, stride=2), :] = e
        p0[m, pl.ds(1, 32, stride=2), :] = e
    for x in range(-2 * halo, BX + 2 * halo):
        for h in range(2):
            w[h][X0 + x, pl.ds(Y0 - skip, rows), :] = (
                v[h][x_at + x, pl.ds(y_from, rows), :] + p0[x // 2 + halo, pl.ds(16 - skip, rows), :]
            )


def lay_out_1(dst, f1, x_low, x_high, y_low, y_high, own, width):
    count = f1.shape[0]
    for m in range(count):
        i = X1 - own + m
        dst[i, pl.ds(Y1 - 4, 24), :] = f1[m]
        dst[i, pl.ds(Y1 - own - width, width), :] = y_low[pl.ds(m * width, width), :]
        dst[i, pl.ds(Y1 + 16 + own, width), :] = y_high[pl.ds(m * width, width), :]
    for m in range(width):
        dst[X1 - own - width + m, pl.ds(Y1 - 4, 24), :] = x_low[m]
        dst[X1 + 8 + own + m, pl.ds(Y1 - 4, 24), :] = x_high[m]


def put_out_1(out, up_x, down_x, up_y, down_y, f1, own, width):
    for m in range(out.shape[0]):
        i = X1 - own + m
        out[m] = f1[i, pl.ds(Y1 - 4, 24), :]
        up_y[pl.ds(m * width, width), :] = f1[i, pl.ds(Y1 + 16 - own - width, width), :]
        down_y[pl.ds(m * width, width), :] = f1[i, pl.ds(Y1 + own, width), :]
    for m in range(width):
        up_x[m] = f1[X1 + 8 - own - width + m, pl.ds(Y1 - 4, 24), :]
        down_x[m] = f1[X1 + own + m, pl.ds(Y1 - 4, 24), :]


def split_kernel(charge, mine, up, down):
    matrix = pick_matrix(lambda o: jnp.where(o < 64, 2 * o, 2 * o - 127))
    split = dot(flat(charge[...]), matrix).reshape(BX, BY, LANES)
    mine[...] = split
    up[...] = split[BX - HALO :]
    down[...] = split[:HALO]


def edges_kernel(mine, x_low, x_high, up, down):
    at = 0
    for ref in (x_low, mine, x_high):
        for i in range(ref.shape[0]):
            down[pl.ds(at * HALO, HALO), :] = ref[i, pl.ds(0, HALO), :]
            up[pl.ds(at * HALO, HALO), :] = ref[i, pl.ds(BY - HALO, HALO), :]
            at += 1


def lay_out_0(even, odd, ours, others):
    def both(p, q):
        low = iota(p.shape, p.ndim - 1) < 64
        return (
            jnp.where(low, p, pltpu.roll(q, 64, p.ndim - 1)),
            jnp.where(low, pltpu.roll(p, 64, p.ndim - 1), q),
        )

    at = X0 - HALO
    for k in (1, 0, 2):
        for m in range(ours[k].shape[0]):
            e, o = both(ours[k][m], others[k][m])
            even[at, pl.ds(Y0, BY), :] = e
            odd[at, pl.ds(Y0, BY), :] = o
            at += 1
    for k, row in ((3, Y0 - HALO), (4, Y0 + BY)):
        e, o = both(ours[k][...], others[k][...])
        for m in range(BX + 2 * HALO):
            even[X0 - HALO + m, pl.ds(row, HALO), :] = e[m * HALO : (m + 1) * HALO]
            odd[X0 - HALO + m, pl.ds(row, HALO), :] = o[m * HALO : (m + 1) * HALO]


def first_kernel(where, *refs):
    ours, others, refs = refs[0:5], refs[5:10], refs[10:]
    (f_e, f_o, v_e, v_o, send), f1_outs, (f1, v1, r1, t0) = refs[:5], refs[5:10], refs[10:]
    force, v = (f_e, f_o), (v_e, v_o)
    lay_out_0(f_e, f_o, ours, others)
    start_0(v, force, 9, 7)
    restrict_0(f1, t0, v, force, 4)
    coarse_source(send, f1, v1, r1, where()[2])
    put_out_1(*f1_outs, f1, 4, 4)


def middle_kernel(where, *refs):
    f_e, f_o, v_e, v_o, f1_in, x_low, x_high, y_low, y_high, mine, other = refs[:11]
    (n_e, n_o, send), f1_outs = refs[11:14], refs[14:19]
    a_e, a_o, b_e, b_o, f1, v1, r1, p1, y2, p0, t0, f2, v2, t2, t3, s3, p2, a2, b2, near = refs[19:]
    gx, gy, core = where()
    force, v, a0, b0 = (f_e, f_o), (v_e, v_o), (a_e, a_o), (b_e, b_o)
    unpack_2(f2, mine, other, core)
    level_2(near, f2, v2, t2, t3, s3, p2, a2, b2, gx, 4)
    lay_out_1(f1, f1_in, x_low, x_high, y_low, y_high, 4, 4)
    start_1(v1, f1, 7, 12)
    add_from_2(v1, near, y2, p1, gy, core, 4)
    sweep_1(r1, v1, f1, 6, 12)
    sweep_1(v1, r1, f1, 5, 9)
    add_from_1(a0, v, v1, p0, 5, X0, Y0 - 16, 16, 64)
    sweep_0(b0, a0, force, 8, 8)
    sweep_0(a0, b0, force, 7, 8)
    sweep_0(b0, a0, force, 6, 7)
    sweep_0(a0, b0, force, 5, 7)
    restrict_0(f1, t0, a0, force, 2)
    coarse_source(send, f1, v1, r1, core)
    put_out_1(*f1_outs, f1, 2, 2)
    for src, dst in ((a_e, n_e), (a_o, n_o)):
        dst[...] = src[pl.ds(X0 - 2, 20), pl.ds(Y0 - 8, 48), :]


def last_kernel(where, *refs):
    f_e, f_o, n_e, n_o, f1_in, x_low, x_high, y_low, y_high, mine, other, out = refs[:12]
    a_e, a_o, b_e, b_o, f1, v1, r1, p1, y2, p0, _, f2, v2, t2, t3, s3, p2, a2, b2, near = refs[12:]
    gx, gy, core = where()
    force, v, a0, b0 = (f_e, f_o), (n_e, n_o), (a_e, a_o), (b_e, b_o)
    unpack_2(f2, mine, other, core)
    level_2(near, f2, v2, t2, t3, s3, p2, a2, b2, gx, 2)
    lay_out_1(f1, f1_in, x_low, x_high, y_low, y_high, 2, 2)
    start_1(v1, f1, 3, 14)
    add_from_2(v1, near, y2, p1, gy, core, 2)
    sweep_1(r1, v1, f1, 2, 12)
    sweep_1(v1, r1, f1, 1, 10)
    add_from_1(a0, v, v1, p0, 1, 2, 0, 8, 48)
    sweep_0(b0, a0, force, 1, 6)
    low = iota((BY, LANES), 1) < 64

    def body(i):
        centre, nb = beside_0(b0, i, Y0, BY)
        even, odd = (relaxed(0, force[h][i, pl.ds(Y0, BY), :], centre[h], nb[h]) for h in range(2))
        p0[i - X0, pl.ds(0, BY), :] = jnp.where(low, even, pltpu.roll(odd, 64, 1))

    over_layers(X0, BX, 8, body)
    matrix = pick_matrix(lambda o: lax.div(o, 2) + 64 * lax.rem(o, 2))
    out[...] = dot(flat(p0[pl.ds(0, BX), pl.ds(0, BY), :]), matrix).reshape(BX, BY, LANES)


def vm(*shape):
    return pltpu.VMEM(shape, F32)


def kept(*shape):
    return jax.ShapeDtypeStruct(shape, F32)


def scratch_for_cycle():
    x2, y2, _ = sizes_2()
    return (
        [vm(XA0, YA0, LANES)] * 4
        + [vm(XA1, YA1, LANES)] * 3
        + [vm(12, y2, LANES), vm(12, 2 * y2, LANES), vm(20, 64, LANES), vm(16, 48, LANES)]
        + [vm(x2, y2, LANES)] * 2
        + [vm(x2 // 2, y2, LANES), vm(x2 // 4, y2 // 2, LANES), vm(x2 // 2, y2 // 2, LANES), vm(8, y2, LANES)]
        + [vm(16, y2, LANES)] * 2
        + [vm(12, y2, LANES)]
    )


def run(kernel, outs, scratch, flops, *args):
    return pl.pallas_call(
        kernel,
        out_shape=outs,
        scratch_shapes=scratch,
        compiler_params=pltpu.CompilerParams(vmem_limit_bytes=40 * 2**20),
        cost_estimate=pl.CostEstimate(flops=flops, bytes_accessed=2**20, transcendentals=0),
    )(*args)


def where_am_i():
    return lax.axis_index("gx"), lax.axis_index("gy"), lax.axis_index("gz")


def sources_out(layers, width):
    y = kept(layers * width, LANES)
    return [kept(peers(), 8, LANES), kept(layers, 24, LANES)] + [kept(width, 24, LANES)] * 2 + [y] * 2


def peers():
    return lax.axis_size("gx") * lax.axis_size("gy")


def split(charge):
    return run(split_kernel, [kept(BX, BY, LANES)] + [kept(HALO, BY, LANES)] * 2, [], 10**6, charge)


def edges(*args):
    return run(edges_kernel, [kept((BX + 2 * HALO) * HALO, LANES)] * 2, [], 10**6, *args)


def first(*args):
    outs = [kept(XA0, YA0, LANES)] * 4 + sources_out(16, 4)
    scratch = [vm(XA1, YA1, LANES)] * 3 + [vm(16, 48, LANES)]
    return run(functools.partial(first_kernel, where_am_i), outs, scratch, 10**7, *args)


def middle(*args):
    outs = [kept(20, 48, LANES)] * 2 + sources_out(12, 2)
    return run(functools.partial(middle_kernel, where_am_i), outs, scratch_for_cycle(), 4 * 10**7, *args)


def last(*args):
    outs = kept(BX, BY, LANES)
    return run(functools.partial(last_kernel, where_am_i), outs, scratch_for_cycle(), 2 * 10**7, *args)


def from_(value, axis, step):
    size = lax.axis_size(axis)
    return lax.ppermute(value, axis, [(i, (i + step) % size) for i in range(size)])


def exchange(send, f1, up_x, down_x, up_y, down_y):
    x_low, x_high = from_(up_x, "gx", 1), from_(down_x, "gx", -1)
    y_low, y_high = from_(up_y, "gy", 1), from_(down_y, "gy", -1)
    mine = lax.all_to_all(send, ("gx", "gy"), 0, 0, tiled=True)
    return f1, x_low, x_high, y_low, y_high, mine, from_(mine, "gz", 1)


def local(charge):
    mine, up, down = split(charge)
    x_low, x_high = from_(up, "gx", 1), from_(down, "gx", -1)
    up, down = edges(mine, x_low, x_high)
    y_low, y_high = from_(up, "gy", 1), from_(down, "gy", -1)
    ours = (mine, x_low, x_high, y_low, y_high)
    others = [from_(v, "gz", 1) for v in ours]
    f_e, f_o, v_e, v_o, *rest = first(*ours, *others)
    n_e, n_o, *rest = middle(f_e, f_o, v_e, v_o, *exchange(*rest))
    return last(f_e, f_o, n_e, n_o, *exchange(*rest))


def solution(mesh):
    return jax.shard_map(
        local,
        mesh=mesh,
        in_specs=(P(("groups", "gx"), "gy", "gz"),),
        out_specs=P(("groups", "gx"), "gy", "gz"),
        check_vma=False,
    )
```

```python
import functools

import jax
import jax.numpy as jnp
import numpy as np
from jax import lax
from jax.experimental import pallas as pl
from jax.experimental.pallas import tpu as pltpu
from jax.sharding import PartitionSpec as P

LEVELS = 7
LANES = 128
OMEGA = 2.0 / 3.0
SCREEN = 0.001
F32 = jnp.float32

BX, BY = 16, 32
X0, Y0, XA0, YA0 = 12, 24, 40, 80
X1, Y1, XA1, YA1 = 10, 16, 32, 48
HALO = 10


def coefficients(level):
    a = 0.25**level
    return a, OMEGA / (6.0 * a + SCREEN)


def residual_of(level, f, v, nb):
    a, _ = coefficients(level)
    apart = 6.0 * v - nb
    if level:
        apart = a * apart
    return (f - apart) - SCREEN * v


def relaxed(level, f, v, nb):
    return v + coefficients(level)[1] * residual_of(level, f, v, nb)


def twice_from_zero(level, f, nb):
    a, k = coefficients(level)
    return (2.0 * k - k * k * SCREEN) * f - (k * k * a) * (6.0 * f - nb)


def iota(shape, dim):
    return lax.broadcasted_iota(jnp.int32, shape, dim)


def parts(v):
    high = v.astype(jnp.bfloat16)
    rest = v - high.astype(F32)
    middle = rest.astype(jnp.bfloat16)
    return high, middle, (rest - middle.astype(F32)).astype(jnp.bfloat16)


def product(a, b):
    return lax.dot_general(a, b, (((1,), (0,)), ((), ())), preferred_element_type=F32)


def dot(a, b):
    b = b.astype(jnp.bfloat16)
    high, middle, low = (product(p, b) for p in parts(a))
    return high + (middle + low)


def over_layers(start, count, block, body):
    def step(b, carry):
        for u in range(block):
            body(start + b * block + u)
        return carry

    lax.fori_loop(0, -(-count // block), step, 0)


def beside_0(refs, i, j, rows):
    even, odd = (r[i, pl.ds(j, rows), :] for r in refs)
    along_z = odd + pltpu.roll(odd, 1, 1), even + pltpu.roll(even, LANES - 1, 1)
    out = []
    for r, z in zip(refs, along_z):
        out.append(
            (r[i - 1, pl.ds(j, rows), :] + r[i + 1, pl.ds(j, rows), :])
            + (r[i, pl.ds(j - 1, rows), :] + r[i, pl.ds(j + 1, rows), :])
            + z
        )
    return (even, odd), out


def sweep_0(dst, src, force, halo, block):
    def body(i):
        for j in range(Y0 - 8, Y0 + 40, 16):
            centre, nb = beside_0(src, i, j, 16)
            for h in range(2):
                dst[h][i, pl.ds(j, 16), :] = relaxed(0, force[h][i, pl.ds(j, 16), :], centre[h], nb[h])

    over_layers(X0 - halo, BX + 2 * halo, block, body)


def start_0(dst, force, halo, block):
    def body(i):
        for j in range(Y0 - 16, Y0 + 48, 16):
            centre, nb = beside_0(force, i, j, 16)
            for h in range(2):
                dst[h][i, pl.ds(j, 16), :] = twice_from_zero(0, centre[h], nb[h])

    over_layers(X0 - halo, BX + 2 * halo, block, body)


def restrict_0(f1, t0, v, force, halo):
    def body(q):
        for j in range(Y0 - 8, Y0 + 40, 16):
            total = None
            for i in (X0 - 2 * halo + 2 * q, X0 - 2 * halo + 2 * q + 1):
                centre, nb = beside_0(v, i, j, 16)
                for h in range(2):
                    r = residual_of(0, force[h][i, pl.ds(j, 16), :], centre[h], nb[h])
                    total = r if total is None else total + r
            t0[q, pl.ds(j - Y0 + 8, 16), :] = total

    layers = BX // 2 + 2 * halo
    over_layers(0, layers, 4, body)
    for m in range(layers):
        f1[X1 - halo + m, pl.ds(Y1 - 4, 24), :] = 0.125 * (t0[m, pl.ds(0, 24, stride=2), :] + t0[m, pl.ds(1, 24, stride=2), :])


def mean_matrix(source_of_out):
    source, out = iota((LANES, LANES), 0), source_of_out(iota((LANES, LANES), 1))
    return jnp.where((source == out) | (source == out + 1), 0.125, 0.0).astype(F32)


def pick_matrix(source_of_out):
    return jnp.where(iota((LANES, LANES), 0) == source_of_out(iota((LANES, LANES), 1)), 1.0, 0.0).astype(F32)


def beside_1(ref, i, j, rows):
    centre = ref[i, pl.ds(j, rows), :]
    nb = (
        (ref[i - 1, pl.ds(j, rows), :] + ref[i + 1, pl.ds(j, rows), :])
        + (ref[i, pl.ds(j - 1, rows), :] + ref[i, pl.ds(j + 1, rows), :])
        + (pltpu.roll(centre, 1, 1) + pltpu.roll(centre, LANES - 1, 1))
    )
    return centre, nb


def sweep_1(dst, src, force, halo, block):
    def body(i):
        centre, nb = beside_1(src, i, Y1 - 8, 32)
        dst[i, pl.ds(Y1 - 8, 32), :] = relaxed(1, force[i, pl.ds(Y1 - 8, 32), :], centre, nb)

    over_layers(X1 - halo, BX // 2 + 2 * halo, block, body)


def start_1(dst, force, halo, block):
    def body(i):
        centre, nb = beside_1(force, i, Y1 - 8, 32)
        dst[i, pl.ds(Y1 - 8, 32), :] = twice_from_zero(1, centre, nb)

    over_layers(X1 - halo, BX // 2 + 2 * halo, block, body)


def sizes_2():
    return lax.axis_size("gx") * BX // 4, lax.axis_size("gy") * BY // 4, lax.axis_size("gz") * LANES // 4


def bottom_shape():
    return tuple(n // 8 for n in sizes_2())


def coarse_source(out, f1, v1, r1, core):
    start_1(v1, f1, 1, 10)

    def body(i):
        centre, nb = beside_1(v1, i, Y1, 16)
        r1[i, pl.ds(Y1, 16), :] = residual_of(1, f1[i, pl.ds(Y1, 16), :], centre, nb)

    over_layers(X1, BX // 2, 8, body)
    layers = []
    for q in range(4):
        i = X1 + 2 * q
        s = (r1[i, pl.ds(Y1, 8, stride=2), :] + r1[i, pl.ds(Y1 + 1, 8, stride=2), :]) + (
            r1[i + 1, pl.ds(Y1, 8, stride=2), :] + r1[i + 1, pl.ds(Y1 + 1, 8, stride=2), :]
        )
        layers.append(jnp.where(core == 0, s[0:4], s[4:8]))
    n = sizes_2()[2]
    at = lambda o: 2 * lax.rem(o + n // 2 * core, n)
    low = mean_matrix(lambda o: jnp.where(o < n, at(o), -2))
    high = mean_matrix(lambda o: jnp.where(o >= n, at(o), -2))
    packed = dot(jnp.concatenate(layers[0:2], axis=0), low) + dot(jnp.concatenate(layers[2:4], axis=0), high)
    for s in range(out.shape[0]):
        out[s] = packed


def across(v):
    n, rows = v.shape[0], v.shape[1]
    up = jnp.concatenate([v[n - 1 :], v[: n - 1]], axis=0)
    down = jnp.concatenate([v[1:], v[:1]], axis=0)
    return (up + down) + (pltpu.roll(v, 1, 1) + pltpu.roll(v, rows - 1, 1))


def applied(level, v):
    a, _ = coefficients(level)
    z1 = pltpu.roll(v, 1, 2) + pltpu.roll(v, LANES - 1, 2)
    z2 = pltpu.roll(v, 2, 2) + pltpu.roll(v, LANES - 2, 2)
    one = across(v)
    sv = one + z1
    ssv = across(one + 2.0 * z1) + (z2 + 2.0 * v)
    t = 6.0 * v - sv
    tt = 6.0 * t - (6.0 * sv - ssv)
    return t, a * t + SCREEN * v, (a * a) * tt + (2.0 * a * SCREEN) * t + (SCREEN * SCREEN) * v


def start_whole(level, f):
    a, k = coefficients(level)
    t, af, aaf = applied(level, f)
    return (2.0 * k - k * k * SCREEN) * f - (k * k * a) * t, f - 2.0 * k * af + (k * k) * aaf, af


def smooth_whole(level, f, af, v):
    a, k = coefficients(level)
    t, _, aav = applied(level, v)
    r = (f - a * t) - SCREEN * v
    return v + 2.0 * k * r - (k * k) * (af - aav)


def bottom_matrix(shape):
    def beside(v):
        return sum(np.roll(v, step, axis) for axis in (1, 2, 3) for step in (1, -1))

    def residual(level, f, v):
        return f - ((6.0 * v - beside(v)) * 0.25**level + SCREEN * v)

    def cycle(level, f):
        v = np.zeros_like(f)
        for _ in range(2):
            v = v + OMEGA * residual(level, f, v) / (6.0 * 0.25**level + SCREEN)
        if level == LEVELS - 1:
            return v
        n, x, y, z = f.shape
        coarse = residual(level, f, v).reshape(n, x // 2, 2, y // 2, 2, z // 2, 2).mean(axis=(2, 4, 6))
        v = v + cycle(level + 1, coarse).repeat(2, 1).repeat(2, 2).repeat(2, 3)
        for _ in range(2):
            v = v + OMEGA * residual(level, f, v) / (6.0 * 0.25**level + SCREEN)
        return v

    cells = shape[0] * shape[1] * shape[2]
    return cycle(5, np.eye(cells).reshape(cells, *shape)).reshape(cells, cells).astype(np.float32)


def down_z(level):
    n = sizes_2()[2] >> (level - 1)
    return mean_matrix(lambda o: 2 * lax.rem(o, n))


def up_z(level):
    n = sizes_2()[2] >> (level - 2)
    return pick_matrix(lambda o: lax.div(lax.rem(o, n), 2))


def pair_layers(v):
    v = v.reshape(v.shape[0] // 2, 2, *v.shape[1:])
    return v[:, 0] + v[:, 1]


def twice(v):
    return jnp.concatenate([v[:, None], v[:, None]], axis=1).reshape(2 * v.shape[0], *v.shape[1:])


def flat(v):
    return v.reshape(-1, LANES)


def solve_bottom(s, shape, matrix):
    x5, y5, z5 = shape
    cells = x5 * y5 * z5
    rows = s.shape[0]
    cell, row = iota((rows, cells), 1), iota((rows, cells), 0)
    mine = (cell // (y5 * z5) == row // (2 * y5)) & (lax.rem(cell // z5, y5) == lax.rem(row, 2 * y5) // 2)
    source, out = iota((LANES, cells), 0), lax.rem(iota((LANES, cells), 1), z5)
    means = jnp.where((source == 2 * out) | (source == 2 * out + 1), 0.125, 0.0).astype(F32)
    f5 = jnp.sum(jnp.where(mine, dot(s, means), 0.0), axis=0, keepdims=True)
    f_high, f_middle, f_low = parts(jnp.broadcast_to(f5, (8, cells)))
    m_high, m_middle, m_low = parts(matrix[...])
    v5 = product(f_high, m_high) + (
        (product(f_high, m_middle) + product(f_middle, m_high))
        + (product(f_high, m_low) + product(f_middle, m_middle) + product(f_low, m_high))
    )
    spread = jnp.where(mine, jnp.broadcast_to(v5[0:1], (rows, cells)), 0.0)
    source, out = lax.rem(iota((cells, LANES), 0), z5), lax.rem(iota((cells, LANES), 1), 2 * z5)
    return dot(spread, jnp.where(source == out // 2, 1.0, 0.0).astype(F32))


def solve_3(f3, t3, matrix):
    x4, y4 = f3.shape[0] // 2, f3.shape[1] // 2
    v3, r3, af3 = start_whole(3, f3)
    t3[...] = pair_layers(r3)
    s = t3[:, pl.ds(0, y4, stride=2), :] + t3[:, pl.ds(1, y4, stride=2), :]
    f4 = dot(flat(s), down_z(3)).reshape(x4, y4, LANES)
    v4, r4, af4 = start_whole(4, f4)
    e4 = solve_bottom(flat(pair_layers(r4)), bottom_shape(), matrix).reshape(x4 // 2, y4, LANES)
    v4 = smooth_whole(4, f4, af4, v4 + twice(e4))
    e3 = dot(flat(v4), up_z(3)).reshape(x4, y4, LANES)
    t3[:, pl.ds(0, y4, stride=2), :] = e3
    t3[:, pl.ds(1, y4, stride=2), :] = e3
    return smooth_whole(3, f3, af3, v3 + twice(t3[...]))


def unpack_2(f2, mine, other, core):
    low = iota((8, LANES), 1) < 64
    top = iota((8, LANES), 0) < 4
    along_y = lax.axis_size("gy")

    def body(gx):
        for gy in range(along_y):
            t, p = mine[gx * along_y + gy], other[gx * along_y + gy]
            u, w = jnp.where(core == 0, t, p), jnp.where(core == 0, p, t)
            ur, wr = pltpu.roll(u, 64, 1), pltpu.roll(w, 64, 1)
            for xp in range(2):
                d = jnp.where(low, u, ur) if xp == 0 else jnp.where(low, ur, u)
                e = jnp.where(low, w, wr) if xp == 0 else jnp.where(low, wr, w)
                f2[gx * 4 + 2 * xp, pl.ds(gy * 8, 8), :] = jnp.where(top, d, pltpu.roll(e, 4, 0))
                f2[gx * 4 + 2 * xp + 1, pl.ds(gy * 8, 8), :] = jnp.where(top, pltpu.roll(d, 4, 0), e)

    over_layers(0, f2.shape[0] // 4, 4, body)


def beside_2(centre, before, after):
    rows = centre.shape[0]
    return (
        (before + after)
        + (pltpu.roll(centre, 1, 0) + pltpu.roll(centre, rows - 1, 0))
        + (pltpu.roll(centre, 1, 1) + pltpu.roll(centre, LANES - 1, 1))
    )


def level_2(near, f2, v2, t2, t3, s3, p2, a2, b2, matrix, fetch, gx, halo):
    n, rows = f2.shape[0], f2.shape[1]

    def around(ref, i):
        return ref[i], ref[lax.rem(i + n - 1, n)], ref[lax.rem(i + 1, n)]

    def first(i):
        centre, before, after = around(f2, i)
        v2[i] = twice_from_zero(2, centre, beside_2(centre, before, after))

    over_layers(0, n, 16, first)

    def second(q):
        pair = []
        for i in (2 * q, 2 * q + 1):
            centre, before, after = around(v2, i)
            pair.append(residual_of(2, f2[i], centre, beside_2(centre, before, after)))
        t2[q] = pair[0] + pair[1]

    over_layers(0, n // 2, 8, second)
    s = t2[:, pl.ds(0, rows // 2, stride=2), :] + t2[:, pl.ds(1, rows // 2, stride=2), :]
    f3 = dot(flat(s), down_z(2)).reshape(n // 2, rows // 2, LANES)
    fetch.wait()
    s3[...] = solve_3(f3, t3, matrix)

    count = 4 + 2 * halo + 4
    start = gx * 4 - halo - 2 + n
    e = jnp.concatenate([s3[lax.rem(lax.div(start, 2) + m, n // 2)] for m in range(count // 2)], axis=0)
    e = dot(e, up_z(2)).reshape(count // 2, rows // 2, LANES)
    p2[pl.ds(0, count // 2), pl.ds(0, rows // 2, stride=2), :] = e
    p2[pl.ds(0, count // 2), pl.ds(1, rows // 2, stride=2), :] = e
    for m in range(count):
        a2[m] = v2[lax.rem(start + m, n)] + p2[m // 2]
    for m in range(1, count - 1):
        nb = beside_2(a2[m], a2[m - 1], a2[m + 1])
        b2[m] = relaxed(2, f2[lax.rem(start + m, n)], a2[m], nb)
    for m in range(2, count - 2):
        nb = beside_2(b2[m], b2[m - 1], b2[m + 1])
        near[m - 2] = relaxed(2, f2[lax.rem(start + m, n)], b2[m], nb)


def add_from_2(v1, near, y2, p1, gy, core, halo):
    layers = 4 + 2 * halo
    rows, n = sizes_2()[1:]
    for m in range(layers):
        y2[m, pl.ds(0, rows), :] = near[m]
        y2[m, pl.ds(rows, rows), :] = near[m]
    start = pl.multiple_of(lax.rem(gy * 8 + rows - 4, rows), 4)
    picked = jnp.concatenate([y2[m, pl.ds(start, 16), :] for m in range(layers)], axis=0)
    e = dot(picked, pick_matrix(lambda o: lax.rem(lax.div(o, 2) + n // 2 * core, n))).reshape(layers, 16, LANES)
    p1[pl.ds(0, layers), pl.ds(0, 16, stride=2), :] = e
    p1[pl.ds(0, layers), pl.ds(1, 16, stride=2), :] = e
    for m in range(2 * layers):
        i = X1 - 2 * halo + m
        v1[i, pl.ds(Y1 - 8, 32), :] = v1[i, pl.ds(Y1 - 8, 32), :] + p1[m // 2]


def add_from_1(w, v, v1, p0, halo, x_at, y_from, skip, rows):
    for m in range(BX // 2 + 2 * halo):
        e = v1[X1 - halo + m, pl.ds(Y1 - 8, 32), :]
        p0[m, pl.ds(0, 32, stride=2), :] = e
        p0[m, pl.ds(1, 32, stride=2), :] = e
    for x in range(-2 * halo, BX + 2 * halo):
        for h in range(2):
            w[h][X0 + x, pl.ds(Y0 - skip, rows), :] = (
                v[h][x_at + x, pl.ds(y_from, rows), :] + p0[x // 2 + halo, pl.ds(16 - skip, rows), :]
            )


def lay_out_1(dst, f1, edges, core, own, width):
    up, down = edges[0][...], edges[1][...]
    other_up, other_down = (pltpu.roll(edge[...], 64, 1) for edge in edges[2:])
    first = core == 0
    x_low, y_low = jnp.where(first, up, other_up), jnp.where(first, other_up, up)
    x_high, y_high = jnp.where(first, down, other_down), jnp.where(first, other_down, down)
    for m in range(f1.shape[0]):
        i = X1 - own + m
        dst[i, pl.ds(Y1 - 4, 24), :] = f1[m]
        dst[i, pl.ds(Y1 - own - width, width), :] = y_low[m * width : (m + 1) * width]
        dst[i, pl.ds(Y1 + 16 + own, width), :] = y_high[m * width : (m + 1) * width]
    for m in range(width):
        dst[X1 - own - width + m, pl.ds(Y1 - 4, 24), :] = x_low[m * 24 : (m + 1) * 24]
        dst[X1 + 8 + own + m, pl.ds(Y1 - 4, 24), :] = x_high[m * 24 : (m + 1) * 24]


def put_out_1(out, up, down, f1, core, own, width):
    for m in range(out.shape[0]):
        out[m] = f1[X1 - own + m, pl.ds(Y1 - 4, 24), :]

    @pl.when(core == 0)
    def _():
        for m in range(width):
            up[pl.ds(m * 24, 24), :] = f1[X1 + 8 - own - width + m, pl.ds(Y1 - 4, 24), :]
            down[pl.ds(m * 24, 24), :] = f1[X1 + own + m, pl.ds(Y1 - 4, 24), :]

    @pl.when(core == 1)
    def _():
        for m in range(out.shape[0]):
            up[pl.ds(m * width, width), :] = f1[X1 - own + m, pl.ds(Y1 + 16 - own - width, width), :]
            down[pl.ds(m * width, width), :] = f1[X1 - own + m, pl.ds(Y1 + own, width), :]


def split_kernel(charge, mine, up, down):
    matrix = pick_matrix(lambda o: jnp.where(o < 64, 2 * o, 2 * o - 127))
    split = dot(flat(charge[...]), matrix).reshape(BX, BY, LANES)
    mine[...] = split
    up[...] = split[BX - HALO :]
    down[...] = split[:HALO]


def edges_kernel(mine, x_low, x_high, up, down):
    at = 0
    for ref in (x_low, mine, x_high):
        for i in range(ref.shape[0]):
            down[pl.ds(at * HALO, HALO), :] = ref[i, pl.ds(0, HALO), :]
            up[pl.ds(at * HALO, HALO), :] = ref[i, pl.ds(BY - HALO, HALO), :]
            at += 1


def lay_out_0(even, odd, ours, others):
    def both(p, q):
        low = iota(p.shape, p.ndim - 1) < 64
        return (
            jnp.where(low, p, pltpu.roll(q, 64, p.ndim - 1)),
            jnp.where(low, pltpu.roll(p, 64, p.ndim - 1), q),
        )

    at = X0 - HALO
    for k in (1, 0, 2):
        for m in range(ours[k].shape[0]):
            e, o = both(ours[k][m], others[k][m])
            even[at, pl.ds(Y0, BY), :] = e
            odd[at, pl.ds(Y0, BY), :] = o
            at += 1
    for k, row in ((3, Y0 - HALO), (4, Y0 + BY)):
        e, o = both(ours[k][...], others[k][...])
        for m in range(BX + 2 * HALO):
            even[X0 - HALO + m, pl.ds(row, HALO), :] = e[m * HALO : (m + 1) * HALO]
            odd[X0 - HALO + m, pl.ds(row, HALO), :] = o[m * HALO : (m + 1) * HALO]


def first_kernel(where, *refs):
    ours, others, refs = refs[0:5], refs[5:10], refs[10:]
    (f_e, f_o, v_e, v_o, send), f1_outs, (f1, v1, r1, t0) = refs[:5], refs[5:8], refs[8:]
    core = where()[2]
    force, v = (f_e, f_o), (v_e, v_o)
    lay_out_0(f_e, f_o, ours, others)
    start_0(v, force, 9, 7)
    restrict_0(f1, t0, v, force, 4)
    coarse_source(send, f1, v1, r1, core)
    put_out_1(*f1_outs, f1, core, 4, 4)


def middle_kernel(where, *refs):
    bottom, f_e, f_o, v_e, v_o, f1_in, mine, other, *edges = refs[:12]
    (n_e, n_o, send), f1_outs = refs[12:15], refs[15:18]
    a_e, a_o, b_e, b_o, f1, v1, r1, p1, y2, p0, t0, f2, v2, t2, t3, s3, p2, a2, b2, near, matrix, arrived = refs[18:]
    fetch = pltpu.make_async_copy(bottom, matrix, arrived)
    fetch.start()
    gx, gy, core = where()
    force, v, a0, b0 = (f_e, f_o), (v_e, v_o), (a_e, a_o), (b_e, b_o)
    unpack_2(f2, mine, other, core)
    level_2(near, f2, v2, t2, t3, s3, p2, a2, b2, matrix, fetch, gx, 4)
    lay_out_1(f1, f1_in, edges, core, 4, 4)
    start_1(v1, f1, 7, 12)
    add_from_2(v1, near, y2, p1, gy, core, 4)
    sweep_1(r1, v1, f1, 6, 12)
    sweep_1(v1, r1, f1, 5, 9)
    add_from_1(a0, v, v1, p0, 5, X0, Y0 - 16, 16, 64)
    sweep_0(b0, a0, force, 8, 8)
    sweep_0(a0, b0, force, 7, 8)
    sweep_0(b0, a0, force, 6, 7)
    sweep_0(a0, b0, force, 5, 7)
    restrict_0(f1, t0, a0, force, 2)
    coarse_source(send, f1, v1, r1, core)
    put_out_1(*f1_outs, f1, core, 2, 2)
    for src, dst in ((a_e, n_e), (a_o, n_o)):
        dst[...] = src[pl.ds(X0 - 2, 20), pl.ds(Y0 - 8, 48), :]


def last_kernel(where, *refs):
    bottom, f_e, f_o, n_e, n_o, f1_in, mine, other, *edges = refs[:12]
    out, a_e, a_o, b_e, b_o, f1, v1, r1, p1, y2, p0, _, f2, v2, t2, t3, s3, p2, a2, b2, near, matrix, arrived = refs[12:]
    fetch = pltpu.make_async_copy(bottom, matrix, arrived)
    fetch.start()
    gx, gy, core = where()
    force, v, a0, b0 = (f_e, f_o), (n_e, n_o), (a_e, a_o), (b_e, b_o)
    unpack_2(f2, mine, other, core)
    level_2(near, f2, v2, t2, t3, s3, p2, a2, b2, matrix, fetch, gx, 2)
    lay_out_1(f1, f1_in, edges, core, 2, 2)
    start_1(v1, f1, 3, 14)
    add_from_2(v1, near, y2, p1, gy, core, 2)
    sweep_1(r1, v1, f1, 2, 12)
    sweep_1(v1, r1, f1, 1, 10)
    add_from_1(a0, v, v1, p0, 1, 2, 0, 8, 48)
    sweep_0(b0, a0, force, 1, 6)
    low = iota((BY, LANES), 1) < 64

    def body(i):
        centre, nb = beside_0(b0, i, Y0, BY)
        even, odd = (relaxed(0, force[h][i, pl.ds(Y0, BY), :], centre[h], nb[h]) for h in range(2))
        p0[i - X0, pl.ds(0, BY), :] = jnp.where(low, even, pltpu.roll(odd, 64, 1))

    over_layers(X0, BX, 8, body)
    matrix = pick_matrix(lambda o: lax.div(o, 2) + 64 * lax.rem(o, 2))
    out[...] = dot(flat(p0[pl.ds(0, BX), pl.ds(0, BY), :]), matrix).reshape(BX, BY, LANES)


def vm(*shape):
    return pltpu.VMEM(shape, F32)


def kept(*shape):
    return jax.ShapeDtypeStruct(shape, F32)


def scratch_for_cycle():
    x2, y2, _ = sizes_2()
    cells = int(np.prod(bottom_shape()))
    return (
        [vm(XA0, YA0, LANES)] * 4
        + [vm(XA1, YA1, LANES)] * 3
        + [vm(12, y2, LANES), vm(12, 2 * y2, LANES), vm(20, 64, LANES), vm(16, 48, LANES)]
        + [vm(x2, y2, LANES)] * 2
        + [vm(x2 // 2, y2, LANES), vm(x2 // 4, y2 // 2, LANES), vm(x2 // 2, y2 // 2, LANES), vm(8, y2, LANES)]
        + [vm(16, y2, LANES)] * 2
        + [vm(12, y2, LANES), vm(cells, cells), pltpu.SemaphoreType.DMA(())]
    )


def run(kernel, outs, scratch, flops, *args, fetched=0):
    spaces = [pltpu.HBM] * fetched + [pltpu.VMEM] * (len(args) - fetched)
    return pl.pallas_call(
        kernel,
        in_specs=[pl.BlockSpec(memory_space=space) for space in spaces],
        out_shape=outs,
        scratch_shapes=scratch,
        compiler_params=pltpu.CompilerParams(vmem_limit_bytes=40 * 2**20),
        cost_estimate=pl.CostEstimate(flops=flops, bytes_accessed=2**20, transcendentals=0),
    )(*args)


def where_am_i():
    return lax.axis_index("gx"), lax.axis_index("gy"), lax.axis_index("gz")


def sources_out(layers, width):
    return [kept(peers(), 8, LANES), kept(layers, 24, LANES)] + [kept(width * 24, LANES)] * 2


def peers():
    return lax.axis_size("gx") * lax.axis_size("gy")


def split(charge):
    return run(split_kernel, [kept(BX, BY, LANES)] + [kept(HALO, BY, LANES)] * 2, [], 10**6, charge)


def edges(*args):
    return run(edges_kernel, [kept((BX + 2 * HALO) * HALO, LANES)] * 2, [], 10**6, *args)


def first(*args):
    outs = [kept(XA0, YA0, LANES)] * 4 + sources_out(16, 4)
    scratch = [vm(XA1, YA1, LANES)] * 3 + [vm(16, 48, LANES)]
    return run(functools.partial(first_kernel, where_am_i), outs, scratch, 10**7, *args)


def middle(*args):
    outs = [kept(20, 48, LANES)] * 2 + sources_out(12, 2)
    return run(functools.partial(middle_kernel, where_am_i), outs, scratch_for_cycle(), 4 * 10**7, *args, fetched=1)


def last(*args):
    outs = kept(BX, BY, LANES)
    return run(functools.partial(last_kernel, where_am_i), outs, scratch_for_cycle(), 2 * 10**7, *args, fetched=1)


def from_(value, axis, step):
    size = lax.axis_size(axis)
    return lax.ppermute(value, axis, [(i, (i + step) % size) for i in range(size)])


def beside_(value, step):
    axes = ("gx", "gy", "gz")
    sizes = [lax.axis_size(axis) for axis in axes]
    pairs = []
    for device in np.ndindex(*sizes):
        to = list(device)
        to[device[2]] = (to[device[2]] + step) % sizes[device[2]]
        pairs.append((int(np.ravel_multi_index(device, sizes)), int(np.ravel_multi_index(to, sizes))))
    return lax.ppermute(value, axes, pairs)


def exchange(send, f1, up, down):
    up, down = beside_(up, 1), beside_(down, -1)
    mine = lax.all_to_all(send, ("gx", "gy"), 0, 0, tiled=True)
    other, other_up, other_down = (from_(v, "gz", 1) for v in (mine, up, down))
    return f1, mine, other, up, down, other_up, other_down


def local(charge):
    mine, up, down = split(charge)
    x_low, x_high = from_(up, "gx", 1), from_(down, "gx", -1)
    up, down = edges(mine, x_low, x_high)
    y_low, y_high = from_(up, "gy", 1), from_(down, "gy", -1)
    ours = (mine, x_low, x_high, y_low, y_high)
    others = [from_(v, "gz", 1) for v in ours]
    f_e, f_o, v_e, v_o, *rest = first(*ours, *others)
    bottom = jnp.asarray(bottom_matrix(bottom_shape()))
    n_e, n_o, *rest = middle(bottom, f_e, f_o, v_e, v_o, *exchange(*rest))
    return last(bottom, f_e, f_o, n_e, n_o, *exchange(*rest))


def solution(mesh):
    return jax.shard_map(
        local,
        mesh=mesh,
        in_specs=(P(("groups", "gx"), "gy", "gz"),),
        out_specs=P(("groups", "gx"), "gy", "gz"),
        check_vma=False,
    )
```

```python
import functools

import jax
import jax.numpy as jnp
import numpy as np
from jax import lax
from jax.experimental import pallas as pl
from jax.experimental.pallas import tpu as pltpu
from jax.sharding import PartitionSpec as P

LEVELS = 7
LANES = 128
OMEGA = 2.0 / 3.0
SCREEN = 0.001
F32 = jnp.float32

BX, BY = 16, 32
X0, Y0, XA0, YA0 = 12, 24, 40, 80
X1, Y1, XA1, YA1 = 10, 16, 32, 48
HALO = 10


def coefficients(level):
    a = 0.25**level
    return a, OMEGA / (6.0 * a + SCREEN)


def residual_of(level, f, v, nb):
    a, _ = coefficients(level)
    apart = 6.0 * v - nb
    if level:
        apart = a * apart
    return (f - apart) - SCREEN * v


def relaxed(level, f, v, nb):
    return v + coefficients(level)[1] * residual_of(level, f, v, nb)


def twice_from_zero(level, f, nb):
    a, k = coefficients(level)
    return (2.0 * k - k * k * SCREEN) * f - (k * k * a) * (6.0 * f - nb)


def iota(shape, dim):
    return lax.broadcasted_iota(jnp.int32, shape, dim)


def parts(v):
    high = v.astype(jnp.bfloat16)
    rest = v - high.astype(F32)
    middle = rest.astype(jnp.bfloat16)
    return high, middle, (rest - middle.astype(F32)).astype(jnp.bfloat16)


def product(a, b):
    return lax.dot_general(a, b, (((1,), (0,)), ((), ())), preferred_element_type=F32)


def dot(a, b):
    b = b.astype(jnp.bfloat16)
    high, middle, low = (product(p, b) for p in parts(a))
    return high + (middle + low)


def over_layers(start, count, block, body):
    def step(b, carry):
        for u in range(block):
            body(start + b * block + u)
        return carry

    lax.fori_loop(0, -(-count // block), step, 0)


def beside_0(refs, i, j, rows):
    even, odd = (r[i, pl.ds(j, rows), :] for r in refs)
    along_z = odd + pltpu.roll(odd, 1, 1), even + pltpu.roll(even, LANES - 1, 1)
    out = []
    for r, z in zip(refs, along_z):
        out.append(
            (r[i - 1, pl.ds(j, rows), :] + r[i + 1, pl.ds(j, rows), :])
            + (r[i, pl.ds(j - 1, rows), :] + r[i, pl.ds(j + 1, rows), :])
            + z
        )
    return (even, odd), out


def sweep_0(dst, src, force, halo, block):
    def body(i):
        for j in range(Y0 - 8, Y0 + 40, 16):
            centre, nb = beside_0(src, i, j, 16)
            for h in range(2):
                dst[h][i, pl.ds(j, 16), :] = relaxed(0, force[h][i, pl.ds(j, 16), :], centre[h], nb[h])

    over_layers(X0 - halo, BX + 2 * halo, block, body)


def start_0(dst, force, halo, block):
    def body(i):
        for j in range(Y0 - 16, Y0 + 48, 16):
            centre, nb = beside_0(force, i, j, 16)
            for h in range(2):
                dst[h][i, pl.ds(j, 16), :] = twice_from_zero(0, centre[h], nb[h])

    over_layers(X0 - halo, BX + 2 * halo, block, body)


def restrict_0(f1, t0, v, force, halo):
    def body(q):
        for j in range(Y0 - 8, Y0 + 40, 16):
            total = None
            for i in (X0 - 2 * halo + 2 * q, X0 - 2 * halo + 2 * q + 1):
                centre, nb = beside_0(v, i, j, 16)
                for h in range(2):
                    r = residual_of(0, force[h][i, pl.ds(j, 16), :], centre[h], nb[h])
                    total = r if total is None else total + r
            t0[q, pl.ds(j - Y0 + 8, 16), :] = total

    layers = BX // 2 + 2 * halo
    over_layers(0, layers, layers // 2, body)
    for m in range(layers):
        f1[X1 - halo + m, pl.ds(Y1 - 4, 24), :] = 0.125 * (t0[m, pl.ds(0, 24, stride=2), :] + t0[m, pl.ds(1, 24, stride=2), :])


def mean_matrix(source_of_out):
    source, out = iota((LANES, LANES), 0), source_of_out(iota((LANES, LANES), 1))
    return jnp.where((source == out) | (source == out + 1), 0.125, 0.0).astype(F32)


def pick_matrix(source_of_out):
    return jnp.where(iota((LANES, LANES), 0) == source_of_out(iota((LANES, LANES), 1)), 1.0, 0.0).astype(F32)


def beside_1(ref, i, j, rows):
    centre = ref[i, pl.ds(j, rows), :]
    nb = (
        (ref[i - 1, pl.ds(j, rows), :] + ref[i + 1, pl.ds(j, rows), :])
        + (ref[i, pl.ds(j - 1, rows), :] + ref[i, pl.ds(j + 1, rows), :])
        + (pltpu.roll(centre, 1, 1) + pltpu.roll(centre, LANES - 1, 1))
    )
    return centre, nb


def sweep_1(dst, src, force, halo, block):
    def body(i):
        centre, nb = beside_1(src, i, Y1 - 8, 32)
        dst[i, pl.ds(Y1 - 8, 32), :] = relaxed(1, force[i, pl.ds(Y1 - 8, 32), :], centre, nb)

    over_layers(X1 - halo, BX // 2 + 2 * halo, block, body)


def start_1(dst, force, halo, block):
    def body(i):
        centre, nb = beside_1(force, i, Y1 - 8, 32)
        dst[i, pl.ds(Y1 - 8, 32), :] = twice_from_zero(1, centre, nb)

    over_layers(X1 - halo, BX // 2 + 2 * halo, block, body)


def sizes_2():
    return lax.axis_size("gx") * BX // 4, lax.axis_size("gy") * BY // 4, lax.axis_size("gz") * LANES // 4


def bottom_shape():
    return tuple(n // 8 for n in sizes_2())


def coarse_source(out, f1, v1, r1, core):
    start_1(v1, f1, 1, 10)

    def body(i):
        centre, nb = beside_1(v1, i, Y1, 16)
        r1[i, pl.ds(Y1, 16), :] = residual_of(1, f1[i, pl.ds(Y1, 16), :], centre, nb)

    over_layers(X1, BX // 2, 8, body)
    layers = []
    for q in range(4):
        i = X1 + 2 * q
        s = (r1[i, pl.ds(Y1, 8, stride=2), :] + r1[i, pl.ds(Y1 + 1, 8, stride=2), :]) + (
            r1[i + 1, pl.ds(Y1, 8, stride=2), :] + r1[i + 1, pl.ds(Y1 + 1, 8, stride=2), :]
        )
        layers.append(jnp.where(core == 0, s[0:4], s[4:8]))
    n = sizes_2()[2]
    at = lambda o: 2 * lax.rem(o + n // 2 * core, n)
    low = mean_matrix(lambda o: jnp.where(o < n, at(o), -2))
    high = mean_matrix(lambda o: jnp.where(o >= n, at(o), -2))
    packed = dot(jnp.concatenate(layers[0:2], axis=0), low) + dot(jnp.concatenate(layers[2:4], axis=0), high)
    for s in range(out.shape[0]):
        out[s] = packed


def turned(v, step, n):
    axis = v.ndim - 1
    moved = pltpu.roll(v, step % LANES, axis)
    if n == LANES:
        return moved
    lane = lax.rem(iota(v.shape, axis), n)
    wrapped = pltpu.roll(v, (step - n if step > 0 else step + n) % LANES, axis)
    return jnp.where(lane < step if step > 0 else lane >= n + step, wrapped, moved)


def along_z(v, step, n):
    return turned(v, step, n) + turned(v, -step, n)


def next_segment(v, n):
    return pltpu.roll(v, n % LANES, v.ndim - 1)


def across(v, n):
    last, rows = v.shape[0] - 1, v.shape[1]
    up = jnp.concatenate([next_segment(v[last:], n), v[:last]], axis=0)
    down = jnp.concatenate([v[1:], next_segment(v[:1], -n)], axis=0)
    return (up + down) + (pltpu.roll(v, 1, 1) + pltpu.roll(v, rows - 1, 1))


def applied(level, v, n):
    a, _ = coefficients(level)
    z1, z2 = along_z(v, 1, n), along_z(v, 2, n)
    one = across(v, n)
    sv = one + z1
    ssv = across(one + 2.0 * z1, n) + (z2 + 2.0 * v)
    t = 6.0 * v - sv
    tt = 6.0 * t - (6.0 * sv - ssv)
    return t, a * t + SCREEN * v, (a * a) * tt + (2.0 * a * SCREEN) * t + (SCREEN * SCREEN) * v


def start_whole(level, f, n=LANES):
    a, k = coefficients(level)
    t, af, aaf = applied(level, f, n)
    return (2.0 * k - k * k * SCREEN) * f - (k * k * a) * t, f - 2.0 * k * af + (k * k) * aaf, af


def smooth_whole(level, f, af, v, n=LANES):
    a, k = coefficients(level)
    t, _, aav = applied(level, v, n)
    r = (f - a * t) - SCREEN * v
    return v + 2.0 * k * r - (k * k) * (af - aav)


def bottom_matrix(shape):
    def beside(v):
        return sum(np.roll(v, step, axis) for axis in (1, 2, 3) for step in (1, -1))

    def residual(level, f, v):
        return f - ((6.0 * v - beside(v)) * 0.25**level + SCREEN * v)

    def cycle(level, f):
        v = np.zeros_like(f)
        for _ in range(2):
            v = v + OMEGA * residual(level, f, v) / (6.0 * 0.25**level + SCREEN)
        if level == LEVELS - 1:
            return v
        n, x, y, z = f.shape
        coarse = residual(level, f, v).reshape(n, x // 2, 2, y // 2, 2, z // 2, 2).mean(axis=(2, 4, 6))
        v = v + cycle(level + 1, coarse).repeat(2, 1).repeat(2, 2).repeat(2, 3)
        for _ in range(2):
            v = v + OMEGA * residual(level, f, v) / (6.0 * 0.25**level + SCREEN)
        return v

    cells = shape[0] * shape[1] * shape[2]
    return cycle(5, np.eye(cells).reshape(cells, *shape)).reshape(cells, cells).astype(np.float32)


def up_z(level):
    n = sizes_2()[2] >> (level - 2)
    return pick_matrix(lambda o: lax.div(lax.rem(o, n), 2))


def pair_layers(v):
    v = v.reshape(v.shape[0] // 2, 2, *v.shape[1:])
    return v[:, 0] + v[:, 1]


def twice(v):
    return jnp.concatenate([v[:, None], v[:, None]], axis=1).reshape(2 * v.shape[0], *v.shape[1:])


def flat(v):
    return v.reshape(-1, LANES)


def solve_bottom(s, shape, matrix):
    x5, y5, z5 = shape
    cells = x5 * y5 * z5
    rows = s.shape[0]
    cell, row = iota((rows, cells), 1), iota((rows, cells), 0)
    mine = (cell // (y5 * z5) == row // (2 * y5)) & (lax.rem(cell // z5, y5) == lax.rem(row, 2 * y5) // 2)
    source, out = iota((LANES, cells), 0), lax.rem(iota((LANES, cells), 1), z5)
    means = jnp.where((source == 2 * out) | (source == 2 * out + 1), 0.125, 0.0).astype(F32)
    f5 = jnp.sum(jnp.where(mine, dot(s, means), 0.0), axis=0, keepdims=True)
    f_high, f_middle, f_low = parts(jnp.broadcast_to(f5, (8, cells)))
    m_high, m_middle, m_low = parts(matrix[...])
    v5 = product(f_high, m_high) + (
        (product(f_high, m_middle) + product(f_middle, m_high))
        + (product(f_high, m_low) + product(f_middle, m_middle) + product(f_low, m_high))
    )
    spread = jnp.where(mine, jnp.broadcast_to(v5[0:1], (rows, cells)), 0.0)
    source, out = lax.rem(iota((cells, LANES), 0), z5), lax.rem(iota((cells, LANES), 1), 2 * z5)
    return dot(spread, jnp.where(source == out // 2, 1.0, 0.0).astype(F32))


def solve_3(f3, t3, matrix):
    n, x3, y4 = sizes_2()[2] // 2, f3.shape[0], f3.shape[1] // 2
    segments, x4 = LANES // n, x3 // 2
    v3, r3, af3 = start_whole(3, f3, n)
    t3[...] = pair_layers(r3)
    s = flat(t3[:, pl.ds(0, y4, stride=2), :] + t3[:, pl.ds(1, y4, stride=2), :])
    means = [mean_matrix(lambda o: n * q + 2 * lax.rem(o, n // 2)) for q in range(segments)]
    f4 = jnp.concatenate([dot(s, m).reshape(x4, y4, LANES) for m in means], axis=0)
    v4, r4, af4 = start_whole(4, f4)
    e4 = solve_bottom(flat(pair_layers(r4)), bottom_shape(), matrix).reshape(-1, y4, LANES)
    v4 = smooth_whole(4, f4, af4, v4 + twice(e4))
    picks = [pick_matrix(lambda o: jnp.where(o // n == q, lax.rem(o, n) // 2, -1)) for q in range(segments)]
    e3 = sum(dot(flat(v4[x4 * q : x4 * (q + 1)]), m) for q, m in enumerate(picks)).reshape(x4, y4, LANES)
    t3[:, pl.ds(0, y4, stride=2), :] = e3
    t3[:, pl.ds(1, y4, stride=2), :] = e3
    return smooth_whole(3, f3, af3, v3 + twice(t3[...]), n)


def unpack_2(f2, mine, other, core):
    low = iota((8, LANES), 1) < 64
    top = iota((8, LANES), 0) < 4
    along_y = lax.axis_size("gy")
    half = (f2.shape[0] - 2) // 4

    def body(gx):
        for gy in range(along_y):
            tiles = []
            for g in (gx, gx + half):
                t, p = mine[g * along_y + gy], other[g * along_y + gy]
                u, w = jnp.where(core == 0, t, p), jnp.where(core == 0, p, t)
                tiles.append((u, w))
            (u, w), (u2, w2) = tiles
            for xp in range(2):
                if xp == 0:
                    d, e = jnp.where(low, u, pltpu.roll(u2, 64, 1)), jnp.where(low, w, pltpu.roll(w2, 64, 1))
                else:
                    d, e = jnp.where(low, pltpu.roll(u, 64, 1), u2), jnp.where(low, pltpu.roll(w, 64, 1), w2)
                f2[1 + gx * 4 + 2 * xp, pl.ds(gy * 8, 8), :] = jnp.where(top, d, pltpu.roll(e, 4, 0))
                f2[2 + gx * 4 + 2 * xp, pl.ds(gy * 8, 8), :] = jnp.where(top, pltpu.roll(d, 4, 0), e)

    over_layers(0, half, 4, body)


def close_2(v):
    last = v.shape[0] - 2
    v[0] = next_segment(v[last], 64)
    v[last + 1] = next_segment(v[1], -64)


def beside_2(centre, before, after, n):
    rows = centre.shape[0]
    return (
        (before + after) + (pltpu.roll(centre, 1, 0) + pltpu.roll(centre, rows - 1, 0)) + along_z(centre, 1, n)
    )


def level_2(near, f2, v2, t2, t3, s3, p2, a2, b2, bottom, gx, halo):
    n, rows, length = f2.shape[0] - 2, f2.shape[1], sizes_2()[2]
    close_2(f2)

    def first(i):
        v2[i] = twice_from_zero(2, f2[i], beside_2(f2[i], f2[i - 1], f2[i + 1], length))

    over_layers(1, n, 16, first)
    close_2(v2)

    def second(q):
        pair = []
        for i in (2 * q + 1, 2 * q + 2):
            pair.append(residual_of(2, f2[i], v2[i], beside_2(v2[i], v2[i - 1], v2[i + 1], length)))
        t2[q] = pair[0] + pair[1]

    over_layers(0, n // 2, 8, second)
    s = t2[:, pl.ds(0, rows // 2, stride=2), :] + t2[:, pl.ds(1, rows // 2, stride=2), :]
    x3 = n // 4

    def means(part):
        def source(o):
            q = o // (length // 2)
            return jnp.where(lax.rem(q, 2) == part, q // 2 * length + 2 * lax.rem(o, length // 2), -2)

        return mean_matrix(source)

    f3 = dot(flat(s[:x3]), means(0)) + dot(flat(s[x3:]), means(1))
    s3[...] = solve_3(f3.reshape(x3, rows // 2, LANES), t3, bottom)

    count = 4 + 2 * halo + 4
    start = gx * 4 - halo - 2 + 2 * n
    lines = []
    for m in range(count // 2):
        at = lax.rem(lax.div(start, 2) + m, n)
        line = s3[lax.rem(at, x3)]
        lines.append(pltpu.roll(line, lax.rem(LANES - length // 2 * lax.div(at, x3), LANES), 1))
    e = dot(jnp.concatenate(lines, axis=0), up_z(2)).reshape(count // 2, rows // 2, LANES)
    p2[pl.ds(0, count // 2), pl.ds(0, rows // 2, stride=2), :] = e
    p2[pl.ds(0, count // 2), pl.ds(1, rows // 2, stride=2), :] = e
    low = iota((rows, LANES), 1) < 64
    for m in range(count):
        at = lax.rem(start + m, 2 * n)
        i, lower = 1 + lax.rem(at, n), at < n
        whole = []
        for ref in (v2, f2):
            turned_half = pltpu.roll(ref[i], 64, 1)
            whole.append(jnp.where(low, jnp.where(lower, ref[i], turned_half), jnp.where(lower, turned_half, ref[i])))
        a2[m] = whole[0] + p2[m // 2]
        t2[m] = whole[1]
    for m in range(1, count - 1):
        nb = beside_2(a2[m], a2[m - 1], a2[m + 1], LANES)
        b2[m] = relaxed(2, t2[m], a2[m], nb)
    for m in range(2, count - 2):
        nb = beside_2(b2[m], b2[m - 1], b2[m + 1], LANES)
        near[m - 2] = relaxed(2, t2[m], b2[m], nb)


def add_from_2(v1, near, y2, p1, gy, core, halo):
    layers = 4 + 2 * halo
    rows, n = sizes_2()[1:]
    for m in range(layers):
        y2[m, pl.ds(0, rows), :] = near[m]
        y2[m, pl.ds(rows, rows), :] = near[m]
    start = pl.multiple_of(lax.rem(gy * 8 + rows - 4, rows), 4)
    picked = jnp.concatenate([y2[m, pl.ds(start, 16), :] for m in range(layers)], axis=0)
    e = dot(picked, pick_matrix(lambda o: lax.rem(lax.div(o, 2) + n // 2 * core, n))).reshape(layers, 16, LANES)
    p1[pl.ds(0, layers), pl.ds(0, 16, stride=2), :] = e
    p1[pl.ds(0, layers), pl.ds(1, 16, stride=2), :] = e
    for m in range(2 * layers):
        i = X1 - 2 * halo + m
        v1[i, pl.ds(Y1 - 8, 32), :] = v1[i, pl.ds(Y1 - 8, 32), :] + p1[m // 2]


def add_from_1(w, v, v1, p0, halo, x_at, y_from, skip, rows):
    for m in range(BX // 2 + 2 * halo):
        e = v1[X1 - halo + m, pl.ds(Y1 - 8, 32), :]
        p0[m, pl.ds(0, 32, stride=2), :] = e
        p0[m, pl.ds(1, 32, stride=2), :] = e
    for x in range(-2 * halo, BX + 2 * halo):
        for h in range(2):
            w[h][X0 + x, pl.ds(Y0 - skip, rows), :] = (
                v[h][x_at + x, pl.ds(y_from, rows), :] + p0[x // 2 + halo, pl.ds(16 - skip, rows), :]
            )


def lay_out_1(dst, f1, edges, core, own, width):
    up, down = edges[0][...], edges[1][...]
    other_up, other_down = (pltpu.roll(edge[...], 64, 1) for edge in edges[2:])
    first = core == 0
    x_low, y_low = jnp.where(first, up, other_up), jnp.where(first, other_up, up)
    x_high, y_high = jnp.where(first, down, other_down), jnp.where(first, other_down, down)
    for m in range(f1.shape[0]):
        i = X1 - own + m
        dst[i, pl.ds(Y1 - 4, 24), :] = f1[m]
        dst[i, pl.ds(Y1 - own - width, width), :] = y_low[m * width : (m + 1) * width]
        dst[i, pl.ds(Y1 + 16 + own, width), :] = y_high[m * width : (m + 1) * width]
    for m in range(width):
        dst[X1 - own - width + m, pl.ds(Y1 - 4, 24), :] = x_low[m * 24 : (m + 1) * 24]
        dst[X1 + 8 + own + m, pl.ds(Y1 - 4, 24), :] = x_high[m * 24 : (m + 1) * 24]


def put_out_1(out, up, down, f1, core, own, width):
    for m in range(out.shape[0]):
        out[m] = f1[X1 - own + m, pl.ds(Y1 - 4, 24), :]

    @pl.when(core == 0)
    def _():
        for m in range(width):
            up[pl.ds(m * 24, 24), :] = f1[X1 + 8 - own - width + m, pl.ds(Y1 - 4, 24), :]
            down[pl.ds(m * 24, 24), :] = f1[X1 + own + m, pl.ds(Y1 - 4, 24), :]

    @pl.when(core == 1)
    def _():
        for m in range(out.shape[0]):
            up[pl.ds(m * width, width), :] = f1[X1 - own + m, pl.ds(Y1 + 16 - own - width, width), :]
            down[pl.ds(m * width, width), :] = f1[X1 - own + m, pl.ds(Y1 + own, width), :]


def split_kernel(charge, mine, up, down):
    matrix = pick_matrix(lambda o: jnp.where(o < 64, 2 * o, 2 * o - 127))
    split = dot(flat(charge[...]), matrix).reshape(BX, BY, LANES)
    mine[...] = split
    up[...] = split[BX - HALO :]
    down[...] = split[:HALO]


def edges_kernel(mine, x_low, x_high, up, down):
    at = 0
    for ref in (x_low, mine, x_high):
        for i in range(ref.shape[0]):
            down[pl.ds(at * HALO, HALO), :] = ref[i, pl.ds(0, HALO), :]
            up[pl.ds(at * HALO, HALO), :] = ref[i, pl.ds(BY - HALO, HALO), :]
            at += 1


def lay_out_0(even, odd, ours, others):
    def both(p, q):
        low = iota(p.shape, p.ndim - 1) < 64
        return (
            jnp.where(low, p, pltpu.roll(q, 64, p.ndim - 1)),
            jnp.where(low, pltpu.roll(p, 64, p.ndim - 1), q),
        )

    at = X0 - HALO
    for k in (1, 0, 2):
        for m in range(ours[k].shape[0]):
            e, o = both(ours[k][m], others[k][m])
            even[at, pl.ds(Y0, BY), :] = e
            odd[at, pl.ds(Y0, BY), :] = o
            at += 1
    for k, row in ((3, Y0 - HALO), (4, Y0 + BY)):
        e, o = both(ours[k][...], others[k][...])
        for m in range(BX + 2 * HALO):
            even[X0 - HALO + m, pl.ds(row, HALO), :] = e[m * HALO : (m + 1) * HALO]
            odd[X0 - HALO + m, pl.ds(row, HALO), :] = o[m * HALO : (m + 1) * HALO]


def first_kernel(where, *refs):
    ours, others, refs = refs[0:5], refs[5:10], refs[10:]
    (f_e, f_o, v_e, v_o, send), f1_outs, (f1, v1, r1, t0) = refs[:5], refs[5:8], refs[8:]
    core = where()[2]
    force, v = (f_e, f_o), (v_e, v_o)
    lay_out_0(f_e, f_o, ours, others)
    start_0(v, force, 9, 17)
    restrict_0(f1, t0, v, force, 4)
    coarse_source(send, f1, v1, r1, core)
    put_out_1(*f1_outs, f1, core, 4, 4)


def middle_kernel(where, *refs):
    bottom, f_e, f_o, v_e, v_o, f1_in, mine, other, *edges = refs[:12]
    (n_e, n_o, send), f1_outs = refs[12:15], refs[15:18]
    a_e, a_o, b_e, b_o, f1, v1, r1, p1, y2, p0, t0, f2, v2, t2, t3, s3, p2, a2, b2, near = refs[18:]
    gx, gy, core = where()
    force, v, a0, b0 = (f_e, f_o), (v_e, v_o), (a_e, a_o), (b_e, b_o)
    unpack_2(f2, mine, other, core)
    level_2(near, f2, v2, t2, t3, s3, p2, a2, b2, bottom, gx, 4)
    lay_out_1(f1, f1_in, edges, core, 4, 4)
    start_1(v1, f1, 7, 12)
    add_from_2(v1, near, y2, p1, gy, core, 4)
    sweep_1(r1, v1, f1, 6, 12)
    sweep_1(v1, r1, f1, 5, 9)
    add_from_1(a0, v, v1, p0, 5, X0, Y0 - 16, 16, 64)
    sweep_0(b0, a0, force, 8, 16)
    sweep_0(a0, b0, force, 7, 15)
    sweep_0(b0, a0, force, 6, 14)
    sweep_0(a0, b0, force, 5, 13)
    restrict_0(f1, t0, a0, force, 2)
    coarse_source(send, f1, v1, r1, core)
    put_out_1(*f1_outs, f1, core, 2, 2)
    for src, dst in ((a_e, n_e), (a_o, n_o)):
        dst[...] = src[pl.ds(X0 - 2, 20), pl.ds(Y0 - 8, 48), :]


def last_kernel(where, *refs):
    bottom, f_e, f_o, n_e, n_o, f1_in, mine, other, *edges = refs[:12]
    out, a_e, a_o, b_e, b_o, f1, v1, r1, p1, y2, p0, _, f2, v2, t2, t3, s3, p2, a2, b2, near, held, left = refs[12:]
    gx, gy, core = where()
    force, v, a0, b0 = (f_e, f_o), (n_e, n_o), (a_e, a_o), (b_e, b_o)
    unpack_2(f2, mine, other, core)
    level_2(near, f2, v2, t2, t3, s3, p2, a2, b2, bottom, gx, 2)
    lay_out_1(f1, f1_in, edges, core, 2, 2)
    start_1(v1, f1, 3, 14)
    add_from_2(v1, near, y2, p1, gy, core, 2)
    sweep_1(r1, v1, f1, 2, 12)
    sweep_1(v1, r1, f1, 1, 10)
    add_from_1(a0, v, v1, p0, 1, 2, 0, 8, 48)
    sweep_0(b0, a0, force, 1, 9)
    low = iota((BY, LANES), 1) < 64
    matrix = pick_matrix(lambda o: lax.div(o, 2) + 64 * lax.rem(o, 2))
    pieces = [pl.ds(4 * k, 4) for k in range(BX // 4)]
    stores = [pltpu.make_async_copy(held.at[p], out.at[p], left.at[k]) for k, p in enumerate(pieces)]
    for k, store in enumerate(stores):
        lines = []
        for i in range(X0 + 4 * k, X0 + 4 * k + 4):
            centre, nb = beside_0(b0, i, Y0, BY)
            even, odd = (relaxed(0, force[h][i, pl.ds(Y0, BY), :], centre[h], nb[h]) for h in range(2))
            lines.append(jnp.where(low, even, pltpu.roll(odd, 64, 1)))
        held[pieces[k]] = dot(jnp.concatenate(lines, axis=0), matrix).reshape(4, BY, LANES)
        store.start()
    for store in stores:
        store.wait()


def vm(*shape):
    return pltpu.VMEM(shape, F32)


def kept(*shape):
    return jax.ShapeDtypeStruct(shape, F32)


def scratch_for_cycle():
    x2, y2, _ = sizes_2()
    return (
        [vm(XA0, YA0, LANES)] * 4
        + [vm(XA1, YA1, LANES)] * 3
        + [vm(12, y2, LANES), vm(12, 2 * y2, LANES), vm(20, 64, LANES), vm(16, 48, LANES)]
        + [vm(x2 // 2 + 2, y2, LANES)] * 2
        + [vm(16, y2, LANES), vm(x2 // 16, y2 // 2, LANES), vm(x2 // 8, y2 // 2, LANES), vm(8, y2, LANES)]
        + [vm(16, y2, LANES)] * 2
        + [vm(12, y2, LANES)]
    )


def run(kernel, outs, scratch, flops, *args, out_space=pltpu.VMEM):
    spec = pl.BlockSpec(memory_space=out_space)
    return pl.pallas_call(
        kernel,
        out_shape=outs,
        out_specs=[spec] * len(outs) if isinstance(outs, list) else spec,
        scratch_shapes=scratch,
        compiler_params=pltpu.CompilerParams(vmem_limit_bytes=40 * 2**20),
        cost_estimate=pl.CostEstimate(flops=flops, bytes_accessed=2**20, transcendentals=0),
    )(*args)


def where_am_i():
    return lax.axis_index("gx"), lax.axis_index("gy"), lax.axis_index("gz")


def sources_out(layers, width):
    return [kept(peers(), 8, LANES), kept(layers, 24, LANES)] + [kept(width * 24, LANES)] * 2


def peers():
    return lax.axis_size("gx") * lax.axis_size("gy")


def split(charge):
    return run(split_kernel, [kept(BX, BY, LANES)] + [kept(HALO, BY, LANES)] * 2, [], 10**6, charge)


def edges(*args):
    return run(edges_kernel, [kept((BX + 2 * HALO) * HALO, LANES)] * 2, [], 10**6, *args)


def first(*args):
    outs = [kept(XA0, YA0, LANES)] * 4 + sources_out(16, 4)
    scratch = [vm(XA1, YA1, LANES)] * 3 + [vm(16, 48, LANES)]
    return run(functools.partial(first_kernel, where_am_i), outs, scratch, 10**7, *args)


def middle(*args):
    outs = [kept(20, 48, LANES)] * 2 + sources_out(12, 2)
    return run(functools.partial(middle_kernel, where_am_i), outs, scratch_for_cycle(), 4 * 10**7, *args)


def last(*args):
    outs = kept(BX, BY, LANES)
    scratch = scratch_for_cycle() + [vm(BX, BY, LANES), pltpu.SemaphoreType.DMA((BX // 4,))]
    return run(functools.partial(last_kernel, where_am_i), outs, scratch, 2 * 10**7, *args, out_space=pltpu.HBM)


def from_(value, axis, step):
    size = lax.axis_size(axis)
    return lax.ppermute(value, axis, [(i, (i + step) % size) for i in range(size)])


def beside_(value, step):
    axes = ("gx", "gy", "gz")
    sizes = [lax.axis_size(axis) for axis in axes]
    pairs = []
    for device in np.ndindex(*sizes):
        to = list(device)
        to[device[2]] = (to[device[2]] + step) % sizes[device[2]]
        pairs.append((int(np.ravel_multi_index(device, sizes)), int(np.ravel_multi_index(to, sizes))))
    return lax.ppermute(value, axes, pairs)


def exchange(send, f1, up, down):
    up, down = beside_(up, 1), beside_(down, -1)
    mine = lax.all_to_all(send, ("gx", "gy"), 0, 0, tiled=True)
    other, other_up, other_down = (from_(v, "gz", 1) for v in (mine, up, down))
    return f1, mine, other, up, down, other_up, other_down


def local(charge):
    mine, up, down = split(charge)
    x_low, x_high = from_(up, "gx", 1), from_(down, "gx", -1)
    up, down = edges(mine, x_low, x_high)
    y_low, y_high = from_(up, "gy", 1), from_(down, "gy", -1)
    ours = (mine, x_low, x_high, y_low, y_high)
    others = [from_(v, "gz", 1) for v in ours]
    f_e, f_o, v_e, v_o, *rest = first(*ours, *others)
    bottom = jnp.asarray(bottom_matrix(bottom_shape()))
    n_e, n_o, *rest = middle(bottom, f_e, f_o, v_e, v_o, *exchange(*rest))
    return last(bottom, f_e, f_o, n_e, n_o, *exchange(*rest))


def solution(mesh):
    return jax.shard_map(
        local,
        mesh=mesh,
        in_specs=(P(("groups", "gx"), "gy", "gz"),),
        out_specs=P(("groups", "gx"), "gy", "gz"),
        check_vma=False,
    )
```

```python
import functools

import jax
import jax.numpy as jnp
import numpy as np
from jax import lax
from jax.experimental import pallas as pl
from jax.experimental.pallas import tpu as pltpu
from jax.sharding import PartitionSpec as P

LEVELS = 7
LANES = 128
OMEGA = 2.0 / 3.0
SCREEN = 0.001
F32 = jnp.float32

BX, BY = 16, 32
X0, Y0, XA0, YA0 = 12, 24, 40, 80
X1, Y1, XA1, YA1 = 10, 16, 32, 48
HALO = 10


def coefficients(level):
    a = 0.25**level
    return a, OMEGA / (6.0 * a + SCREEN)


def residual_of(level, f, v, nb):
    a, _ = coefficients(level)
    apart = 6.0 * v - nb
    if level:
        apart = a * apart
    return (f - apart) - SCREEN * v


def relaxed(level, f, v, nb):
    return v + coefficients(level)[1] * residual_of(level, f, v, nb)


def twice_from_zero(level, f, nb):
    a, k = coefficients(level)
    return (2.0 * k - k * k * SCREEN) * f - (k * k * a) * (6.0 * f - nb)


def iota(shape, dim):
    return lax.broadcasted_iota(jnp.int32, shape, dim)


def parts(v):
    high = v.astype(jnp.bfloat16)
    rest = v - high.astype(F32)
    middle = rest.astype(jnp.bfloat16)
    return high, middle, (rest - middle.astype(F32)).astype(jnp.bfloat16)


def product(a, b):
    return lax.dot_general(a, b, (((1,), (0,)), ((), ())), preferred_element_type=F32)


def dot(a, b):
    b = b.astype(jnp.bfloat16)
    high, middle, low = (product(p, b) for p in parts(a))
    return high + (middle + low)


def over_layers(start, count, block, body):
    def step(b, carry):
        for u in range(block):
            body(start + b * block + u)
        return carry

    lax.fori_loop(0, -(-count // block), step, 0)


def beside_0(refs, i, j, rows):
    even, odd = (r[i, pl.ds(j, rows), :] for r in refs)
    along_z = odd + pltpu.roll(odd, 1, 1), even + pltpu.roll(even, LANES - 1, 1)
    out = []
    for r, z in zip(refs, along_z):
        out.append(
            (r[i - 1, pl.ds(j, rows), :] + r[i + 1, pl.ds(j, rows), :])
            + (r[i, pl.ds(j - 1, rows), :] + r[i, pl.ds(j + 1, rows), :])
            + z
        )
    return (even, odd), out


def sweep_0(dst, src, force, halo, block):
    def body(i):
        for j in range(Y0 - 8, Y0 + 40, 16):
            centre, nb = beside_0(src, i, j, 16)
            for h in range(2):
                dst[h][i, pl.ds(j, 16), :] = relaxed(0, force[h][i, pl.ds(j, 16), :], centre[h], nb[h])

    over_layers(X0 - halo, BX + 2 * halo, block, body)


def start_0(dst, force, halo, block):
    def body(i):
        for j in range(Y0 - 16, Y0 + 48, 16):
            centre, nb = beside_0(force, i, j, 16)
            for h in range(2):
                dst[h][i, pl.ds(j, 16), :] = twice_from_zero(0, centre[h], nb[h])

    over_layers(X0 - halo, BX + 2 * halo, block, body)


def restrict_0(f1, t0, v, force, halo):
    def body(q):
        for j in range(Y0 - 8, Y0 + 40, 16):
            total = None
            for i in (X0 - 2 * halo + 2 * q, X0 - 2 * halo + 2 * q + 1):
                centre, nb = beside_0(v, i, j, 16)
                for h in range(2):
                    r = residual_of(0, force[h][i, pl.ds(j, 16), :], centre[h], nb[h])
                    total = r if total is None else total + r
            t0[q, pl.ds(j - Y0 + 8, 16), :] = total

    layers = BX // 2 + 2 * halo
    over_layers(0, layers, layers // 2, body)
    for m in range(layers):
        f1[X1 - halo + m, pl.ds(Y1 - 4, 24), :] = 0.125 * (t0[m, pl.ds(0, 24, stride=2), :] + t0[m, pl.ds(1, 24, stride=2), :])


def mean_matrix(source_of_out, gap=1):
    source, out = iota((LANES, LANES), 0), source_of_out(iota((LANES, LANES), 1))
    return jnp.where((source == out) | (source == out + gap), 0.125, 0.0).astype(F32)


def pick_matrix(source_of_out):
    return jnp.where(iota((LANES, LANES), 0) == source_of_out(iota((LANES, LANES), 1)), 1.0, 0.0).astype(F32)


def beside_1(ref, i, j, rows):
    centre = ref[i, pl.ds(j, rows), :]
    nb = (
        (ref[i - 1, pl.ds(j, rows), :] + ref[i + 1, pl.ds(j, rows), :])
        + (ref[i, pl.ds(j - 1, rows), :] + ref[i, pl.ds(j + 1, rows), :])
        + (pltpu.roll(centre, 1, 1) + pltpu.roll(centre, LANES - 1, 1))
    )
    return centre, nb


def sweep_1(dst, src, force, halo, block):
    def body(i):
        centre, nb = beside_1(src, i, Y1 - 8, 32)
        dst[i, pl.ds(Y1 - 8, 32), :] = relaxed(1, force[i, pl.ds(Y1 - 8, 32), :], centre, nb)

    over_layers(X1 - halo, BX // 2 + 2 * halo, block, body)


def start_1(dst, force, halo, block):
    def body(i):
        centre, nb = beside_1(force, i, Y1 - 8, 32)
        dst[i, pl.ds(Y1 - 8, 32), :] = twice_from_zero(1, centre, nb)

    over_layers(X1 - halo, BX // 2 + 2 * halo, block, body)


def sizes_2():
    return lax.axis_size("gx") * BX // 4, lax.axis_size("gy") * BY // 4, lax.axis_size("gz") * LANES // 4


def bottom_shape():
    return tuple(n // 8 for n in sizes_2())


def coarse_source(out, f1, v1, r1, core):
    start_1(v1, f1, 1, 10)

    def body(i):
        centre, nb = beside_1(v1, i, Y1, 16)
        r1[i, pl.ds(Y1, 16), :] = residual_of(1, f1[i, pl.ds(Y1, 16), :], centre, nb)

    over_layers(X1, BX // 2, 8, body)
    layers = []
    for q in range(4):
        i = X1 + 2 * q
        s = (r1[i, pl.ds(Y1, 8, stride=2), :] + r1[i, pl.ds(Y1 + 1, 8, stride=2), :]) + (
            r1[i + 1, pl.ds(Y1, 8, stride=2), :] + r1[i + 1, pl.ds(Y1 + 1, 8, stride=2), :]
        )
        layers.append(jnp.where(core == 0, s[0:4], s[4:8]))
    n = sizes_2()[2]
    at = lambda o: 2 * lax.rem(o // 2 + n // 2 * core, n)
    low = mean_matrix(lambda o: jnp.where(lax.rem(o, 2) == 0, at(o), -2))
    high = mean_matrix(lambda o: jnp.where(lax.rem(o, 2) == 1, at(o), -2))
    packed = dot(jnp.concatenate(layers[0:2], axis=0), low) + dot(jnp.concatenate(layers[2:4], axis=0), high)
    for s in range(out.shape[0]):
        out[s] = packed


def along_z(v, step, parts):
    axis = v.ndim - 1
    return pltpu.roll(v, step * parts, axis) + pltpu.roll(v, LANES - step * parts, axis)


def next_part(v, parts, ahead):
    if parts == 1:
        return v
    axis = v.ndim - 1
    q = lax.rem(iota(v.shape, axis), parts)
    if ahead:
        return jnp.where(q == 0, pltpu.roll(v, LANES + 1 - parts, axis), pltpu.roll(v, 1, axis))
    return jnp.where(q == parts - 1, pltpu.roll(v, parts - 1, axis), pltpu.roll(v, LANES - 1, axis))


def across(v, parts):
    last, rows = v.shape[0] - 1, v.shape[1]
    up = jnp.concatenate([next_part(v[last:], parts, True), v[:last]], axis=0)
    down = jnp.concatenate([v[1:], next_part(v[:1], parts, False)], axis=0)
    return (up + down) + (pltpu.roll(v, 1, 1) + pltpu.roll(v, rows - 1, 1))


def applied(level, v, parts):
    a, _ = coefficients(level)
    z1, z2 = along_z(v, 1, parts), along_z(v, 2, parts)
    one = across(v, parts)
    sv = one + z1
    ssv = across(one + 2.0 * z1, parts) + (z2 + 2.0 * v)
    t = 6.0 * v - sv
    tt = 6.0 * t - (6.0 * sv - ssv)
    return t, a * t + SCREEN * v, (a * a) * tt + (2.0 * a * SCREEN) * t + (SCREEN * SCREEN) * v


def start_whole(level, f, parts=1):
    a, k = coefficients(level)
    t, af, aaf = applied(level, f, parts)
    return (2.0 * k - k * k * SCREEN) * f - (k * k * a) * t, f - 2.0 * k * af + (k * k) * aaf, af


def smooth_whole(level, f, af, v, parts=1):
    a, k = coefficients(level)
    t, _, aav = applied(level, v, parts)
    r = (f - a * t) - SCREEN * v
    return v + 2.0 * k * r - (k * k) * (af - aav)


def bottom_matrix(shape):
    def beside(v):
        return sum(np.roll(v, step, axis) for axis in (1, 2, 3) for step in (1, -1))

    def residual(level, f, v):
        return f - ((6.0 * v - beside(v)) * 0.25**level + SCREEN * v)

    def cycle(level, f):
        v = np.zeros_like(f)
        for _ in range(2):
            v = v + OMEGA * residual(level, f, v) / (6.0 * 0.25**level + SCREEN)
        if level == LEVELS - 1:
            return v
        n, x, y, z = f.shape
        coarse = residual(level, f, v).reshape(n, x // 2, 2, y // 2, 2, z // 2, 2).mean(axis=(2, 4, 6))
        v = v + cycle(level + 1, coarse).repeat(2, 1).repeat(2, 2).repeat(2, 3)
        for _ in range(2):
            v = v + OMEGA * residual(level, f, v) / (6.0 * 0.25**level + SCREEN)
        return v

    cells = shape[0] * shape[1] * shape[2]
    return cycle(5, np.eye(cells).reshape(cells, *shape)).reshape(cells, cells).astype(np.float32)


def pair_layers(v):
    v = v.reshape(v.shape[0] // 2, 2, *v.shape[1:])
    return v[:, 0] + v[:, 1]


def twice(v):
    return jnp.concatenate([v[:, None], v[:, None]], axis=1).reshape(2 * v.shape[0], *v.shape[1:])


def flat(v):
    return v.reshape(-1, LANES)


def solve_bottom(s, shape, matrix):
    x5, y5, z5 = shape
    cells = x5 * y5 * z5
    rows = s.shape[0]
    cell, row = iota((rows, cells), 1), iota((rows, cells), 0)
    mine = (cell // (y5 * z5) == row // (2 * y5)) & (lax.rem(cell // z5, y5) == lax.rem(row, 2 * y5) // 2)
    source, out = iota((LANES, cells), 0), lax.rem(iota((LANES, cells), 1), z5)
    means = jnp.where((source == 2 * out) | (source == 2 * out + 1), 0.125, 0.0).astype(F32)
    f5 = jnp.sum(jnp.where(mine, dot(s, means), 0.0), axis=0, keepdims=True)
    f_high, f_middle, f_low = parts(jnp.broadcast_to(f5, (8, cells)))
    m_high, m_middle, m_low = parts(matrix[...])
    v5 = product(f_high, m_high) + (
        (product(f_high, m_middle) + product(f_middle, m_high))
        + (product(f_high, m_low) + product(f_middle, m_middle) + product(f_low, m_high))
    )
    spread = jnp.where(mine, jnp.broadcast_to(v5[0:1], (rows, cells)), 0.0)
    source, out = lax.rem(iota((cells, LANES), 0), z5), lax.rem(iota((cells, LANES), 1), 2 * z5)
    return dot(spread, jnp.where(source == out // 2, 1.0, 0.0).astype(F32))


def solve_3(f3, t3, matrix):
    x4, y4 = f3.shape[0] // 2, f3.shape[1] // 2
    parts_3 = LANES // (sizes_2()[2] // 2)
    v3, r3, af3 = start_whole(3, f3, parts_3)
    t3[...] = pair_layers(r3)
    s = flat(t3[:, pl.ds(0, y4, stride=2), :] + t3[:, pl.ds(1, y4, stride=2), :])
    z4 = LANES // parts_3 // 2
    means = [mean_matrix(lambda o: 2 * parts_3 * lax.rem(o, z4) + q, parts_3) for q in range(parts_3)]
    f4 = jnp.concatenate([dot(s, m).reshape(x4, y4, LANES) for m in means], axis=0)
    v4, r4, af4 = start_whole(4, f4)
    e4 = solve_bottom(flat(pair_layers(r4)), bottom_shape(), matrix).reshape(-1, y4, LANES)
    v4 = smooth_whole(4, f4, af4, v4 + twice(e4))
    picks = [pick_matrix(lambda o: jnp.where(lax.rem(o, parts_3) == q, o // parts_3 // 2, -1)) for q in range(parts_3)]
    e3 = sum(dot(flat(v4[x4 * q : x4 * (q + 1)]), m) for q, m in enumerate(picks)).reshape(x4, y4, LANES)
    t3[:, pl.ds(0, y4, stride=2), :] = e3
    t3[:, pl.ds(1, y4, stride=2), :] = e3
    return smooth_whole(3, f3, af3, v3 + twice(t3[...]), parts_3)


def unpack_2(f2, mine, other, core):
    even = lax.rem(iota((8, LANES), 1), 2) == 0
    top = iota((8, LANES), 0) < 4
    along_y = lax.axis_size("gy")
    half = (f2.shape[0] - 2) // 4

    def body(gx):
        for gy in range(along_y):
            tiles = []
            for g in (gx, gx + half):
                t, p = mine[g * along_y + gy], other[g * along_y + gy]
                u, w = jnp.where(core == 0, t, p), jnp.where(core == 0, p, t)
                tiles.append((u, w))
            (u, w), (u2, w2) = tiles
            for xp in range(2):
                if xp == 0:
                    d, e = jnp.where(even, u, pltpu.roll(u2, 1, 1)), jnp.where(even, w, pltpu.roll(w2, 1, 1))
                else:
                    d, e = jnp.where(even, pltpu.roll(u, LANES - 1, 1), u2), jnp.where(even, pltpu.roll(w, LANES - 1, 1), w2)
                f2[1 + gx * 4 + 2 * xp, pl.ds(gy * 8, 8), :] = jnp.where(top, d, pltpu.roll(e, 4, 0))
                f2[2 + gx * 4 + 2 * xp, pl.ds(gy * 8, 8), :] = jnp.where(top, pltpu.roll(d, 4, 0), e)

    over_layers(0, half, 4, body)


def close_2(v):
    last = v.shape[0] - 2
    v[0] = next_part(v[last], 2, True)
    v[last + 1] = next_part(v[1], 2, False)


def beside_2(centre, before, after):
    rows = centre.shape[0]
    return (
        (before + after) + (pltpu.roll(centre, 1, 0) + pltpu.roll(centre, rows - 1, 0)) + along_z(centre, 1, 2)
    )


def level_2(near, f2, v2, t2, t3, s3, p2, a2, b2, bottom, gx, halo):
    n, rows = f2.shape[0] - 2, f2.shape[1]
    close_2(f2)

    def first(i):
        v2[i] = twice_from_zero(2, f2[i], beside_2(f2[i], f2[i - 1], f2[i + 1]))

    over_layers(1, n, 16, first)
    close_2(v2)

    def second(q):
        pair = []
        for i in (2 * q + 1, 2 * q + 2):
            pair.append(residual_of(2, f2[i], v2[i], beside_2(v2[i], v2[i - 1], v2[i + 1])))
        t2[q] = pair[0] + pair[1]

    over_layers(0, n // 2, 8, second)
    s = t2[:, pl.ds(0, rows // 2, stride=2), :] + t2[:, pl.ds(1, rows // 2, stride=2), :]
    x3 = n // 4

    def means(part):
        def source(o):
            q = lax.rem(o, 4)
            return jnp.where(lax.rem(q, 2) == part, o // 4 * 4 + q // 2, -4)

        return mean_matrix(source, 2)

    f3 = dot(flat(s[:x3]), means(0)) + dot(flat(s[x3:]), means(1))
    s3[...] = solve_3(f3.reshape(x3, rows // 2, LANES), t3, bottom)

    count = 4 + 2 * halo + 4
    start = gx * 4 - halo - 2 + 2 * n
    lines = []
    for m in range(count // 2):
        at = lax.rem(lax.div(start, 2) + m, n)
        line = s3[lax.rem(at, x3)]
        lines.append(pltpu.roll(line, lax.rem(LANES - lax.div(at, x3), LANES), 1))
    e = dot(jnp.concatenate(lines, axis=0), pick_matrix(lambda o: o // 4 * 4)).reshape(count // 2, rows // 2, LANES)
    p2[pl.ds(0, count // 2), pl.ds(0, rows // 2, stride=2), :] = e
    p2[pl.ds(0, count // 2), pl.ds(1, rows // 2, stride=2), :] = e
    even = lax.rem(iota((rows, LANES), 1), 2) == 0
    for m in range(count):
        at = lax.rem(start + m, 2 * n)
        i, lower = 1 + lax.rem(at, n), at < n
        whole = []
        for ref in (v2, f2):
            line = ref[i]
            moved = pltpu.roll(line, jnp.where(lower, 1, LANES - 1), 1)
            whole.append(jnp.where(even == lower, line, moved))
        a2[m] = whole[0] + p2[m // 2]
        t2[m] = whole[1]
    for m in range(1, count - 1):
        nb = beside_2(a2[m], a2[m - 1], a2[m + 1])
        b2[m] = relaxed(2, t2[m], a2[m], nb)
    for m in range(2, count - 2):
        nb = beside_2(b2[m], b2[m - 1], b2[m + 1])
        near[m - 2] = relaxed(2, t2[m], b2[m], nb)


def add_from_2(v1, near, y2, p1, gy, core, halo):
    layers = 4 + 2 * halo
    rows, n = sizes_2()[1:]
    for m in range(layers):
        y2[m, pl.ds(0, rows), :] = near[m]
        y2[m, pl.ds(rows, rows), :] = near[m]
    start = pl.multiple_of(lax.rem(gy * 8 + rows - 4, rows), 4)
    picked = jnp.concatenate([y2[m, pl.ds(start, 16), :] for m in range(layers)], axis=0)
    e = dot(picked, pick_matrix(lambda o: 2 * lax.rem(lax.div(o, 2) + n // 2 * core, n))).reshape(layers, 16, LANES)
    p1[pl.ds(0, layers), pl.ds(0, 16, stride=2), :] = e
    p1[pl.ds(0, layers), pl.ds(1, 16, stride=2), :] = e
    for m in range(2 * layers):
        i = X1 - 2 * halo + m
        v1[i, pl.ds(Y1 - 8, 32), :] = v1[i, pl.ds(Y1 - 8, 32), :] + p1[m // 2]


def add_from_1(w, v, v1, p0, halo, x_at, y_from, skip, rows):
    for m in range(BX // 2 + 2 * halo):
        e = v1[X1 - halo + m, pl.ds(Y1 - 8, 32), :]
        p0[m, pl.ds(0, 32, stride=2), :] = e
        p0[m, pl.ds(1, 32, stride=2), :] = e
    for x in range(-2 * halo, BX + 2 * halo):
        for h in range(2):
            w[h][X0 + x, pl.ds(Y0 - skip, rows), :] = (
                v[h][x_at + x, pl.ds(y_from, rows), :] + p0[x // 2 + halo, pl.ds(16 - skip, rows), :]
            )


def lay_out_1(dst, f1, edges, core, own, width):
    up, down = edges[0][...], edges[1][...]
    other_up, other_down = (pltpu.roll(edge[...], 64, 1) for edge in edges[2:])
    first = core == 0
    x_low, y_low = jnp.where(first, up, other_up), jnp.where(first, other_up, up)
    x_high, y_high = jnp.where(first, down, other_down), jnp.where(first, other_down, down)
    for m in range(f1.shape[0]):
        i = X1 - own + m
        dst[i, pl.ds(Y1 - 4, 24), :] = f1[m]
        dst[i, pl.ds(Y1 - own - width, width), :] = y_low[m * width : (m + 1) * width]
        dst[i, pl.ds(Y1 + 16 + own, width), :] = y_high[m * width : (m + 1) * width]
    for m in range(width):
        dst[X1 - own - width + m, pl.ds(Y1 - 4, 24), :] = x_low[m * 24 : (m + 1) * 24]
        dst[X1 + 8 + own + m, pl.ds(Y1 - 4, 24), :] = x_high[m * 24 : (m + 1) * 24]


def put_out_1(out, up, down, f1, core, own, width):
    for m in range(out.shape[0]):
        out[m] = f1[X1 - own + m, pl.ds(Y1 - 4, 24), :]

    @pl.when(core == 0)
    def _():
        for m in range(width):
            up[pl.ds(m * 24, 24), :] = f1[X1 + 8 - own - width + m, pl.ds(Y1 - 4, 24), :]
            down[pl.ds(m * 24, 24), :] = f1[X1 + own + m, pl.ds(Y1 - 4, 24), :]

    @pl.when(core == 1)
    def _():
        for m in range(out.shape[0]):
            up[pl.ds(m * width, width), :] = f1[X1 - own + m, pl.ds(Y1 + 16 - own - width, width), :]
            down[pl.ds(m * width, width), :] = f1[X1 - own + m, pl.ds(Y1 + own, width), :]


def split_kernel(charge, mine, up, down):
    matrix = pick_matrix(lambda o: jnp.where(o < 64, 2 * o, 2 * o - 127))
    split = dot(flat(charge[...]), matrix).reshape(BX, BY, LANES)
    mine[...] = split
    up[...] = split[BX - HALO :]
    down[...] = split[:HALO]


def edges_kernel(mine, x_low, x_high, up, down):
    at = 0
    for ref in (x_low, mine, x_high):
        for i in range(ref.shape[0]):
            down[pl.ds(at * HALO, HALO), :] = ref[i, pl.ds(0, HALO), :]
            up[pl.ds(at * HALO, HALO), :] = ref[i, pl.ds(BY - HALO, HALO), :]
            at += 1


def lay_out_0(even, odd, ours, others):
    def both(p, q):
        low = iota(p.shape, p.ndim - 1) < 64
        return (
            jnp.where(low, p, pltpu.roll(q, 64, p.ndim - 1)),
            jnp.where(low, pltpu.roll(p, 64, p.ndim - 1), q),
        )

    at = X0 - HALO
    for k in (1, 0, 2):
        for m in range(ours[k].shape[0]):
            e, o = both(ours[k][m], others[k][m])
            even[at, pl.ds(Y0, BY), :] = e
            odd[at, pl.ds(Y0, BY), :] = o
            at += 1
    for k, row in ((3, Y0 - HALO), (4, Y0 + BY)):
        e, o = both(ours[k][...], others[k][...])
        for m in range(BX + 2 * HALO):
            even[X0 - HALO + m, pl.ds(row, HALO), :] = e[m * HALO : (m + 1) * HALO]
            odd[X0 - HALO + m, pl.ds(row, HALO), :] = o[m * HALO : (m + 1) * HALO]


def first_kernel(where, *refs):
    ours, others, refs = refs[0:5], refs[5:10], refs[10:]
    (f_e, f_o, v_e, v_o, send), f1_outs, (f1, v1, r1, t0) = refs[:5], refs[5:8], refs[8:]
    core = where()[2]
    force, v = (f_e, f_o), (v_e, v_o)
    lay_out_0(f_e, f_o, ours, others)
    start_0(v, force, 9, 17)
    restrict_0(f1, t0, v, force, 4)
    coarse_source(send, f1, v1, r1, core)
    put_out_1(*f1_outs, f1, core, 4, 4)


def middle_kernel(where, *refs):
    bottom, f_e, f_o, v_e, v_o, f1_in, mine, other, *edges = refs[:12]
    (n_e, n_o, send), f1_outs = refs[12:15], refs[15:18]
    a_e, a_o, b_e, b_o, f1, v1, r1, p1, y2, p0, t0, f2, v2, t2, t3, s3, p2, a2, b2, near = refs[18:]
    gx, gy, core = where()
    force, v, a0, b0 = (f_e, f_o), (v_e, v_o), (a_e, a_o), (b_e, b_o)
    unpack_2(f2, mine, other, core)
    level_2(near, f2, v2, t2, t3, s3, p2, a2, b2, bottom, gx, 4)
    lay_out_1(f1, f1_in, edges, core, 4, 4)
    start_1(v1, f1, 7, 12)
    add_from_2(v1, near, y2, p1, gy, core, 4)
    sweep_1(r1, v1, f1, 6, 12)
    sweep_1(v1, r1, f1, 5, 9)
    add_from_1(a0, v, v1, p0, 5, X0, Y0 - 16, 16, 64)
    sweep_0(b0, a0, force, 8, 16)
    sweep_0(a0, b0, force, 7, 15)
    sweep_0(b0, a0, force, 6, 14)
    sweep_0(a0, b0, force, 5, 13)
    restrict_0(f1, t0, a0, force, 2)
    coarse_source(send, f1, v1, r1, core)
    put_out_1(*f1_outs, f1, core, 2, 2)
    for src, dst in ((a_e, n_e), (a_o, n_o)):
        dst[...] = src[pl.ds(X0 - 2, 20), pl.ds(Y0 - 8, 48), :]


def last_kernel(where, *refs):
    bottom, f_e, f_o, n_e, n_o, f1_in, mine, other, *edges = refs[:12]
    out, a_e, a_o, b_e, b_o, f1, v1, r1, p1, y2, p0, _, f2, v2, t2, t3, s3, p2, a2, b2, near, held, left = refs[12:]
    gx, gy, core = where()
    force, v, a0, b0 = (f_e, f_o), (n_e, n_o), (a_e, a_o), (b_e, b_o)
    unpack_2(f2, mine, other, core)
    level_2(near, f2, v2, t2, t3, s3, p2, a2, b2, bottom, gx, 2)
    lay_out_1(f1, f1_in, edges, core, 2, 2)
    start_1(v1, f1, 3, 14)
    add_from_2(v1, near, y2, p1, gy, core, 2)
    sweep_1(r1, v1, f1, 2, 12)
    sweep_1(v1, r1, f1, 1, 10)
    add_from_1(a0, v, v1, p0, 1, 2, 0, 8, 48)
    sweep_0(b0, a0, force, 1, 9)
    low = iota((BY, LANES), 1) < 64
    matrix = pick_matrix(lambda o: lax.div(o, 2) + 64 * lax.rem(o, 2))
    pieces = [pl.ds(4 * k, 4) for k in range(BX // 4)]
    stores = [pltpu.make_async_copy(held.at[p], out.at[p], left.at[k]) for k, p in enumerate(pieces)]
    for k, store in enumerate(stores):
        lines = []
        for i in range(X0 + 4 * k, X0 + 4 * k + 4):
            centre, nb = beside_0(b0, i, Y0, BY)
            even, odd = (relaxed(0, force[h][i, pl.ds(Y0, BY), :], centre[h], nb[h]) for h in range(2))
            lines.append(jnp.where(low, even, pltpu.roll(odd, 64, 1)))
        held[pieces[k]] = dot(jnp.concatenate(lines, axis=0), matrix).reshape(4, BY, LANES)
        store.start()
    for store in stores:
        store.wait()


def vm(*shape):
    return pltpu.VMEM(shape, F32)


def kept(*shape):
    return jax.ShapeDtypeStruct(shape, F32)


def scratch_for_cycle():
    x2, y2, _ = sizes_2()
    return (
        [vm(XA0, YA0, LANES)] * 4
        + [vm(XA1, YA1, LANES)] * 3
        + [vm(12, y2, LANES), vm(12, 2 * y2, LANES), vm(20, 64, LANES), vm(16, 48, LANES)]
        + [vm(x2 // 2 + 2, y2, LANES)] * 2
        + [vm(16, y2, LANES), vm(x2 // 16, y2 // 2, LANES), vm(x2 // 8, y2 // 2, LANES), vm(8, y2, LANES)]
        + [vm(16, y2, LANES)] * 2
        + [vm(12, y2, LANES)]
    )


def run(kernel, outs, scratch, flops, *args, out_space=pltpu.VMEM):
    spec = pl.BlockSpec(memory_space=out_space)
    return pl.pallas_call(
        kernel,
        out_shape=outs,
        out_specs=[spec] * len(outs) if isinstance(outs, list) else spec,
        scratch_shapes=scratch,
        compiler_params=pltpu.CompilerParams(vmem_limit_bytes=40 * 2**20),
        cost_estimate=pl.CostEstimate(flops=flops, bytes_accessed=2**20, transcendentals=0),
    )(*args)


def where_am_i():
    return lax.axis_index("gx"), lax.axis_index("gy"), lax.axis_index("gz")


def sources_out(layers, width):
    return [kept(peers(), 8, LANES), kept(layers, 24, LANES)] + [kept(width * 24, LANES)] * 2


def peers():
    return lax.axis_size("gx") * lax.axis_size("gy")


def split(charge):
    return run(split_kernel, [kept(BX, BY, LANES)] + [kept(HALO, BY, LANES)] * 2, [], 10**6, charge)


def edges(*args):
    return run(edges_kernel, [kept((BX + 2 * HALO) * HALO, LANES)] * 2, [], 10**6, *args)


def first(*args):
    outs = [kept(XA0, YA0, LANES)] * 4 + sources_out(16, 4)
    scratch = [vm(XA1, YA1, LANES)] * 3 + [vm(16, 48, LANES)]
    return run(functools.partial(first_kernel, where_am_i), outs, scratch, 10**7, *args)


def middle(*args):
    outs = [kept(20, 48, LANES)] * 2 + sources_out(12, 2)
    return run(functools.partial(middle_kernel, where_am_i), outs, scratch_for_cycle(), 4 * 10**7, *args)


def last(*args):
    outs = kept(BX, BY, LANES)
    scratch = scratch_for_cycle() + [vm(BX, BY, LANES), pltpu.SemaphoreType.DMA((BX // 4,))]
    return run(functools.partial(last_kernel, where_am_i), outs, scratch, 2 * 10**7, *args, out_space=pltpu.HBM)


def from_(value, axis, step):
    size = lax.axis_size(axis)
    return lax.ppermute(value, axis, [(i, (i + step) % size) for i in range(size)])


def beside_(value, step):
    axes = ("gx", "gy", "gz")
    sizes = [lax.axis_size(axis) for axis in axes]
    pairs = []
    for device in np.ndindex(*sizes):
        to = list(device)
        to[device[2]] = (to[device[2]] + step) % sizes[device[2]]
        pairs.append((int(np.ravel_multi_index(device, sizes)), int(np.ravel_multi_index(to, sizes))))
    return lax.ppermute(value, axes, pairs)


def exchange(send, f1, up, down):
    up, down = beside_(up, 1), beside_(down, -1)
    mine = lax.all_to_all(send, ("gx", "gy"), 0, 0, tiled=True)
    other, other_up, other_down = (from_(v, "gz", 1) for v in (mine, up, down))
    return f1, mine, other, up, down, other_up, other_down


def local(charge):
    mine, up, down = split(charge)
    x_low, x_high = from_(up, "gx", 1), from_(down, "gx", -1)
    up, down = edges(mine, x_low, x_high)
    y_low, y_high = from_(up, "gy", 1), from_(down, "gy", -1)
    ours = (mine, x_low, x_high, y_low, y_high)
    others = [from_(v, "gz", 1) for v in ours]
    f_e, f_o, v_e, v_o, *rest = first(*ours, *others)
    bottom = jnp.asarray(bottom_matrix(bottom_shape()))
    n_e, n_o, *rest = middle(bottom, f_e, f_o, v_e, v_o, *exchange(*rest))
    return last(bottom, f_e, f_o, n_e, n_o, *exchange(*rest))


def solution(mesh):
    return jax.shard_map(
        local,
        mesh=mesh,
        in_specs=(P(("groups", "gx"), "gy", "gz"),),
        out_specs=P(("groups", "gx"), "gy", "gz"),
        check_vma=False,
    )
```

```python
import functools

import jax
import jax.numpy as jnp
import numpy as np
from jax import lax
from jax.experimental import pallas as pl
from jax.experimental.pallas import tpu as pltpu
from jax.sharding import PartitionSpec as P

LEVELS = 7
LANES = 128
OMEGA = 2.0 / 3.0
SCREEN = 0.001
F32 = jnp.float32

BX, BY = 16, 32
X0, Y0, XA0, YA0 = 12, 24, 40, 80
X1, Y1, XA1, YA1 = 10, 16, 32, 48
HALO = 10
EDGES = (((4, 4), (4, 4)), ((1, 3), (2, 2)))


def coefficients(level):
    a = 0.25**level
    return a, OMEGA / (6.0 * a + SCREEN)


def residual_of(level, f, v, nb):
    a, _ = coefficients(level)
    apart = 6.0 * v - nb
    if level:
        apart = a * apart
    return (f - apart) - SCREEN * v


def relaxed(level, f, v, nb):
    return v + coefficients(level)[1] * residual_of(level, f, v, nb)


def twice_from_zero(level, f, nb):
    a, k = coefficients(level)
    return (2.0 * k - k * k * SCREEN) * f - (k * k * a) * (6.0 * f - nb)


def iota(shape, dim):
    return lax.broadcasted_iota(jnp.int32, shape, dim)


def parts(v):
    high = v.astype(jnp.bfloat16)
    rest = v - high.astype(F32)
    middle = rest.astype(jnp.bfloat16)
    return high, middle, (rest - middle.astype(F32)).astype(jnp.bfloat16)


def product(a, b):
    return lax.dot_general(a, b, (((1,), (0,)), ((), ())), preferred_element_type=F32)


def dot(a, b):
    b = b.astype(jnp.bfloat16)
    high, middle, low = (product(p, b) for p in parts(a))
    return high + (middle + low)


def over_layers(start, count, block, body):
    def step(b, carry):
        for u in range(block):
            body(start + b * block + u)
        return carry

    lax.fori_loop(0, -(-count // block), step, 0)


def beside_0(refs, i, j, rows):
    even, odd = (r[i, pl.ds(j, rows), :] for r in refs)
    along_z = odd + pltpu.roll(odd, 1, 1), even + pltpu.roll(even, LANES - 1, 1)
    out = []
    for r, z in zip(refs, along_z):
        out.append(
            (r[i - 1, pl.ds(j, rows), :] + r[i + 1, pl.ds(j, rows), :])
            + (r[i, pl.ds(j - 1, rows), :] + r[i, pl.ds(j + 1, rows), :])
            + z
        )
    return (even, odd), out


def sweep_0(dst, src, force, halo, block):
    def body(i):
        for j in range(Y0 - 8, Y0 + 40, 16):
            centre, nb = beside_0(src, i, j, 16)
            for h in range(2):
                dst[h][i, pl.ds(j, 16), :] = relaxed(0, force[h][i, pl.ds(j, 16), :], centre[h], nb[h])

    over_layers(X0 - halo, BX + 2 * halo, block, body)


def start_0(dst, force, halo, block):
    def body(i):
        for j in range(Y0 - 16, Y0 + 48, 16):
            centre, nb = beside_0(force, i, j, 16)
            for h in range(2):
                dst[h][i, pl.ds(j, 16), :] = twice_from_zero(0, centre[h], nb[h])

    over_layers(X0 - halo, BX + 2 * halo, block, body)


def restrict_0(f1, t0, v, force, halo):
    rows = BY + 4 * halo

    def body(q):
        for y in range(0, rows, 16):
            count = min(16, rows - y)
            j = Y0 - 2 * halo + y
            total = None
            for i in (X0 - 2 * halo + 2 * q, X0 - 2 * halo + 2 * q + 1):
                centre, nb = beside_0(v, i, j, count)
                for h in range(2):
                    r = residual_of(0, force[h][i, pl.ds(j, count), :], centre[h], nb[h])
                    total = r if total is None else total + r
            t0[q, pl.ds(y, count), :] = total

    layers = BX // 2 + 2 * halo
    over_layers(0, layers, layers // 2, body)
    for m in range(layers):
        pairs = [t0[m, pl.ds(k, rows // 2, stride=2), :] for k in range(2)]
        f1[X1 - halo + m, pl.ds(Y1 - halo, rows // 2), :] = 0.125 * (pairs[0] + pairs[1])


def mean_matrix(source_of_out, gap=1):
    source, out = iota((LANES, LANES), 0), source_of_out(iota((LANES, LANES), 1))
    return jnp.where((source == out) | (source == out + gap), 0.125, 0.0).astype(F32)


def pick_matrix(source_of_out):
    return jnp.where(iota((LANES, LANES), 0) == source_of_out(iota((LANES, LANES), 1)), 1.0, 0.0).astype(F32)


def beside_1(ref, i, j, rows):
    centre = ref[i, pl.ds(j, rows), :]
    nb = (
        (ref[i - 1, pl.ds(j, rows), :] + ref[i + 1, pl.ds(j, rows), :])
        + (ref[i, pl.ds(j - 1, rows), :] + ref[i, pl.ds(j + 1, rows), :])
        + (pltpu.roll(centre, 1, 1) + pltpu.roll(centre, LANES - 1, 1))
    )
    return centre, nb


def sweep_1(dst, src, force, halo, block):
    def body(i):
        centre, nb = beside_1(src, i, Y1 - 8, 32)
        dst[i, pl.ds(Y1 - 8, 32), :] = relaxed(1, force[i, pl.ds(Y1 - 8, 32), :], centre, nb)

    over_layers(X1 - halo, BX // 2 + 2 * halo, block, body)


def start_1(dst, force, halo, block):
    def body(i):
        centre, nb = beside_1(force, i, Y1 - 8, 32)
        dst[i, pl.ds(Y1 - 8, 32), :] = twice_from_zero(1, centre, nb)

    over_layers(X1 - halo, BX // 2 + 2 * halo, block, body)


def sizes_2():
    return lax.axis_size("gx") * BX // 4, lax.axis_size("gy") * BY // 4, lax.axis_size("gz") * LANES // 4


def bottom_shape():
    return tuple(n // 8 for n in sizes_2())


def coarse_source(out, f1, v1, r1, core):
    start_1(v1, f1, 1, 10)

    def body(i):
        centre, nb = beside_1(v1, i, Y1, 16)
        r1[i, pl.ds(Y1, 16), :] = residual_of(1, f1[i, pl.ds(Y1, 16), :], centre, nb)

    over_layers(X1, BX // 2, 8, body)
    layers = []
    for q in range(4):
        i = X1 + 2 * q
        s = (r1[i, pl.ds(Y1, 8, stride=2), :] + r1[i, pl.ds(Y1 + 1, 8, stride=2), :]) + (
            r1[i + 1, pl.ds(Y1, 8, stride=2), :] + r1[i + 1, pl.ds(Y1 + 1, 8, stride=2), :]
        )
        layers.append(jnp.where(core == 0, s[0:4], s[4:8]))
    n = sizes_2()[2]
    at = lambda o: 2 * lax.rem(o // 2 + n // 2 * core, n)
    low = mean_matrix(lambda o: jnp.where(lax.rem(o, 2) == 0, at(o), -2))
    high = mean_matrix(lambda o: jnp.where(lax.rem(o, 2) == 1, at(o), -2))
    packed = dot(jnp.concatenate(layers[0:2], axis=0), low) + dot(jnp.concatenate(layers[2:4], axis=0), high)
    for s in range(out.shape[0]):
        out[s] = packed


def along_z(v, step, parts):
    axis = v.ndim - 1
    return pltpu.roll(v, step * parts, axis) + pltpu.roll(v, LANES - step * parts, axis)


def next_part(v, parts, ahead):
    if parts == 1:
        return v
    axis = v.ndim - 1
    q = lax.rem(iota(v.shape, axis), parts)
    if ahead:
        return jnp.where(q == 0, pltpu.roll(v, LANES + 1 - parts, axis), pltpu.roll(v, 1, axis))
    return jnp.where(q == parts - 1, pltpu.roll(v, parts - 1, axis), pltpu.roll(v, LANES - 1, axis))


def across(v, parts):
    last, rows = v.shape[0] - 1, v.shape[1]
    up = jnp.concatenate([next_part(v[last:], parts, True), v[:last]], axis=0)
    down = jnp.concatenate([v[1:], next_part(v[:1], parts, False)], axis=0)
    return (up + down) + (pltpu.roll(v, 1, 1) + pltpu.roll(v, rows - 1, 1))


def applied(level, v, parts):
    a, _ = coefficients(level)
    z1, z2 = along_z(v, 1, parts), along_z(v, 2, parts)
    one = across(v, parts)
    sv = one + z1
    ssv = across(one + 2.0 * z1, parts) + (z2 + 2.0 * v)
    t = 6.0 * v - sv
    tt = 6.0 * t - (6.0 * sv - ssv)
    return t, a * t + SCREEN * v, (a * a) * tt + (2.0 * a * SCREEN) * t + (SCREEN * SCREEN) * v


def start_whole(level, f, parts=1):
    a, k = coefficients(level)
    t, af, aaf = applied(level, f, parts)
    return (2.0 * k - k * k * SCREEN) * f - (k * k * a) * t, f - 2.0 * k * af + (k * k) * aaf, af


def smooth_whole(level, f, af, v, parts=1):
    a, k = coefficients(level)
    t, _, aav = applied(level, v, parts)
    r = (f - a * t) - SCREEN * v
    return v + 2.0 * k * r - (k * k) * (af - aav)


def bottom_matrix(shape):
    def beside(v):
        return sum(np.roll(v, step, axis) for axis in (1, 2, 3) for step in (1, -1))

    def residual(level, f, v):
        return f - ((6.0 * v - beside(v)) * 0.25**level + SCREEN * v)

    def cycle(level, f):
        v = np.zeros_like(f)
        for _ in range(2):
            v = v + OMEGA * residual(level, f, v) / (6.0 * 0.25**level + SCREEN)
        if level == LEVELS - 1:
            return v
        n, x, y, z = f.shape
        coarse = residual(level, f, v).reshape(n, x // 2, 2, y // 2, 2, z // 2, 2).mean(axis=(2, 4, 6))
        v = v + cycle(level + 1, coarse).repeat(2, 1).repeat(2, 2).repeat(2, 3)
        for _ in range(2):
            v = v + OMEGA * residual(level, f, v) / (6.0 * 0.25**level + SCREEN)
        return v

    cells = shape[0] * shape[1] * shape[2]
    return cycle(5, np.eye(cells).reshape(cells, *shape)).reshape(cells, cells).astype(np.float32)


def pair_layers(v):
    v = v.reshape(v.shape[0] // 2, 2, *v.shape[1:])
    return v[:, 0] + v[:, 1]


def twice(v):
    return jnp.concatenate([v[:, None], v[:, None]], axis=1).reshape(2 * v.shape[0], *v.shape[1:])


def flat(v):
    return v.reshape(-1, LANES)


def solve_bottom(s, shape, matrix):
    x5, y5, z5 = shape
    cells = x5 * y5 * z5
    rows = s.shape[0]
    cell, row = iota((rows, cells), 1), iota((rows, cells), 0)
    mine = (cell // (y5 * z5) == row // (2 * y5)) & (lax.rem(cell // z5, y5) == lax.rem(row, 2 * y5) // 2)
    source, out = iota((LANES, cells), 0), lax.rem(iota((LANES, cells), 1), z5)
    means = jnp.where((source == 2 * out) | (source == 2 * out + 1), 0.125, 0.0).astype(F32)
    f5 = jnp.sum(jnp.where(mine, dot(s, means), 0.0), axis=0, keepdims=True)
    f_high, f_middle, f_low = parts(jnp.broadcast_to(f5, (8, cells)))
    m_high, m_middle, m_low = parts(matrix[...])
    v5 = product(f_high, m_high) + (
        (product(f_high, m_middle) + product(f_middle, m_high))
        + (product(f_high, m_low) + product(f_middle, m_middle) + product(f_low, m_high))
    )
    spread = jnp.where(mine, jnp.broadcast_to(v5[0:1], (rows, cells)), 0.0)
    source, out = lax.rem(iota((cells, LANES), 0), z5), lax.rem(iota((cells, LANES), 1), 2 * z5)
    return dot(spread, jnp.where(source == out // 2, 1.0, 0.0).astype(F32))


def solve_3(f3, t3, matrix):
    x4, y4 = f3.shape[0] // 2, f3.shape[1] // 2
    parts_3 = LANES // (sizes_2()[2] // 2)
    v3, r3, af3 = start_whole(3, f3, parts_3)
    t3[...] = pair_layers(r3)
    s = flat(t3[:, pl.ds(0, y4, stride=2), :] + t3[:, pl.ds(1, y4, stride=2), :])
    z4 = LANES // parts_3 // 2
    means = [mean_matrix(lambda o: 2 * parts_3 * lax.rem(o, z4) + q, parts_3) for q in range(parts_3)]
    f4 = jnp.concatenate([dot(s, m).reshape(x4, y4, LANES) for m in means], axis=0)
    v4, r4, af4 = start_whole(4, f4)
    e4 = solve_bottom(flat(pair_layers(r4)), bottom_shape(), matrix).reshape(-1, y4, LANES)
    v4 = smooth_whole(4, f4, af4, v4 + twice(e4))
    picks = [pick_matrix(lambda o: jnp.where(lax.rem(o, parts_3) == q, o // parts_3 // 2, -1)) for q in range(parts_3)]
    e3 = sum(dot(flat(v4[x4 * q : x4 * (q + 1)]), m) for q, m in enumerate(picks)).reshape(x4, y4, LANES)
    t3[:, pl.ds(0, y4, stride=2), :] = e3
    t3[:, pl.ds(1, y4, stride=2), :] = e3
    return smooth_whole(3, f3, af3, v3 + twice(t3[...]), parts_3)


def unpack_2(f2, mine, other, core):
    even = lax.rem(iota((8, LANES), 1), 2) == 0
    top = iota((8, LANES), 0) < 4
    along_y = lax.axis_size("gy")
    half = (f2.shape[0] - 2) // 4

    def body(gx):
        for gy in range(along_y):
            tiles = []
            for g in (gx, gx + half):
                t, p = mine[g * along_y + gy], other[g * along_y + gy]
                u, w = jnp.where(core == 0, t, p), jnp.where(core == 0, p, t)
                tiles.append((u, w))
            (u, w), (u2, w2) = tiles
            for xp in range(2):
                if xp == 0:
                    d, e = jnp.where(even, u, pltpu.roll(u2, 1, 1)), jnp.where(even, w, pltpu.roll(w2, 1, 1))
                else:
                    d, e = jnp.where(even, pltpu.roll(u, LANES - 1, 1), u2), jnp.where(even, pltpu.roll(w, LANES - 1, 1), w2)
                f2[1 + gx * 4 + 2 * xp, pl.ds(gy * 8, 8), :] = jnp.where(top, d, pltpu.roll(e, 4, 0))
                f2[2 + gx * 4 + 2 * xp, pl.ds(gy * 8, 8), :] = jnp.where(top, pltpu.roll(d, 4, 0), e)

    over_layers(0, half, 4, body)


def close_2(v):
    last = v.shape[0] - 2
    v[0] = next_part(v[last], 2, True)
    v[last + 1] = next_part(v[1], 2, False)


def beside_2(centre, before, after):
    rows = centre.shape[0]
    return (
        (before + after) + (pltpu.roll(centre, 1, 0) + pltpu.roll(centre, rows - 1, 0)) + along_z(centre, 1, 2)
    )


def level_2(near, f2, v2, t2, t3, s3, p2, a2, b2, bottom, gx, halo):
    n, rows = f2.shape[0] - 2, f2.shape[1]
    close_2(f2)

    def first(i):
        v2[i] = twice_from_zero(2, f2[i], beside_2(f2[i], f2[i - 1], f2[i + 1]))

    over_layers(1, n, 16, first)
    close_2(v2)

    def second(q):
        pair = []
        for i in (2 * q + 1, 2 * q + 2):
            pair.append(residual_of(2, f2[i], v2[i], beside_2(v2[i], v2[i - 1], v2[i + 1])))
        t2[q] = pair[0] + pair[1]

    over_layers(0, n // 2, 8, second)
    s = t2[:, pl.ds(0, rows // 2, stride=2), :] + t2[:, pl.ds(1, rows // 2, stride=2), :]
    x3 = n // 4

    def means(part):
        def source(o):
            q = lax.rem(o, 4)
            return jnp.where(lax.rem(q, 2) == part, o // 4 * 4 + q // 2, -4)

        return mean_matrix(source, 2)

    f3 = dot(flat(s[:x3]), means(0)) + dot(flat(s[x3:]), means(1))
    s3[...] = solve_3(f3.reshape(x3, rows // 2, LANES), t3, bottom)

    count = 4 + 2 * halo + 4
    start = gx * 4 - halo - 2 + 2 * n
    lines = []
    for m in range(count // 2):
        at = lax.rem(lax.div(start, 2) + m, n)
        line = s3[lax.rem(at, x3)]
        lines.append(pltpu.roll(line, lax.rem(LANES - lax.div(at, x3), LANES), 1))
    e = dot(jnp.concatenate(lines, axis=0), pick_matrix(lambda o: o // 4 * 4)).reshape(count // 2, rows // 2, LANES)
    p2[pl.ds(0, count // 2), pl.ds(0, rows // 2, stride=2), :] = e
    p2[pl.ds(0, count // 2), pl.ds(1, rows // 2, stride=2), :] = e
    even = lax.rem(iota((rows, LANES), 1), 2) == 0
    for m in range(count):
        at = lax.rem(start + m, 2 * n)
        i, lower = 1 + lax.rem(at, n), at < n
        whole = []
        for ref in (v2, f2):
            line = ref[i]
            moved = pltpu.roll(line, jnp.where(lower, 1, LANES - 1), 1)
            whole.append(jnp.where(even == lower, line, moved))
        a2[m] = whole[0] + p2[m // 2]
        t2[m] = whole[1]
    for m in range(1, count - 1):
        nb = beside_2(a2[m], a2[m - 1], a2[m + 1])
        b2[m] = relaxed(2, t2[m], a2[m], nb)
    for m in range(2, count - 2):
        nb = beside_2(b2[m], b2[m - 1], b2[m + 1])
        near[m - 2] = relaxed(2, t2[m], b2[m], nb)


def add_from_2(v1, near, y2, p1, gy, core, halo):
    layers = 4 + 2 * halo
    rows, n = sizes_2()[1:]
    for m in range(layers):
        y2[m, pl.ds(0, rows), :] = near[m]
        y2[m, pl.ds(rows, rows), :] = near[m]
    start = pl.multiple_of(lax.rem(gy * 8 + rows - 4, rows), 4)
    picked = jnp.concatenate([y2[m, pl.ds(start, 16), :] for m in range(layers)], axis=0)
    e = dot(picked, pick_matrix(lambda o: 2 * lax.rem(lax.div(o, 2) + n // 2 * core, n))).reshape(layers, 16, LANES)
    p1[pl.ds(0, layers), pl.ds(0, 16, stride=2), :] = e
    p1[pl.ds(0, layers), pl.ds(1, 16, stride=2), :] = e
    for m in range(2 * layers):
        i = X1 - 2 * halo + m
        v1[i, pl.ds(Y1 - 8, 32), :] = v1[i, pl.ds(Y1 - 8, 32), :] + p1[m // 2]


def add_from_1(w, v, v1, p0, halo, x_at, y_from, skip, rows):
    for m in range(BX // 2 + 2 * halo):
        e = v1[X1 - halo + m, pl.ds(Y1 - 8, 32), :]
        p0[m, pl.ds(0, 32, stride=2), :] = e
        p0[m, pl.ds(1, 32, stride=2), :] = e
    for x in range(-2 * halo, BX + 2 * halo):
        for h in range(2):
            w[h][X0 + x, pl.ds(Y0 - skip, rows), :] = (
                v[h][x_at + x, pl.ds(y_from, rows), :] + p0[x // 2 + halo, pl.ds(16 - skip, rows), :]
            )


def lay_out_1(dst, f1, edges, core, own, x_edges, y_edges):
    up, down = edges[0][...], edges[1][...]
    other_up, other_down = (pltpu.roll(edge[...], 64, 1) for edge in edges[2:])
    first = core == 0
    x_low, y_low = jnp.where(first, up, other_up), jnp.where(first, other_up, up)
    x_high, y_high = jnp.where(first, down, other_down), jnp.where(first, other_down, down)
    past, width = y_edges
    for m in range(f1.shape[0]):
        i = X1 - own + m
        dst[i, pl.ds(Y1 - 4, 24), :] = f1[m]
        dst[i, pl.ds(Y1 - past - width, width), :] = y_low[m * width : (m + 1) * width]
        dst[i, pl.ds(Y1 + 16 + past, width), :] = y_high[m * width : (m + 1) * width]
    past, width = x_edges
    for m in range(width):
        known = slice(m * 24 + 4 - own, m * 24 + 20 + own)
        dst[X1 - past - width + m, pl.ds(Y1 - own, 16 + 2 * own), :] = x_low[known]
        dst[X1 + 8 + past + m, pl.ds(Y1 - own, 16 + 2 * own), :] = x_high[known]


def put_out_1(out, up, down, f1, core, own, x_edges, y_edges):
    for m in range(out.shape[0]):
        out[m] = f1[X1 - own + m, pl.ds(Y1 - 4, 24), :]

    @pl.when(core == 0)
    def _():
        past, width = x_edges
        for m in range(width):
            up[pl.ds(m * 24, 24), :] = f1[X1 + 8 - past - width + m, pl.ds(Y1 - 4, 24), :]
            down[pl.ds(m * 24, 24), :] = f1[X1 + past + m, pl.ds(Y1 - 4, 24), :]

    @pl.when(core == 1)
    def _():
        past, width = y_edges
        for m in range(out.shape[0]):
            up[pl.ds(m * width, width), :] = f1[X1 - own + m, pl.ds(Y1 + 16 - past - width, width), :]
            down[pl.ds(m * width, width), :] = f1[X1 - own + m, pl.ds(Y1 + past, width), :]


def split_kernel(charge, mine, up, down):
    matrix = pick_matrix(lambda o: jnp.where(o < 64, 2 * o, 2 * o - 127))
    split = dot(flat(charge[...]), matrix).reshape(BX, BY, LANES)
    mine[...] = split
    up[...] = split[BX - HALO :]
    down[...] = split[:HALO]


def edges_kernel(mine, x_low, x_high, up, down):
    at = 0
    for ref in (x_low, mine, x_high):
        for i in range(ref.shape[0]):
            down[pl.ds(at * HALO, HALO), :] = ref[i, pl.ds(0, HALO), :]
            up[pl.ds(at * HALO, HALO), :] = ref[i, pl.ds(BY - HALO, HALO), :]
            at += 1


def lay_out_0(even, odd, ours, others):
    def both(p, q):
        low = iota(p.shape, p.ndim - 1) < 64
        return (
            jnp.where(low, p, pltpu.roll(q, 64, p.ndim - 1)),
            jnp.where(low, pltpu.roll(p, 64, p.ndim - 1), q),
        )

    at = X0 - HALO
    for k in (1, 0, 2):
        for m in range(ours[k].shape[0]):
            e, o = both(ours[k][m], others[k][m])
            even[at, pl.ds(Y0, BY), :] = e
            odd[at, pl.ds(Y0, BY), :] = o
            at += 1
    for k, row in ((3, Y0 - HALO), (4, Y0 + BY)):
        e, o = both(ours[k][...], others[k][...])
        for m in range(BX + 2 * HALO):
            even[X0 - HALO + m, pl.ds(row, HALO), :] = e[m * HALO : (m + 1) * HALO]
            odd[X0 - HALO + m, pl.ds(row, HALO), :] = o[m * HALO : (m + 1) * HALO]


def first_kernel(where, *refs):
    ours, others, refs = refs[0:5], refs[5:10], refs[10:]
    (f_e, f_o, v_e, v_o, send), f1_outs, (f1, v1, r1, t0) = refs[:5], refs[5:8], refs[8:]
    core = where()[2]
    force, v = (f_e, f_o), (v_e, v_o)
    lay_out_0(f_e, f_o, ours, others)
    start_0(v, force, 9, 17)
    restrict_0(f1, t0, v, force, 4)
    coarse_source(send, f1, v1, r1, core)
    put_out_1(*f1_outs, f1, core, 4, *EDGES[0])


def middle_kernel(where, *refs):
    bottom, f_e, f_o, v_e, v_o, f1_in, mine, other, *edges = refs[:12]
    (n_e, n_o, send), f1_outs = refs[12:15], refs[15:18]
    a_e, a_o, b_e, b_o, f1, v1, r1, p1, y2, p0, t0, f2, v2, t2, t3, s3, p2, a2, b2, near = refs[18:]
    gx, gy, core = where()
    force, v, a0, b0 = (f_e, f_o), (v_e, v_o), (a_e, a_o), (b_e, b_o)
    unpack_2(f2, mine, other, core)
    level_2(near, f2, v2, t2, t3, s3, p2, a2, b2, bottom, gx, 4)
    lay_out_1(f1, f1_in, edges, core, 4, *EDGES[0])
    start_1(v1, f1, 7, 12)
    add_from_2(v1, near, y2, p1, gy, core, 4)
    sweep_1(r1, v1, f1, 6, 12)
    sweep_1(v1, r1, f1, 5, 9)
    add_from_1(a0, v, v1, p0, 5, X0, Y0 - 16, 16, 64)
    sweep_0(b0, a0, force, 8, 16)
    sweep_0(a0, b0, force, 7, 15)
    sweep_0(b0, a0, force, 6, 14)
    sweep_0(a0, b0, force, 5, 13)
    restrict_0(f1, t0, a0, force, 2)
    coarse_source(send, f1, v1, r1, core)
    put_out_1(*f1_outs, f1, core, 2, *EDGES[1])
    for src, dst in ((a_e, n_e), (a_o, n_o)):
        dst[...] = src[pl.ds(X0 - 2, 20), pl.ds(Y0 - 8, 48), :]


def last_kernel(where, *refs):
    bottom, f_e, f_o, n_e, n_o, f1_in, mine, other, *edges = refs[:12]
    out, a_e, a_o, b_e, b_o, f1, v1, r1, p1, y2, p0, _, f2, v2, t2, t3, s3, p2, a2, b2, near, held, left = refs[12:]
    gx, gy, core = where()
    force, v, a0, b0 = (f_e, f_o), (n_e, n_o), (a_e, a_o), (b_e, b_o)
    unpack_2(f2, mine, other, core)
    level_2(near, f2, v2, t2, t3, s3, p2, a2, b2, bottom, gx, 2)
    lay_out_1(f1, f1_in, edges, core, 2, *EDGES[1])
    start_1(v1, f1, 3, 14)
    add_from_2(v1, near, y2, p1, gy, core, 2)
    sweep_1(r1, v1, f1, 2, 12)
    sweep_1(v1, r1, f1, 1, 10)
    add_from_1(a0, v, v1, p0, 1, 2, 0, 8, 48)
    sweep_0(b0, a0, force, 1, 9)
    low = iota((BY, LANES), 1) < 64
    matrix = pick_matrix(lambda o: lax.div(o, 2) + 64 * lax.rem(o, 2))
    pieces = [pl.ds(4 * k, 4) for k in range(BX // 4)]
    stores = [pltpu.make_async_copy(held.at[p], out.at[p], left.at[k]) for k, p in enumerate(pieces)]
    for k, store in enumerate(stores):
        lines = []
        for i in range(X0 + 4 * k, X0 + 4 * k + 4):
            centre, nb = beside_0(b0, i, Y0, BY)
            even, odd = (relaxed(0, force[h][i, pl.ds(Y0, BY), :], centre[h], nb[h]) for h in range(2))
            lines.append(jnp.where(low, even, pltpu.roll(odd, 64, 1)))
        held[pieces[k]] = dot(jnp.concatenate(lines, axis=0), matrix).reshape(4, BY, LANES)
        store.start()
    for store in stores:
        store.wait()


def vm(*shape):
    return pltpu.VMEM(shape, F32)


def kept(*shape):
    return jax.ShapeDtypeStruct(shape, F32)


def scratch_for_cycle():
    x2, y2, _ = sizes_2()
    return (
        [vm(XA0, YA0, LANES)] * 4
        + [vm(XA1, YA1, LANES)] * 3
        + [vm(12, y2, LANES), vm(12, 2 * y2, LANES), vm(20, 64, LANES), vm(16, 48, LANES)]
        + [vm(x2 // 2 + 2, y2, LANES)] * 2
        + [vm(16, y2, LANES), vm(x2 // 16, y2 // 2, LANES), vm(x2 // 8, y2 // 2, LANES), vm(8, y2, LANES)]
        + [vm(16, y2, LANES)] * 2
        + [vm(12, y2, LANES)]
    )


def run(kernel, outs, scratch, flops, *args, out_space=pltpu.VMEM):
    spec = pl.BlockSpec(memory_space=out_space)
    return pl.pallas_call(
        kernel,
        out_shape=outs,
        out_specs=[spec] * len(outs) if isinstance(outs, list) else spec,
        scratch_shapes=scratch,
        compiler_params=pltpu.CompilerParams(vmem_limit_bytes=40 * 2**20),
        cost_estimate=pl.CostEstimate(flops=flops, bytes_accessed=2**20, transcendentals=0),
    )(*args)


def where_am_i():
    return lax.axis_index("gx"), lax.axis_index("gy"), lax.axis_index("gz")


def sources_out(layers, width):
    return [kept(peers(), 8, LANES), kept(layers, 24, LANES)] + [kept(width * 24, LANES)] * 2


def peers():
    return lax.axis_size("gx") * lax.axis_size("gy")


def split(charge):
    return run(split_kernel, [kept(BX, BY, LANES)] + [kept(HALO, BY, LANES)] * 2, [], 10**6, charge)


def edges(*args):
    return run(edges_kernel, [kept((BX + 2 * HALO) * HALO, LANES)] * 2, [], 10**6, *args)


def first(*args):
    outs = [kept(XA0, YA0, LANES)] * 4 + sources_out(16, EDGES[0][0][1])
    scratch = [vm(XA1, YA1, LANES)] * 3 + [vm(16, 48, LANES)]
    return run(functools.partial(first_kernel, where_am_i), outs, scratch, 10**7, *args)


def middle(*args):
    outs = [kept(20, 48, LANES)] * 2 + sources_out(12, EDGES[1][0][1])
    return run(functools.partial(middle_kernel, where_am_i), outs, scratch_for_cycle(), 4 * 10**7, *args)


def last(*args):
    outs = kept(BX, BY, LANES)
    scratch = scratch_for_cycle() + [vm(BX, BY, LANES), pltpu.SemaphoreType.DMA((BX // 4,))]
    return run(functools.partial(last_kernel, where_am_i), outs, scratch, 2 * 10**7, *args, out_space=pltpu.HBM)


def from_(value, axis, step):
    size = lax.axis_size(axis)
    return lax.ppermute(value, axis, [(i, (i + step) % size) for i in range(size)])


def beside_(value, step):
    axes = ("gx", "gy", "gz")
    sizes = [lax.axis_size(axis) for axis in axes]
    pairs = []
    for device in np.ndindex(*sizes):
        to = list(device)
        to[device[2]] = (to[device[2]] + step) % sizes[device[2]]
        pairs.append((int(np.ravel_multi_index(device, sizes)), int(np.ravel_multi_index(to, sizes))))
    return lax.ppermute(value, axes, pairs)


def exchange(send, f1, up, down):
    up, down = beside_(up, 1), beside_(down, -1)
    mine = lax.all_to_all(send, ("gx", "gy"), 0, 0, tiled=True)
    other, other_up, other_down = (from_(v, "gz", 1) for v in (mine, up, down))
    return f1, mine, other, up, down, other_up, other_down


def local(charge):
    mine, up, down = split(charge)
    x_low, x_high = from_(up, "gx", 1), from_(down, "gx", -1)
    up, down = edges(mine, x_low, x_high)
    y_low, y_high = from_(up, "gy", 1), from_(down, "gy", -1)
    ours = (mine, x_low, x_high, y_low, y_high)
    others = [from_(v, "gz", 1) for v in ours]
    f_e, f_o, v_e, v_o, *rest = first(*ours, *others)
    bottom = jnp.asarray(bottom_matrix(bottom_shape()))
    n_e, n_o, *rest = middle(bottom, f_e, f_o, v_e, v_o, *exchange(*rest))
    return last(bottom, f_e, f_o, n_e, n_o, *exchange(*rest))


def solution(mesh):
    return jax.shard_map(
        local,
        mesh=mesh,
        in_specs=(P(("groups", "gx"), "gy", "gz"),),
        out_specs=P(("groups", "gx"), "gy", "gz"),
        check_vma=False,
    )
```

```python
import functools

import jax
import jax.numpy as jnp
import numpy as np
from jax import lax
from jax.experimental import pallas as pl
from jax.experimental.pallas import tpu as pltpu
from jax.sharding import PartitionSpec as P

LEVELS = 7
LANES = 128
OMEGA = 2.0 / 3.0
SCREEN = 0.001
F32 = jnp.float32

BX, BY = 16, 32
X0, Y0, XA0, YA0 = 12, 24, 40, 80
X1, Y1, XA1, YA1 = 10, 16, 32, 48
HALO = 10
EDGES = (((4, 4), (4, 4)), ((1, 3), (2, 2)))


def coefficients(level):
    a = 0.25**level
    return a, OMEGA / (6.0 * a + SCREEN)


def residual_of(level, f, v, nb):
    a, _ = coefficients(level)
    apart = 6.0 * v - nb
    if level:
        apart = a * apart
    return (f - apart) - SCREEN * v


def relaxed(level, f, v, nb):
    return v + coefficients(level)[1] * residual_of(level, f, v, nb)


def twice_from_zero(level, f, nb):
    a, k = coefficients(level)
    return (2.0 * k - k * k * SCREEN) * f - (k * k * a) * (6.0 * f - nb)


def iota(shape, dim):
    return lax.broadcasted_iota(jnp.int32, shape, dim)


def parts(v):
    high = v.astype(jnp.bfloat16)
    rest = v - high.astype(F32)
    middle = rest.astype(jnp.bfloat16)
    return high, middle, (rest - middle.astype(F32)).astype(jnp.bfloat16)


def product(a, b):
    return lax.dot_general(a, b, (((1,), (0,)), ((), ())), preferred_element_type=F32)


def dot(a, b):
    b = b.astype(jnp.bfloat16)
    high, middle, low = (product(p, b) for p in parts(a))
    return high + (middle + low)


def over_layers(start, count, block, body):
    def step(b, carry):
        for u in range(block):
            body(start + b * block + u)
        return carry

    lax.fori_loop(0, -(-count // block), step, 0)


def beside_0(refs, i, j, rows):
    even, odd = (r[i, pl.ds(j, rows), :] for r in refs)
    along_z = odd + pltpu.roll(odd, 1, 1), even + pltpu.roll(even, LANES - 1, 1)
    out = []
    for r, z in zip(refs, along_z):
        out.append(
            (r[i - 1, pl.ds(j, rows), :] + r[i + 1, pl.ds(j, rows), :])
            + (r[i, pl.ds(j - 1, rows), :] + r[i, pl.ds(j + 1, rows), :])
            + z
        )
    return (even, odd), out


def sweep_0(dst, src, force, halo, block):
    def body(i):
        for j in range(Y0 - 8, Y0 + 40, 16):
            centre, nb = beside_0(src, i, j, 16)
            for h in range(2):
                dst[h][i, pl.ds(j, 16), :] = relaxed(0, force[h][i, pl.ds(j, 16), :], centre[h], nb[h])

    over_layers(X0 - halo, BX + 2 * halo, block, body)


def start_0(dst, force, halo, block):
    def body(i):
        for j in range(Y0 - 16, Y0 + 48, 16):
            centre, nb = beside_0(force, i, j, 16)
            for h in range(2):
                dst[h][i, pl.ds(j, 16), :] = twice_from_zero(0, centre[h], nb[h])

    over_layers(X0 - halo, BX + 2 * halo, block, body)


def restrict_0(f1, t0, v, force, halo):
    def body(q):
        for j in range(Y0 - 8, Y0 + 40, 16):
            total = None
            for i in (X0 - 2 * halo + 2 * q, X0 - 2 * halo + 2 * q + 1):
                centre, nb = beside_0(v, i, j, 16)
                for h in range(2):
                    r = residual_of(0, force[h][i, pl.ds(j, 16), :], centre[h], nb[h])
                    total = r if total is None else total + r
            t0[q, pl.ds(j - Y0 + 8, 16), :] = total

    layers = BX // 2 + 2 * halo
    over_layers(0, layers, layers // 2, body)
    for m in range(layers):
        f1[X1 - halo + m, pl.ds(Y1 - 4, 24), :] = 0.125 * (t0[m, pl.ds(0, 24, stride=2), :] + t0[m, pl.ds(1, 24, stride=2), :])


def mean_matrix(source_of_out, gap=1):
    source, out = iota((LANES, LANES), 0), source_of_out(iota((LANES, LANES), 1))
    return jnp.where((source == out) | (source == out + gap), 0.125, 0.0).astype(F32)


def pick_matrix(source_of_out):
    return jnp.where(iota((LANES, LANES), 0) == source_of_out(iota((LANES, LANES), 1)), 1.0, 0.0).astype(F32)


def beside_1(ref, i, j, rows):
    centre = ref[i, pl.ds(j, rows), :]
    nb = (
        (ref[i - 1, pl.ds(j, rows), :] + ref[i + 1, pl.ds(j, rows), :])
        + (ref[i, pl.ds(j - 1, rows), :] + ref[i, pl.ds(j + 1, rows), :])
        + (pltpu.roll(centre, 1, 1) + pltpu.roll(centre, LANES - 1, 1))
    )
    return centre, nb


def sweep_1(dst, src, force, halo, block):
    def body(i):
        centre, nb = beside_1(src, i, Y1 - 8, 32)
        dst[i, pl.ds(Y1 - 8, 32), :] = relaxed(1, force[i, pl.ds(Y1 - 8, 32), :], centre, nb)

    over_layers(X1 - halo, BX // 2 + 2 * halo, block, body)


def start_1(dst, force, halo, block):
    def body(i):
        centre, nb = beside_1(force, i, Y1 - 8, 32)
        dst[i, pl.ds(Y1 - 8, 32), :] = twice_from_zero(1, centre, nb)

    over_layers(X1 - halo, BX // 2 + 2 * halo, block, body)


def sizes_2():
    return lax.axis_size("gx") * BX // 4, lax.axis_size("gy") * BY // 4, lax.axis_size("gz") * LANES // 4


def bottom_shape():
    return tuple(n // 8 for n in sizes_2())


def coarse_source(out, f1, v1, r1, core):
    start_1(v1, f1, 1, 10)

    def body(i):
        centre, nb = beside_1(v1, i, Y1, 16)
        r1[i, pl.ds(Y1, 16), :] = residual_of(1, f1[i, pl.ds(Y1, 16), :], centre, nb)

    over_layers(X1, BX // 2, 8, body)
    layers = []
    for q in range(4):
        i = X1 + 2 * q
        s = (r1[i, pl.ds(Y1, 8, stride=2), :] + r1[i, pl.ds(Y1 + 1, 8, stride=2), :]) + (
            r1[i + 1, pl.ds(Y1, 8, stride=2), :] + r1[i + 1, pl.ds(Y1 + 1, 8, stride=2), :]
        )
        layers.append(jnp.where(core == 0, s[0:4], s[4:8]))
    n = sizes_2()[2]
    at = lambda o: 2 * lax.rem(o // 2 + n // 2 * core, n)
    low = mean_matrix(lambda o: jnp.where(lax.rem(o, 2) == 0, at(o), -2))
    high = mean_matrix(lambda o: jnp.where(lax.rem(o, 2) == 1, at(o), -2))
    packed = dot(jnp.concatenate(layers[0:2], axis=0), low) + dot(jnp.concatenate(layers[2:4], axis=0), high)
    for s in range(out.shape[0]):
        out[s] = packed


def along_z(v, step, parts):
    axis = v.ndim - 1
    return pltpu.roll(v, step * parts, axis) + pltpu.roll(v, LANES - step * parts, axis)


def next_part(v, parts, ahead):
    if parts == 1:
        return v
    axis = v.ndim - 1
    q = lax.rem(iota(v.shape, axis), parts)
    if ahead:
        return jnp.where(q == 0, pltpu.roll(v, LANES + 1 - parts, axis), pltpu.roll(v, 1, axis))
    return jnp.where(q == parts - 1, pltpu.roll(v, parts - 1, axis), pltpu.roll(v, LANES - 1, axis))


def across(v, parts):
    last, rows = v.shape[0] - 1, v.shape[1]
    up = jnp.concatenate([next_part(v[last:], parts, True), v[:last]], axis=0)
    down = jnp.concatenate([v[1:], next_part(v[:1], parts, False)], axis=0)
    return (up + down) + (pltpu.roll(v, 1, 1) + pltpu.roll(v, rows - 1, 1))


def applied(level, v, parts):
    a, _ = coefficients(level)
    z1, z2 = along_z(v, 1, parts), along_z(v, 2, parts)
    one = across(v, parts)
    sv = one + z1
    ssv = across(one + 2.0 * z1, parts) + (z2 + 2.0 * v)
    t = 6.0 * v - sv
    tt = 6.0 * t - (6.0 * sv - ssv)
    return t, a * t + SCREEN * v, (a * a) * tt + (2.0 * a * SCREEN) * t + (SCREEN * SCREEN) * v


def start_whole(level, f, parts=1):
    a, k = coefficients(level)
    t, af, aaf = applied(level, f, parts)
    return (2.0 * k - k * k * SCREEN) * f - (k * k * a) * t, f - 2.0 * k * af + (k * k) * aaf, af


def smooth_whole(level, f, af, v, parts=1):
    a, k = coefficients(level)
    t, _, aav = applied(level, v, parts)
    r = (f - a * t) - SCREEN * v
    return v + 2.0 * k * r - (k * k) * (af - aav)


def bottom_matrix(shape):
    def beside(v):
        return sum(np.roll(v, step, axis) for axis in (1, 2, 3) for step in (1, -1))

    def residual(level, f, v):
        return f - ((6.0 * v - beside(v)) * 0.25**level + SCREEN * v)

    def cycle(level, f):
        v = np.zeros_like(f)
        for _ in range(2):
            v = v + OMEGA * residual(level, f, v) / (6.0 * 0.25**level + SCREEN)
        if level == LEVELS - 1:
            return v
        n, x, y, z = f.shape
        coarse = residual(level, f, v).reshape(n, x // 2, 2, y // 2, 2, z // 2, 2).mean(axis=(2, 4, 6))
        v = v + cycle(level + 1, coarse).repeat(2, 1).repeat(2, 2).repeat(2, 3)
        for _ in range(2):
            v = v + OMEGA * residual(level, f, v) / (6.0 * 0.25**level + SCREEN)
        return v

    cells = shape[0] * shape[1] * shape[2]
    return cycle(5, np.eye(cells).reshape(cells, *shape)).reshape(cells, cells).astype(np.float32)


def pair_layers(v):
    v = v.reshape(v.shape[0] // 2, 2, *v.shape[1:])
    return v[:, 0] + v[:, 1]


def twice(v):
    return jnp.concatenate([v[:, None], v[:, None]], axis=1).reshape(2 * v.shape[0], *v.shape[1:])


def flat(v):
    return v.reshape(-1, LANES)


def solve_bottom(s, shape, matrix):
    x5, y5, z5 = shape
    cells = x5 * y5 * z5
    rows = s.shape[0]
    cell, row = iota((rows, cells), 1), iota((rows, cells), 0)
    mine = (cell // (y5 * z5) == row // (2 * y5)) & (lax.rem(cell // z5, y5) == lax.rem(row, 2 * y5) // 2)
    source, out = iota((LANES, cells), 0), lax.rem(iota((LANES, cells), 1), z5)
    means = jnp.where((source == 2 * out) | (source == 2 * out + 1), 0.125, 0.0).astype(F32)
    f5 = jnp.sum(jnp.where(mine, dot(s, means), 0.0), axis=0, keepdims=True)
    f_high, f_middle, f_low = parts(jnp.broadcast_to(f5, (8, cells)))
    m_high, m_middle, m_low = parts(matrix[...])
    v5 = product(f_high, m_high) + (
        (product(f_high, m_middle) + product(f_middle, m_high))
        + (product(f_high, m_low) + product(f_middle, m_middle) + product(f_low, m_high))
    )
    spread = jnp.where(mine, jnp.broadcast_to(v5[0:1], (rows, cells)), 0.0)
    source, out = lax.rem(iota((cells, LANES), 0), z5), lax.rem(iota((cells, LANES), 1), 2 * z5)
    return dot(spread, jnp.where(source == out // 2, 1.0, 0.0).astype(F32))


def solve_3(f3, t3, matrix):
    x4, y4 = f3.shape[0] // 2, f3.shape[1] // 2
    parts_3 = LANES // (sizes_2()[2] // 2)
    v3, r3, af3 = start_whole(3, f3, parts_3)
    t3[...] = pair_layers(r3)
    s = flat(t3[:, pl.ds(0, y4, stride=2), :] + t3[:, pl.ds(1, y4, stride=2), :])
    z4 = LANES // parts_3 // 2
    means = [mean_matrix(lambda o: 2 * parts_3 * lax.rem(o, z4) + q, parts_3) for q in range(parts_3)]
    f4 = jnp.concatenate([dot(s, m).reshape(x4, y4, LANES) for m in means], axis=0)
    v4, r4, af4 = start_whole(4, f4)
    e4 = solve_bottom(flat(pair_layers(r4)), bottom_shape(), matrix).reshape(-1, y4, LANES)
    v4 = smooth_whole(4, f4, af4, v4 + twice(e4))
    picks = [pick_matrix(lambda o: jnp.where(lax.rem(o, parts_3) == q, o // parts_3 // 2, -1)) for q in range(parts_3)]
    e3 = sum(dot(flat(v4[x4 * q : x4 * (q + 1)]), m) for q, m in enumerate(picks)).reshape(x4, y4, LANES)
    t3[:, pl.ds(0, y4, stride=2), :] = e3
    t3[:, pl.ds(1, y4, stride=2), :] = e3
    return smooth_whole(3, f3, af3, v3 + twice(t3[...]), parts_3)


def unpack_2(f2, mine, other, core):
    even = lax.rem(iota((8, LANES), 1), 2) == 0
    top = iota((8, LANES), 0) < 4
    along_y = lax.axis_size("gy")
    half = (f2.shape[0] - 2) // 4

    def body(gx):
        for gy in range(along_y):
            tiles = []
            for g in (gx, gx + half):
                t, p = mine[g * along_y + gy], other[g * along_y + gy]
                u, w = jnp.where(core == 0, t, p), jnp.where(core == 0, p, t)
                tiles.append((u, w))
            (u, w), (u2, w2) = tiles
            for xp in range(2):
                if xp == 0:
                    d, e = jnp.where(even, u, pltpu.roll(u2, 1, 1)), jnp.where(even, w, pltpu.roll(w2, 1, 1))
                else:
                    d, e = jnp.where(even, pltpu.roll(u, LANES - 1, 1), u2), jnp.where(even, pltpu.roll(w, LANES - 1, 1), w2)
                f2[1 + gx * 4 + 2 * xp, pl.ds(gy * 8, 8), :] = jnp.where(top, d, pltpu.roll(e, 4, 0))
                f2[2 + gx * 4 + 2 * xp, pl.ds(gy * 8, 8), :] = jnp.where(top, pltpu.roll(d, 4, 0), e)

    over_layers(0, half, 4, body)


def close_2(v):
    last = v.shape[0] - 2
    v[0] = next_part(v[last], 2, True)
    v[last + 1] = next_part(v[1], 2, False)


def beside_2(centre, before, after):
    rows = centre.shape[0]
    return (
        (before + after) + (pltpu.roll(centre, 1, 0) + pltpu.roll(centre, rows - 1, 0)) + along_z(centre, 1, 2)
    )


def level_2(near, f2, v2, t2, t3, s3, p2, a2, b2, bottom, gx, halo):
    n, rows = f2.shape[0] - 2, f2.shape[1]
    close_2(f2)

    def first(i):
        v2[i] = twice_from_zero(2, f2[i], beside_2(f2[i], f2[i - 1], f2[i + 1]))

    over_layers(1, n, 16, first)
    close_2(v2)

    def second(q):
        pair = []
        for i in (2 * q + 1, 2 * q + 2):
            pair.append(residual_of(2, f2[i], v2[i], beside_2(v2[i], v2[i - 1], v2[i + 1])))
        t2[q] = pair[0] + pair[1]

    over_layers(0, n // 2, 8, second)
    s = t2[:, pl.ds(0, rows // 2, stride=2), :] + t2[:, pl.ds(1, rows // 2, stride=2), :]
    x3 = n // 4

    def means(part):
        def source(o):
            q = lax.rem(o, 4)
            return jnp.where(lax.rem(q, 2) == part, o // 4 * 4 + q // 2, -4)

        return mean_matrix(source, 2)

    f3 = dot(flat(s[:x3]), means(0)) + dot(flat(s[x3:]), means(1))
    s3[...] = solve_3(f3.reshape(x3, rows // 2, LANES), t3, bottom)

    count = 4 + 2 * halo + 4
    start = gx * 4 - halo - 2 + 2 * n
    lines = []
    for m in range(count // 2):
        at = lax.rem(lax.div(start, 2) + m, n)
        line = s3[lax.rem(at, x3)]
        lines.append(pltpu.roll(line, lax.rem(LANES - lax.div(at, x3), LANES), 1))
    e = dot(jnp.concatenate(lines, axis=0), pick_matrix(lambda o: o // 4 * 4)).reshape(count // 2, rows // 2, LANES)
    p2[pl.ds(0, count // 2), pl.ds(0, rows // 2, stride=2), :] = e
    p2[pl.ds(0, count // 2), pl.ds(1, rows // 2, stride=2), :] = e
    even = lax.rem(iota((rows, LANES), 1), 2) == 0
    for m in range(count):
        at = lax.rem(start + m, 2 * n)
        i, lower = 1 + lax.rem(at, n), at < n
        whole = []
        for ref in (v2, f2):
            line = ref[i]
            moved = pltpu.roll(line, jnp.where(lower, 1, LANES - 1), 1)
            whole.append(jnp.where(even == lower, line, moved))
        a2[m] = whole[0] + p2[m // 2]
        t2[m] = whole[1]
    for m in range(1, count - 1):
        nb = beside_2(a2[m], a2[m - 1], a2[m + 1])
        b2[m] = relaxed(2, t2[m], a2[m], nb)
    for m in range(2, count - 2):
        nb = beside_2(b2[m], b2[m - 1], b2[m + 1])
        near[m - 2] = relaxed(2, t2[m], b2[m], nb)


def add_from_2(v1, near, y2, p1, gy, core, halo):
    layers = 4 + 2 * halo
    rows, n = sizes_2()[1:]
    for m in range(layers):
        y2[m, pl.ds(0, rows), :] = near[m]
        y2[m, pl.ds(rows, rows), :] = near[m]
    start = pl.multiple_of(lax.rem(gy * 8 + rows - 4, rows), 4)
    picked = jnp.concatenate([y2[m, pl.ds(start, 16), :] for m in range(layers)], axis=0)
    e = dot(picked, pick_matrix(lambda o: 2 * lax.rem(lax.div(o, 2) + n // 2 * core, n))).reshape(layers, 16, LANES)
    p1[pl.ds(0, layers), pl.ds(0, 16, stride=2), :] = e
    p1[pl.ds(0, layers), pl.ds(1, 16, stride=2), :] = e
    for m in range(2 * layers):
        i = X1 - 2 * halo + m
        v1[i, pl.ds(Y1 - 8, 32), :] = v1[i, pl.ds(Y1 - 8, 32), :] + p1[m // 2]


def add_from_1(w, v, v1, p0, halo, x_at, y_from, skip, rows):
    for m in range(BX // 2 + 2 * halo):
        e = v1[X1 - halo + m, pl.ds(Y1 - 8, 32), :]
        p0[m, pl.ds(0, 32, stride=2), :] = e
        p0[m, pl.ds(1, 32, stride=2), :] = e
    for x in range(-2 * halo, BX + 2 * halo):
        for h in range(2):
            w[h][X0 + x, pl.ds(Y0 - skip, rows), :] = (
                v[h][x_at + x, pl.ds(y_from, rows), :] + p0[x // 2 + halo, pl.ds(16 - skip, rows), :]
            )


def lay_out_1(dst, f1, edges, core, own, x_edges, y_edges):
    up, down = edges[0][...], edges[1][...]
    other_up, other_down = (pltpu.roll(edge[...], 64, 1) for edge in edges[2:])
    first = core == 0
    x_low, y_low = jnp.where(first, up, other_up), jnp.where(first, other_up, up)
    x_high, y_high = jnp.where(first, down, other_down), jnp.where(first, other_down, down)
    past, width = y_edges
    for m in range(f1.shape[0]):
        i = X1 - own + m
        dst[i, pl.ds(Y1 - 4, 24), :] = f1[m]
        dst[i, pl.ds(Y1 - past - width, width), :] = y_low[m * width : (m + 1) * width]
        dst[i, pl.ds(Y1 + 16 + past, width), :] = y_high[m * width : (m + 1) * width]
    past, width = x_edges
    for m in range(width):
        known = slice(m * 24 + 4 - own, m * 24 + 20 + own)
        dst[X1 - past - width + m, pl.ds(Y1 - own, 16 + 2 * own), :] = x_low[known]
        dst[X1 + 8 + past + m, pl.ds(Y1 - own, 16 + 2 * own), :] = x_high[known]


def put_out_1(out, up, down, f1, core, own, x_edges, y_edges):
    for m in range(out.shape[0]):
        out[m] = f1[X1 - own + m, pl.ds(Y1 - 4, 24), :]

    @pl.when(core == 0)
    def _():
        past, width = x_edges
        for m in range(width):
            up[pl.ds(m * 24, 24), :] = f1[X1 + 8 - past - width + m, pl.ds(Y1 - 4, 24), :]
            down[pl.ds(m * 24, 24), :] = f1[X1 + past + m, pl.ds(Y1 - 4, 24), :]

    @pl.when(core == 1)
    def _():
        past, width = y_edges
        for m in range(out.shape[0]):
            up[pl.ds(m * width, width), :] = f1[X1 - own + m, pl.ds(Y1 + 16 - past - width, width), :]
            down[pl.ds(m * width, width), :] = f1[X1 - own + m, pl.ds(Y1 + past, width), :]


def split_kernel(charge, mine, up, down):
    matrix = pick_matrix(lambda o: jnp.where(o < 64, 2 * o, 2 * o - 127))
    split = dot(flat(charge[...]), matrix).reshape(BX, BY, LANES)
    mine[...] = split
    up[...] = split[BX - HALO :]
    down[...] = split[:HALO]


def edges_kernel(mine, x_low, x_high, up, down):
    at = 0
    for ref in (x_low, mine, x_high):
        for i in range(ref.shape[0]):
            down[pl.ds(at * HALO, HALO), :] = ref[i, pl.ds(0, HALO), :]
            up[pl.ds(at * HALO, HALO), :] = ref[i, pl.ds(BY - HALO, HALO), :]
            at += 1


def lay_out_0(even, odd, ours, others):
    def both(p, q):
        low = iota(p.shape, p.ndim - 1) < 64
        return (
            jnp.where(low, p, pltpu.roll(q, 64, p.ndim - 1)),
            jnp.where(low, pltpu.roll(p, 64, p.ndim - 1), q),
        )

    at = X0 - HALO
    for k in (1, 0, 2):
        for m in range(ours[k].shape[0]):
            e, o = both(ours[k][m], others[k][m])
            even[at, pl.ds(Y0, BY), :] = e
            odd[at, pl.ds(Y0, BY), :] = o
            at += 1
    for k, row in ((3, Y0 - HALO), (4, Y0 + BY)):
        e, o = both(ours[k][...], others[k][...])
        for m in range(BX + 2 * HALO):
            even[X0 - HALO + m, pl.ds(row, HALO), :] = e[m * HALO : (m + 1) * HALO]
            odd[X0 - HALO + m, pl.ds(row, HALO), :] = o[m * HALO : (m + 1) * HALO]


def first_kernel(where, *refs):
    ours, others, refs = refs[0:5], refs[5:10], refs[10:]
    (f_e, f_o, v_e, v_o, send), f1_outs, (f1, v1, r1, t0) = refs[:5], refs[5:8], refs[8:]
    core = where()[2]
    force, v = (f_e, f_o), (v_e, v_o)
    lay_out_0(f_e, f_o, ours, others)
    start_0(v, force, 9, 17)
    restrict_0(f1, t0, v, force, 4)
    coarse_source(send, f1, v1, r1, core)
    put_out_1(*f1_outs, f1, core, 4, *EDGES[0])


def middle_kernel(where, *refs):
    bottom, f_e, f_o, v_e, v_o, f1_in, mine, other, *edges = refs[:12]
    (n_e, n_o, send), f1_outs = refs[12:15], refs[15:18]
    a_e, a_o, b_e, b_o, f1, v1, r1, p1, y2, p0, t0, f2, v2, t2, t3, s3, p2, a2, b2, near = refs[18:]
    gx, gy, core = where()
    force, v, a0, b0 = (f_e, f_o), (v_e, v_o), (a_e, a_o), (b_e, b_o)
    unpack_2(f2, mine, other, core)
    level_2(near, f2, v2, t2, t3, s3, p2, a2, b2, bottom, gx, 4)
    lay_out_1(f1, f1_in, edges, core, 4, *EDGES[0])
    start_1(v1, f1, 7, 12)
    add_from_2(v1, near, y2, p1, gy, core, 4)
    sweep_1(r1, v1, f1, 6, 12)
    sweep_1(v1, r1, f1, 5, 9)
    add_from_1(a0, v, v1, p0, 5, X0, Y0 - 16, 16, 64)
    sweep_0(b0, a0, force, 8, 16)
    sweep_0(a0, b0, force, 7, 15)
    sweep_0(b0, a0, force, 6, 14)
    sweep_0(a0, b0, force, 5, 13)
    restrict_0(f1, t0, a0, force, 2)
    coarse_source(send, f1, v1, r1, core)
    put_out_1(*f1_outs, f1, core, 2, *EDGES[1])
    for src, dst in ((a_e, n_e), (a_o, n_o)):
        dst[...] = src[pl.ds(X0 - 2, 20), pl.ds(Y0 - 8, 48), :]


def last_kernel(where, *refs):
    bottom, f_e, f_o, n_e, n_o, f1_in, mine, other, *edges = refs[:12]
    out, a_e, a_o, b_e, b_o, f1, v1, r1, p1, y2, p0, _, f2, v2, t2, t3, s3, p2, a2, b2, near, held, left = refs[12:]
    gx, gy, core = where()
    force, v, a0, b0 = (f_e, f_o), (n_e, n_o), (a_e, a_o), (b_e, b_o)
    unpack_2(f2, mine, other, core)
    level_2(near, f2, v2, t2, t3, s3, p2, a2, b2, bottom, gx, 2)
    lay_out_1(f1, f1_in, edges, core, 2, *EDGES[1])
    start_1(v1, f1, 3, 14)
    add_from_2(v1, near, y2, p1, gy, core, 2)
    sweep_1(r1, v1, f1, 2, 12)
    sweep_1(v1, r1, f1, 1, 10)
    add_from_1(a0, v, v1, p0, 1, 2, 0, 8, 48)
    sweep_0(b0, a0, force, 1, 9)
    low = iota((BY, LANES), 1) < 64
    matrix = pick_matrix(lambda o: lax.div(o, 2) + 64 * lax.rem(o, 2))
    pieces = [pl.ds(4 * k, 4) for k in range(BX // 4)]
    stores = [pltpu.make_async_copy(held.at[p], out.at[p], left.at[k]) for k, p in enumerate(pieces)]
    for k, store in enumerate(stores):
        lines = []
        for i in range(X0 + 4 * k, X0 + 4 * k + 4):
            centre, nb = beside_0(b0, i, Y0, BY)
            even, odd = (relaxed(0, force[h][i, pl.ds(Y0, BY), :], centre[h], nb[h]) for h in range(2))
            lines.append(jnp.where(low, even, pltpu.roll(odd, 64, 1)))
        held[pieces[k]] = dot(jnp.concatenate(lines, axis=0), matrix).reshape(4, BY, LANES)
        store.start()
    for store in stores:
        store.wait()


def vm(*shape):
    return pltpu.VMEM(shape, F32)


def kept(*shape):
    return jax.ShapeDtypeStruct(shape, F32)


def scratch_for_cycle():
    x2, y2, _ = sizes_2()
    return (
        [vm(XA0, YA0, LANES)] * 4
        + [vm(XA1, YA1, LANES)] * 3
        + [vm(12, y2, LANES), vm(12, 2 * y2, LANES), vm(20, 64, LANES), vm(16, 48, LANES)]
        + [vm(x2 // 2 + 2, y2, LANES)] * 2
        + [vm(16, y2, LANES), vm(x2 // 16, y2 // 2, LANES), vm(x2 // 8, y2 // 2, LANES), vm(8, y2, LANES)]
        + [vm(16, y2, LANES)] * 2
        + [vm(12, y2, LANES)]
    )


def run(kernel, outs, scratch, flops, *args, out_space=pltpu.VMEM):
    spec = pl.BlockSpec(memory_space=out_space)
    return pl.pallas_call(
        kernel,
        out_shape=outs,
        out_specs=[spec] * len(outs) if isinstance(outs, list) else spec,
        scratch_shapes=scratch,
        compiler_params=pltpu.CompilerParams(vmem_limit_bytes=40 * 2**20),
        cost_estimate=pl.CostEstimate(flops=flops, bytes_accessed=2**20, transcendentals=0),
    )(*args)


def where_am_i():
    return lax.axis_index("gx"), lax.axis_index("gy"), lax.axis_index("gz")


def sources_out(layers, width):
    return [kept(peers(), 8, LANES), kept(layers, 24, LANES)] + [kept(width * 24, LANES)] * 2


def peers():
    return lax.axis_size("gx") * lax.axis_size("gy")


def split(charge):
    return run(split_kernel, [kept(BX, BY, LANES)] + [kept(HALO, BY, LANES)] * 2, [], 10**6, charge)


def edges(*args):
    return run(edges_kernel, [kept((BX + 2 * HALO) * HALO, LANES)] * 2, [], 10**6, *args)


def first(*args):
    outs = [kept(XA0, YA0, LANES)] * 4 + sources_out(16, EDGES[0][0][1])
    scratch = [vm(XA1, YA1, LANES)] * 3 + [vm(16, 48, LANES)]
    return run(functools.partial(first_kernel, where_am_i), outs, scratch, 10**7, *args)


def middle(*args):
    outs = [kept(20, 48, LANES)] * 2 + sources_out(12, EDGES[1][0][1])
    return run(functools.partial(middle_kernel, where_am_i), outs, scratch_for_cycle(), 4 * 10**7, *args)


def last(*args):
    outs = kept(BX, BY, LANES)
    scratch = scratch_for_cycle() + [vm(BX, BY, LANES), pltpu.SemaphoreType.DMA((BX // 4,))]
    return run(functools.partial(last_kernel, where_am_i), outs, scratch, 2 * 10**7, *args, out_space=pltpu.HBM)


def from_(value, axis, step):
    size = lax.axis_size(axis)
    return lax.ppermute(value, axis, [(i, (i + step) % size) for i in range(size)])


def beside_(value, step):
    axes = ("gx", "gy", "gz")
    sizes = [lax.axis_size(axis) for axis in axes]
    pairs = []
    for device in np.ndindex(*sizes):
        to = list(device)
        to[device[2]] = (to[device[2]] + step) % sizes[device[2]]
        pairs.append((int(np.ravel_multi_index(device, sizes)), int(np.ravel_multi_index(to, sizes))))
    return lax.ppermute(value, axes, pairs)


def exchange(send, f1, up, down):
    up, down = beside_(up, 1), beside_(down, -1)
    mine = lax.all_to_all(send, ("gx", "gy"), 0, 0, tiled=True)
    other, other_up, other_down = (from_(v, "gz", 1) for v in (mine, up, down))
    return f1, mine, other, up, down, other_up, other_down


def local(charge):
    mine, up, down = split(charge)
    x_low, x_high = from_(up, "gx", 1), from_(down, "gx", -1)
    up, down = edges(mine, x_low, x_high)
    y_low, y_high = from_(up, "gy", 1), from_(down, "gy", -1)
    ours = (mine, x_low, x_high, y_low, y_high)
    others = [from_(v, "gz", 1) for v in ours]
    f_e, f_o, v_e, v_o, *rest = first(*ours, *others)
    bottom = jnp.asarray(bottom_matrix(bottom_shape()))
    n_e, n_o, *rest = middle(bottom, f_e, f_o, v_e, v_o, *exchange(*rest))
    return last(bottom, f_e, f_o, n_e, n_o, *exchange(*rest))


def solution(mesh):
    return jax.shard_map(
        local,
        mesh=mesh,
        in_specs=(P(("groups", "gx"), "gy", "gz"),),
        out_specs=P(("groups", "gx"), "gy", "gz"),
        check_vma=False,
    )
```
